256 devices in a mesh: lb: 8 (over y, core), rb: 8 (over z), wa: 4 (over x).
Axes of the slice: x: 4, y: 4, z: 8, core: 2. Of those that a mesh axis runs over, the one named last changes fastest.
Arguments:
- state: bfloat16 [4, 4, 4, 1024, 1024], P('wa', None, None, 'lb', 'rb'), may hold values from -14 to 14
- left_env: bfloat16 [3, 4, 1024, 4, 1024], P(None, None, 'lb', 'wa'), may hold values from -1 to 2.5
- right_env: bfloat16 [3, 4, 1024, 4, 1024], P(None, None, 'rb', 'wa'), may hold values from -1 to 2.5
- site_one: float32 [3, 3, 2, 2], replicated, may hold values from -2 to 3
- site_two: float32 [3, 3, 2, 2], replicated, may hold values from -2 to 3
Outputs:
- next_vector: float32 [4, 4, 4, 1024, 1024], P('wa', None, None, 'lb', 'rb')
- coefficients: float32 [2], replicated
The draws below stay inside these ranges and needn't reach their ends.
All inputs are finite; a program needn't handle non-finite values.
Results may differ from the reference program's by a relative error of at most 0.02.
Values may be sent and summed in bfloat16 or wider, within the bound.
A program may use at most 128 MiB of HBM per device.

```python
import math
import jax
import jax.numpy as jnp
from jax import lax

BOND = 4096
BLOCKS = 4
BLOCK_ROWS = 1024
DW = 3
SITE_DIM = 2
PHYS = 4
LEFT_RANGES = 8
RIGHT_RANGES = 8


def environment(key):
    noise_key, diagonal_key = jax.random.split(key)
    full_shape = (DW, BLOCKS, BLOCK_ROWS, BLOCKS, BLOCK_ROWS)
    noise_values = jnp.clip(jax.random.normal(noise_key, full_shape, jnp.float32), -4.0, 4.0)
    diagonal = jax.random.uniform(diagonal_key, (DW, BLOCKS, BLOCK_ROWS), jnp.float32, 0.5, 1.5)
    block_identity = (lax.broadcasted_iota(jnp.int32, (BLOCKS, BLOCKS), 0) == lax.broadcasted_iota(jnp.int32, (BLOCKS, BLOCKS), 1)).astype(jnp.float32)
    row_identity = (lax.broadcasted_iota(jnp.int32, (BLOCK_ROWS, BLOCK_ROWS), 0) == lax.broadcasted_iota(jnp.int32, (BLOCK_ROWS, BLOCK_ROWS), 1)).astype(jnp.float32)
    identity = block_identity[:, None, :, None] * row_identity[None, :, None, :]
    values = noise_values / math.sqrt(BOND) + diagonal[:, :, :, None, None] * identity[None]
    return values.astype(jnp.bfloat16)


def draw_left_env(key, part):
    return environment(jax.random.fold_in(key, 11))


def draw_right_env(key, part):
    return environment(jax.random.fold_in(key, 23))


def site_tensor(key):
    full_shape = (DW, DW, SITE_DIM, SITE_DIM)
    noise_values = jnp.clip(jax.random.normal(key, full_shape, jnp.float32), -4.0, 4.0)
    bond_identity = (lax.broadcasted_iota(jnp.int32, (DW, DW), 0) == lax.broadcasted_iota(jnp.int32, (DW, DW), 1)).astype(jnp.float32)
    spin_identity = (lax.broadcasted_iota(jnp.int32, (SITE_DIM, SITE_DIM), 0) == lax.broadcasted_iota(jnp.int32, (SITE_DIM, SITE_DIM), 1)).astype(jnp.float32)
    return bond_identity[:, :, None, None] * spin_identity[None, None] + 0.5 * noise_values


def draw_site_one(key, part):
    return site_tensor(jax.random.fold_in(key, 41))


def draw_site_two(key, part):
    return site_tensor(jax.random.fold_in(key, 53))


def draw_state(key, part):
    noise_key = jax.random.fold_in(key, 37)
    full_shape = (BLOCKS, BLOCKS, PHYS, BLOCK_ROWS, BLOCK_ROWS)
    left_pos = lax.broadcasted_iota(jnp.float32, (BLOCK_ROWS, BLOCK_ROWS), 0) / BLOCK_ROWS
    rising = jnp.exp(math.log(3.3) * left_pos)
    noise_values = jnp.clip(jax.random.normal(noise_key, full_shape, jnp.float32), -4.0, 4.0)
    scaled = noise_values * rising[None, None, None]
    return scaled.astype(jnp.bfloat16)


def setup_inputs(seed: int = 0) -> dict:
    seeds = jax.random.split(jax.random.key(seed), 6)
    state = draw_state(jax.random.fold_in(seeds[5], 71), 0)
    left_env = draw_left_env(jax.random.fold_in(seeds[5], 71), 0)
    right_env = draw_right_env(jax.random.fold_in(seeds[5], 71), 0)
    site_one = draw_site_one(jax.random.fold_in(seeds[5], 71), 0)
    site_two = draw_site_two(jax.random.fold_in(seeds[5], 71), 0)
    return {"state": state, "left_env": left_env, "right_env": right_env, "site_one": site_one, "site_two": site_two}


EPSILON = 1e-06

def pair_tensor(site_one, site_two):
    joined = jnp.einsum('wuac,uvbd->wvabcd', site_one.astype(jnp.float32), site_two.astype(jnp.float32), precision=lax.Precision.HIGHEST)
    mpo_width = site_one.shape[0]
    states = site_one.shape[2] * site_two.shape[2]
    return joined.reshape(mpo_width, mpo_width, states, states)

def reference(state, left_env, right_env, site_one, site_two):
    mpo_pair = pair_tensor(site_one, site_two)
    mpo_width = left_env.shape[0]
    left_rows = BLOCK_ROWS // LEFT_RANGES
    right_rows = BLOCK_ROWS // RIGHT_RANGES
    trailing = BLOCKS * PHYS * BLOCK_ROWS
    state_rows = jnp.transpose(state, (0, 3, 1, 2, 4))

    def left_contract(env_slice):

        def add_range(running, position):
            offset = (position * left_rows).astype(jnp.int32)
            env_rows = lax.dynamic_slice_in_dim(env_slice, offset, left_rows, 1).reshape(BLOCKS * left_rows, BLOCKS * BLOCK_ROWS)
            state_part = lax.dynamic_slice_in_dim(state_rows, offset, left_rows, 1).reshape(BLOCKS * left_rows, trailing)
            partial_value = jnp.dot(env_rows.T, state_part, preferred_element_type=jnp.float32)
            rounded = lax.optimization_barrier(partial_value.astype(jnp.bfloat16)).astype(jnp.float32)
            return (running + rounded, None)
        running, _ = lax.scan(add_range, jnp.zeros((BLOCKS * BLOCK_ROWS, trailing), jnp.float32), jnp.arange(LEFT_RANGES, dtype=jnp.int32))
        return running
    left_sum = lax.map(left_contract, left_env)
    left_sum = left_sum.reshape(mpo_width, BLOCKS * BLOCK_ROWS, BLOCKS, PHYS, BLOCK_ROWS)
    mixed_state = jnp.einsum('wphsn,wvst->ptvhn', left_sum, mpo_pair, precision=lax.Precision.HIGHEST).astype(jnp.bfloat16)
    env_right = right_env.reshape(mpo_width, BLOCKS, BLOCK_ROWS, BLOCKS * BLOCK_ROWS)

    def add_right(running, position):
        offset = (position * right_rows).astype(jnp.int32)
        mixed_part = lax.dynamic_slice_in_dim(mixed_state, offset, right_rows, 4).reshape(BLOCKS * BLOCK_ROWS * PHYS, mpo_width * BLOCKS * right_rows)
        env_part = lax.dynamic_slice_in_dim(env_right, offset, right_rows, 2).reshape(mpo_width * BLOCKS * right_rows, BLOCKS * BLOCK_ROWS)
        partial_value = jnp.dot(mixed_part, env_part, preferred_element_type=jnp.float32)
        rounded = lax.optimization_barrier(partial_value.astype(jnp.bfloat16)).astype(jnp.float32)
        return (running + rounded, None)
    image_rows, _ = lax.scan(add_right, jnp.zeros((BLOCKS * BLOCK_ROWS * PHYS, BLOCKS * BLOCK_ROWS), jnp.float32), jnp.arange(RIGHT_RANGES, dtype=jnp.int32))
    applied = jnp.transpose(image_rows.reshape(BLOCKS, BLOCK_ROWS, PHYS, BLOCKS, BLOCK_ROWS), (0, 3, 2, 1, 4))
    state_values = state.astype(jnp.float32)
    norm_sq = jnp.mean(state_values * state_values) + EPSILON
    projection = jnp.mean(state_values * applied)
    alpha_coef = projection / norm_sq
    residual = (applied - alpha_coef * state_values) / jnp.sqrt(norm_sq)
    beta_coef = jnp.sqrt(jnp.mean(residual * residual) + EPSILON)
    return (residual / beta_coef, jnp.stack([alpha_coef, beta_coef]))
```

```python
import functools

import jax
import jax.numpy as jnp
from jax import lax
from jax.experimental import pallas as pl
from jax.experimental.pallas import tpu as pltpu
from jax.sharding import Mesh
from jax.sharding import PartitionSpec as P

LB = ("lb_0", "lb_1")
EPSILON = 1e-06
ENTRIES = 4.0 * 4 * 4 * 1024 * 1024
F32, BF16 = jnp.float32, jnp.bfloat16
X, Y, Z, H = 4, 4, 8, 4
N_SEMS = 160
UNITS = (0, 1, 3, 2)


def pair_tensor(site_one, site_two):
    one = site_one[:, :, None, :, None, :, None]
    two = site_two[None, :, :, None, :, None, :]
    return jnp.sum(one * two, axis=1).reshape(144)


def matmul(a, b):
    return lax.dot_general(a, b, (((1,), (0,)), ((), ())), preferred_element_type=F32)


def kernel(
    mpo,
    state,
    left,
    right,
    out,
    coef,
    blocks,
    left_other,
    left_t,
    far,
    up,
    down,
    up_far,
    down_far,
    from_below,
    from_above,
    left_sum,
    mixed,
    envs,
    image,
    ring_half,
    ring_full,
    sums_z,
    sums_y,
    sums_x,
    send_sems,
    recv_sems,
    local_sems,
):
    y, c, z, x = (lax.axis_index(a) for a in ("lb_0", "lb_1", "rb", "wa"))
    other = 1 - c

    def at(dx=0, dy=0, dz=0, core=None):
        return (
            lax.rem(y + dy, Y),
            c if core is None else core,
            lax.rem(z + dz, Z),
            lax.rem(x + dx, X),
        )

    used = []

    def copy(src, dst, device):
        k = len(used)
        used.append(
            pltpu.make_async_remote_copy(
                src_ref=src,
                dst_ref=dst,
                send_sem=send_sems.at[k],
                recv_sem=recv_sems.at[k],
                device_id=device,
                device_id_type=pl.DeviceIdType.MESH,
            )
        )
        return used[-1]

    partner = at(core=other)
    x_up, x_down = at(dx=1), at(dx=X - 1)
    y_up, y_down = at(dy=1), at(dy=Y - 1)
    z_up, z_down = at(dz=1), at(dz=Z - 1)
    z_peers = [at(dz=k) for k in range(1, Z)]
    y_peers = [partner] + [at(dy=k, core=core) for k in range(1, Y) for core in (c, other)]
    x_peers = [at(dx=k) for k in range(1, X)]

    barrier = pltpu.get_barrier_semaphore()
    peers = z_peers + y_peers + x_peers
    for peer in peers:
        pl.semaphore_signal(barrier, inc=1, device_id=peer, device_id_type=pl.DeviceIdType.MESH)

    own = x * 2 + c
    local = [
        pltpu.make_async_copy(state.at[h], blocks.at[h, own], local_sems.at[h]) for h in range(H)
    ]
    local.append(pltpu.make_async_copy(right, envs.at[0], local_sems.at[H]))
    for item in local:
        item.start()
    pl.semaphore_wait(barrier, len(peers))

    g_below = lax.rem(x + X - 1, X) * 2 + c
    g_above = lax.rem(x + 1, X) * 2 + c
    g_far = lax.rem(x + 2, X) * 2 + c
    lo, hi = pl.ds(0, 64), pl.ds(64, 64)
    b_up = [copy(state.at[h], blocks.at[h, own], x_up) for h in range(H)]
    b_down = [copy(state.at[h], blocks.at[h, own], x_down) for h in range(H)]
    b_own = [copy(state.at[h], blocks.at[h, own], partner) for h in range(H)]
    bf_up = [copy(blocks.at[h, g_below, lo], blocks.at[h, g_below, lo], x_up) for h in range(H)]
    bf_down = [copy(blocks.at[h, g_above, hi], blocks.at[h, g_above, hi], x_down) for h in range(H)]
    b_pass = [
        [
            copy(blocks.at[h, g_below], blocks.at[h, g_below], partner),
            copy(blocks.at[h, g_above], blocks.at[h, g_above], partner),
            copy(blocks.at[h, g_far, lo], blocks.at[h, g_far, lo], partner),
            copy(blocks.at[h, g_far, hi], blocks.at[h, g_far, hi], partner),
        ]
        for h in range(H)
    ]

    def start_own(h):
        b_up[h].start()
        b_down[h].start()
        b_own[h].start()

    def pass_near(h):
        b_up[h].wait_recv()
        bf_up[h].start()
        b_pass[h][0].start()
        b_down[h].wait_recv()
        bf_down[h].start()
        b_pass[h][1].start()

    def get_blocks(h):
        bf_up[h].wait_recv()
        b_pass[h][2].start()
        bf_down[h].wait_recv()
        b_pass[h][3].start()
        local[h].wait()
        b_own[h].wait_recv()
        for item in b_pass[h]:
            item.wait_recv()

    a_swap = [
        copy(
            left.at[:, :, pl.ds(pl.multiple_of(k * 256 + other * 128, 128), 128)],
            left_other.at[k],
            partner,
        )
        for k in range(Y)
    ]

    def transpose_own(i, _):
        w, g = i // 4, lax.rem(i, 4)
        for r in range(Y):
            cols = pl.ds(pl.multiple_of(lax.rem(y + r, Y) * 256 + c * 128, 128), 128)
            left_t[
                r,
                pl.ds(pl.multiple_of(w * 128, 128), 128),
                pl.ds(pl.multiple_of((g * 2 + c) * 128, 128), 128),
            ] = left[i, :, cols].T
        return 0

    def transpose_other(i, _):
        w, g = i // 4, lax.rem(i, 4)
        for r in range(Y):
            left_t[
                r,
                pl.ds(pl.multiple_of(w * 128, 128), 128),
                pl.ds(pl.multiple_of((g * 2 + other) * 128, 128), 128),
            ] = left_other[lax.rem(y + r, Y), i].T
        return 0

    start_own(0)
    start_own(1)
    for item in a_swap:
        item.start()
    lax.fori_loop(0, 12, transpose_own, 0)
    for item in a_swap:
        item.wait_recv()
    lax.fori_loop(0, 12, transpose_other, 0)

    top, low = pl.ds(0, 192), pl.ds(192, 192)
    c_far_up = [copy(far.at[h, top], up_far.at[h], y_up) for h in range(H)]
    c_far_down = [copy(far.at[h, low], down_far.at[h], y_down) for h in range(H)]
    c_up_low = [copy(up.at[h, low], from_below.at[h, low], y_up) for h in range(H)]
    c_down_top = [copy(down.at[h, top], from_above.at[h, top], y_down) for h in range(H)]
    c_up_top = [copy(up.at[h, top], from_below.at[h, top], y_up) for h in range(H)]
    c_down_low = [copy(down.at[h, low], from_above.at[h, low], y_down) for h in range(H)]

    def product(r, rows, h, store):
        def tile(j, _):
            cols = pl.ds(pl.multiple_of(j * 256, 256), 256)
            b = blocks[h, :, :, cols].reshape(1024, 256)
            store(cols, matmul(left_t[r, rows, :], b))
            return 0

        lax.fori_loop(0, 2, tile, 0)

    def start_far(h):
        def store(cols, value):
            far[h, :, cols] = value.astype(BF16)

        product(2, pl.ds(0, 384), h, store)
        c_far_up[h].start()
        c_far_down[h].start()

    def start_direct(h):
        def store_up(cols, value):
            up[h, low, cols] = value.astype(BF16)

        def store_down(cols, value):
            down[h, top, cols] = value.astype(BF16)

        product(1, low, h, store_up)
        c_up_low[h].start()
        product(3, top, h, store_down)
        c_down_top[h].start()

    def pass_far(h):
        def store_up(cols, value):
            up[h, top, cols] = (value + up_far[h, :, cols].astype(F32)).astype(BF16)

        def store_down(cols, value):
            down[h, low, cols] = (value + down_far[h, :, cols].astype(F32)).astype(BF16)

        c_far_up[h].wait_recv()
        product(1, top, h, store_up)
        c_up_top[h].start()
        c_far_down[h].wait_recv()
        product(3, low, h, store_down)
        c_down_low[h].start()

    def mix(h):
        def store(cols, value):
            left_sum[:, cols] = (
                value + from_below[h, :, cols].astype(F32) + from_above[h, :, cols].astype(F32)
            )

        for item in (c_up_low[h], c_down_top[h], c_up_top[h], c_down_low[h]):
            item.wait_recv()
        product(0, pl.ds(0, 384), h, store)

        def rows_of(i, _):
            start = pl.multiple_of(i * 16, 16)
            parts = [
                left_sum[pl.ds(w * 128 + start, 16), s * 128 : (s + 1) * 128]
                for w in range(3)
                for s in range(4)
            ]
            for v in range(3):
                for t in range(4):
                    total = None
                    for w in range(3):
                        for s in range(4):
                            term = mpo[((w * 3 + v) * 4 + s) * 4 + t] * parts[w * 4 + s]
                            total = term if total is None else total + term
                    k = v * 4 + h
                    mixed[pl.ds(t * 128 + start, 16), k * 128 : (k + 1) * 128] = total.astype(BF16)
            return 0

        lax.fori_loop(0, 8, rows_of, 0)

    half = pl.ds(c * 6, 6)
    q_lo, q_hi = pl.ds(c * 6, 3), pl.ds(c * 6 + 3, 3)
    r_up = copy(envs.at[0, half], envs.at[3, half], x_up)
    r_down = copy(envs.at[0, half], envs.at[1, half], x_down)
    rf_up = copy(envs.at[3, q_lo], envs.at[2, q_lo], x_up)
    rf_down = copy(envs.at[1, q_hi], envs.at[2, q_hi], x_down)
    rp_below = copy(envs.at[3, half], envs.at[3, half], partner)
    rp_above = copy(envs.at[1, half], envs.at[1, half], partner)
    rp_lo = copy(envs.at[2, q_lo], envs.at[2, q_lo], partner)
    rp_hi = copy(envs.at[2, q_hi], envs.at[2, q_hi], partner)

    def start_envs():
        local[H].wait()
        r_up.start()
        r_down.start()

    def pass_envs():
        r_up.wait_recv()
        rf_up.start()
        rp_below.start()
        r_down.wait_recv()
        rf_down.start()
        rp_above.start()

    def pass_far_envs():
        rf_up.wait_recv()
        rp_lo.start()
        rf_down.wait_recv()
        rp_hi.start()

    pass_near(0)
    start_own(2)
    pass_near(1)
    start_own(3)
    get_blocks(0)
    start_far(0)
    start_direct(0)
    pass_near(2)
    get_blocks(1)
    start_far(1)
    pass_far(0)
    start_direct(1)
    pass_near(3)
    get_blocks(2)
    start_far(2)
    pass_far(1)
    start_direct(2)
    mix(0)
    get_blocks(3)
    start_envs()
    start_far(3)
    pass_far(2)
    start_direct(3)
    mix(1)
    pass_far(3)
    mix(2)
    mix(3)
    pass_envs()

    def zmod(k):
        return lax.rem(z + k, Z)

    first, second = pl.ds(0, 256), pl.ds(256, 256)
    rings = []
    for u in range(4):
        ring = {}
        ring[1] = (
            copy(image.at[u, zmod(4), first], ring_half.at[u, 0], z_up),
            copy(image.at[u, zmod(4), second], ring_half.at[u, 1], z_down),
        )
        for k in (2, 3, 4):
            ring[k] = (
                copy(image.at[u, zmod(5 - k)], ring_full.at[u, 0, k - 2], z_up),
                copy(image.at[u, zmod(3 + k)], ring_full.at[u, 1, k - 2], z_down),
            )
        rings.append(ring)

    def contract(u):
        i = UNITS[u]
        if i == 1:
            rp_above.wait_recv()
        if i == 3:
            rp_below.wait_recv()
        if i == 2:
            rp_lo.wait_recv()
            rp_hi.wait_recv()

        def tile(j, _):
            cols = pl.ds(pl.multiple_of(j * 256, 256), 256)
            value = matmul(mixed[...], envs[i, :, :, cols].reshape(1536, 256)).astype(BF16)
            image[u, j * 2] = value[:, :128]
            image[u, j * 2 + 1] = value[:, 128:]
            return 0

        lax.fori_loop(0, 4, tile, 0)

    def add_into(u, k, rows, term):
        image[u, k, rows] = (image[u, k, rows].astype(F32) + term.astype(F32)).astype(BF16)

    def hop(u, k):
        for side in range(2):
            if k > 1:
                rings[u][k - 1][side].wait_recv()
                owner = zmod(5 - k) if side == 0 else zmod(3 + k)
                if k == 2:
                    add_into(u, owner, (first, second)[side], ring_half[u, side])
                else:
                    add_into(u, owner, pl.ds(0, 512), ring_full[u, side, k - 3])
            rings[u][k][side].start()

    zero = jnp.zeros((8, 128), F32)

    def folded(value):
        return jnp.sum(value.reshape(-1, 8, 128), axis=0)

    def finish(u, sums):
        rings[u][4][0].wait_recv()
        rings[u][4][1].wait_recv()
        h = lax.rem(x + UNITS[u], X)

        def piece(s, sums):
            squares, crossed, images = sums
            rows = pl.ds(pl.multiple_of(s * 128, 128), 128)
            value = (
                image[u, z, rows].astype(F32)
                + ring_full[u, 0, 2, rows].astype(F32)
                + ring_full[u, 1, 2, rows].astype(F32)
            )
            out[h, rows] = value
            start = state[h, :, rows].astype(F32)
            return (
                squares + folded(start * start),
                crossed + folded(start * value),
                images + folded(value * value),
            )

        return lax.fori_loop(0, 4, piece, sums)

    contract(0)
    hop(0, 1)
    contract(1)
    hop(1, 1)
    hop(0, 2)
    hop(1, 2)
    contract(2)
    hop(2, 1)
    hop(0, 3)
    hop(1, 3)
    hop(2, 2)
    hop(0, 4)
    pass_far_envs()
    hop(1, 4)
    contract(3)
    hop(3, 1)
    hop(2, 3)
    hop(3, 2)
    hop(2, 4)
    hop(3, 3)
    sums = finish(0, (zero, zero, zero))
    hop(3, 4)
    sums = finish(1, sums)
    sums = finish(2, sums)
    sums = finish(3, sums)

    def all_sum(values, slots, me, targets):
        slots[me] = values
        sends = [copy(slots.at[me], slots.at[me], target) for target in targets]
        for item in sends:
            item.start()
        for item in sends:
            item.wait_recv()
        return jnp.sum(slots[...], axis=0)

    packed = jnp.concatenate([jnp.sum(v, axis=0, keepdims=True) for v in sums] + [zero[:5]], axis=0)
    packed = all_sum(packed, sums_z, z, z_peers)
    packed = all_sum(packed, sums_y, y * 2 + c, y_peers)
    packed = all_sum(packed, sums_x, x, x_peers)
    means = jnp.sum(packed, axis=1, keepdims=True) * (1.0 / ENTRIES)
    square, projection, image_square = means[0:1], means[1:2], means[2:3]
    norm_sq = square + EPSILON
    alpha = projection / norm_sq
    residual_sq = (image_square - 2.0 * alpha * projection + alpha * alpha * square) / norm_sq
    beta = jnp.sqrt(residual_sq + EPSILON)
    scale = 1.0 / (jnp.sqrt(norm_sq) * beta)
    lane = lax.broadcasted_iota(jnp.int32, (8, 128), 1)
    coef[...] = jnp.where(lane == 0, alpha, beta)

    def scaled(i, _):
        h, s = i // 4, lax.rem(i, 4)
        rows = pl.ds(pl.multiple_of(s * 128, 128), 128)
        out[h, rows] = (out[h, rows] - alpha * state[h, :, rows].astype(F32)) * scale
        return 0

    lax.fori_loop(0, 16, scaled, 0)
    for item in used:
        item.wait_send()


def body(state, left_env, right_env, site_one, site_two):
    mpo = pair_tensor(site_one, site_two)
    rows = state.reshape(4, 4, 128, 128).transpose(0, 2, 1, 3).reshape(4, 128, 512)
    vmem = pl.BlockSpec(memory_space=pltpu.VMEM)
    out, coef = pl.pallas_call(
        kernel,
        out_shape=(
            jax.ShapeDtypeStruct((4, 512, 128), F32),
            jax.ShapeDtypeStruct((8, 128), F32),
        ),
        in_specs=[
            pl.BlockSpec(memory_space=pltpu.SMEM),
            vmem,
            vmem,
            pl.BlockSpec(memory_space=pl.ANY),
        ],
        out_specs=(vmem, vmem),
        scratch_shapes=[
            pltpu.VMEM((4, 8, 128, 512), BF16),
            pltpu.VMEM((4, 12, 128, 128), BF16),
            pltpu.VMEM((4, 384, 1024), BF16),
            pltpu.VMEM((4, 384, 512), BF16),
            pltpu.VMEM((4, 384, 512), BF16),
            pltpu.VMEM((4, 384, 512), BF16),
            pltpu.VMEM((4, 192, 512), BF16),
            pltpu.VMEM((4, 192, 512), BF16),
            pltpu.VMEM((4, 384, 512), BF16),
            pltpu.VMEM((4, 384, 512), BF16),
            pltpu.VMEM((384, 512), F32),
            pltpu.VMEM((512, 1536), BF16),
            pltpu.VMEM((4, 12, 128, 1024), BF16),
            pltpu.VMEM((4, 8, 512, 128), BF16),
            pltpu.VMEM((4, 2, 256, 128), BF16),
            pltpu.VMEM((4, 2, 3, 512, 128), BF16),
            pltpu.VMEM((8, 8, 128), F32),
            pltpu.VMEM((8, 8, 128), F32),
            pltpu.VMEM((4, 8, 128), F32),
            pltpu.SemaphoreType.DMA((N_SEMS,)),
            pltpu.SemaphoreType.DMA((N_SEMS,)),
            pltpu.SemaphoreType.DMA((H + 1,)),
        ],
        compiler_params=pltpu.CompilerParams(
            collective_id=0, has_side_effects=True, vmem_limit_bytes=64_000_000
        ),
        name="lanczos",
    )(mpo, rows, left_env.reshape(12, 128, 1024), right_env.reshape(12, 128, 1024))
    return out.reshape(1, 4, 4, 128, 128), coef[0, :2]


def solution(mesh):
    torus = Mesh(
        mesh.devices.reshape(4, 2, mesh.shape["rb"], mesh.shape["wa"]), ("lb_0", "lb_1", "rb", "wa")
    )
    in_specs = (
        P("wa", None, None, LB, "rb"),
        P(None, None, LB, "wa", None),
        P(None, None, "rb", "wa", None),
        P(),
        P(),
    )
    out_specs = (P("wa", None, None, LB, "rb"), P())
    return jax.shard_map(body, mesh=torus, in_specs=in_specs, out_specs=out_specs, check_vma=False)
```

```python
import functools

import jax
import jax.numpy as jnp
from jax import lax
from jax.experimental import pallas as pl
from jax.experimental.pallas import tpu as pltpu
from jax.sharding import Mesh
from jax.sharding import PartitionSpec as P

LB = ("lb_0", "lb_1")
EPSILON = 1e-06
ENTRIES = 4.0 * 4 * 4 * 1024 * 1024
F32, BF16 = jnp.float32, jnp.bfloat16
X, Y, Z, H = 4, 4, 8, 4
N_SEMS = 240
ITEMS = 8
UNITS = tuple((m, i) for m in range(2) for i in (0, 1, 3, 2))


ORDER = (
    "own.0", "turn.0", "near.0", "own.1", "turn.1", "rest.0", "own.2", "turn.2",
    "blocks.0", "left.0", "direct.0",
    "near.1", "rest.1", "own.3", "near.2", "rest.2", "blocks.1", "left.1", "far.0", "direct.1",
    "near.3", "rest.3", "envs", "blocks.2", "left.2", "far.1", "direct.2",
    "mix.0", "blocks.3", "left.3", "far.2", "direct.3",
    "left.4", "mix.1", "penvs.0", "far.3", "direct.4",
    "left.5", "mix.2", "far.4", "direct.5",
    "penvs.1", "left.6", "mix.3", "con.0", "far.5", "direct.6", "hop.0.2",
    "left.7", "hop.0.3", "mix.4", "hop.0.4", "far.6", "direct.7",
    "penvs.2", "mix.5", "con.1", "con.2", "far.7", "hop.1.2", "hop.2.2", "mix.6", "hop.1.3", "hop.2.3",
    "mix.7", "con.4", "hop.1.4", "hop.2.4", "con.5", "con.6", "hop.4.2", "hop.5.2", "hop.6.2", "fenvs",
    "hop.4.3", "hop.5.3", "con.3", "con.7", "hop.6.3", "hop.4.4", "hop.3.2", "hop.5.4", "hop.7.2", "hop.6.4",
    "fin.0", "fin.1", "fin.2", "hop.3.3", "hop.7.3", "fin.4", "fin.5", "fin.6",
    "hop.3.4", "hop.7.4", "fin.3", "fin.7",
)


def staged(f):
    def run(*args):
        with jax.named_scope(f"{f.__name__}#" + "_".join(str(a) for a in args if isinstance(a, int))):
            return f(*args)

    return run


def matmul(a, b):
    return lax.dot_general(a, b, (((1,), (0,)), ((), ())), preferred_element_type=F32)


def step(
    one,
    two,
    state_in,
    left_in,
    right_in,
    out,
    coef,
    state,
    left,
    pair,
    blocks,
    left_other,
    left_t,
    far,
    up,
    down,
    up_own,
    down_own,
    here,
    up_far,
    down_far,
    from_below,
    from_above,
    mixed,
    envs,
    image,
    ring_half,
    ring_full,
    sums_z,
    sums_xy,
    send_sems,
    recv_sems,
    local_sems,
):
    y, c, z, x = (lax.axis_index(a) for a in ("lb_0", "lb_1", "rb", "wa"))
    other = 1 - c

    def at(dx=0, dy=0, dz=0, core=None):
        return (
            lax.rem(y + dy, Y),
            c if core is None else core,
            lax.rem(z + dz, Z),
            lax.rem(x + dx, X),
        )

    used = []

    def copy(src, dst, device):
        k = len(used)
        used.append(
            pltpu.make_async_remote_copy(
                src_ref=src,
                dst_ref=dst,
                send_sem=send_sems.at[k],
                recv_sem=recv_sems.at[k],
                device_id=device,
                device_id_type=pl.DeviceIdType.MESH,
            )
        )
        return used[-1]

    partner = at(core=other)
    x_up, x_down = at(dx=1), at(dx=X - 1)
    y_up, y_down = at(dy=1), at(dy=Y - 1)
    z_up, z_down = at(dz=1), at(dz=Z - 1)
    z_peers = [at(dz=k) for k in range(1, Z)]
    xy_peers = [
        at(dx=i, dy=j, core=core)
        for i in range(X)
        for j in range(Y)
        for core in (c, other)
        if not (i == 0 and j == 0 and core is c)
    ]

    barrier = pltpu.get_barrier_semaphore()
    peers = z_peers + xy_peers
    for peer in peers:
        pl.semaphore_signal(barrier, inc=1, device_id=peer, device_id_type=pl.DeviceIdType.MESH)

    own = x * 2 + c
    load_state = pltpu.make_async_copy(state_in, state, local_sems.at[H + 1])
    load_left = pltpu.make_async_copy(left_in, left, local_sems.at[H + 2])
    local = [
        pltpu.make_async_copy(state_in.at[pl.ds(h * 4, 4)], blocks.at[h, own], local_sems.at[h])
        for h in range(H)
    ]
    local.append(pltpu.make_async_copy(right_in, envs.at[0], local_sems.at[H]))
    for item in [load_state, load_left] + local:
        item.start()

    with jax.named_scope("pairs"):
        for w in range(3):
            for v in range(3):
                for s in range(4):
                    for t in range(4):
                        total = sum(
                            one[w, s // 2, t // 2, u] * two[u, s % 2, t % 2, v] for u in range(3)
                        )
                        k = ((w * 3 + v) * 4 + s) * 4 + t
                        pair[k] = jnp.full((8, 128), total, F32)
    with jax.named_scope("entry"):
        load_state.wait()
        pl.semaphore_wait(barrier, len(peers))

    g_below = lax.rem(x + X - 1, X) * 2 + c
    g_above = lax.rem(x + 1, X) * 2 + c
    g_far = lax.rem(x + 2, X) * 2 + c
    lo, hi = pl.ds(0, 2), pl.ds(2, 2)
    mine = [state.at[pl.ds(h * 4, 4)] for h in range(H)]

    def send_mine(h, parts, device):
        return [copy(mine[h].at[part], blocks.at[h, own, part], device) for part in parts]

    whole = (pl.ds(0, 4),)
    b_up = [send_mine(h, (lo, hi) if h == 0 else whole, x_up) for h in range(H)]
    b_down = [send_mine(h, (hi, lo) if h == 0 else whole, x_down) for h in range(H)]
    b_own = [copy(mine[h], blocks.at[h, own], partner) for h in range(H)]
    bf_up = [copy(blocks.at[h, g_below, lo], blocks.at[h, g_below, lo], x_up) for h in range(H)]
    bf_down = [copy(blocks.at[h, g_above, hi], blocks.at[h, g_above, hi], x_down) for h in range(H)]
    b_pass = [
        [
            copy(blocks.at[h, g_below], blocks.at[h, g_below], partner),
            copy(blocks.at[h, g_above], blocks.at[h, g_above], partner),
            copy(blocks.at[h, g_far, lo], blocks.at[h, g_far, lo], partner),
            copy(blocks.at[h, g_far, hi], blocks.at[h, g_far, hi], partner),
        ]
        for h in range(H)
    ]

    @staged
    def start_own(h):
        for pair_of in zip(b_up[h], b_down[h]):
            for item in pair_of:
                item.start()
        b_own[h].start()

    @staged
    def pass_near(h):
        b_up[h][0].wait_recv()
        bf_up[h].start()
        b_down[h][0].wait_recv()
        bf_down[h].start()

    @staged
    def pass_rest(h):
        for item in b_up[h][1:]:
            item.wait_recv()
        b_pass[h][0].start()
        for item in b_down[h][1:]:
            item.wait_recv()
        b_pass[h][1].start()

    @staged
    def get_blocks(h):
        bf_up[h].wait_recv()
        b_pass[h][2].start()
        bf_down[h].wait_recv()
        b_pass[h][3].start()
        local[h].wait()
        b_own[h].wait_recv()
        for item in b_pass[h]:
            item.wait_recv()

    a_swap = [
        copy(
            left.at[:, :, pl.ds(pl.multiple_of(k * 256 + other * 128, 128), 128)],
            left_other.at[k],
            partner,
        )
        for k in range(Y)
    ]

    def put_left(r, w, g, core, tile):
        cols = pl.ds(pl.multiple_of((g * 2 + core) * 128, 128), 128)
        rows = pl.ds(pl.multiple_of(r * 192 + w * 64, 64), 64)
        turned = tile.T
        left_t[0, rows, cols] = turned[:64]
        left_t[1, rows, cols] = turned[64:]

    def transpose_own(i, _):
        for r in range(Y):
            cols = pl.ds(pl.multiple_of(lax.rem(y + r, Y) * 256 + c * 128, 128), 128)
            put_left(r, i // 4, lax.rem(i, 4), c, left[i, :, cols])
        return 0

    def transpose_other(i, _):
        for r in range(Y):
            put_left(r, i // 4, lax.rem(i, 4), other, left_other[lax.rem(y + r, Y), i])
        return 0

    top, low = pl.ds(0, 96), pl.ds(96, 96)
    items = range(ITEMS)
    c_far_up = [copy(far.at[i, top], up_far.at[i], y_up) for i in items]
    c_far_down = [copy(far.at[i, low], down_far.at[i], y_down) for i in items]
    c_up_low = [copy(up.at[i, low], from_below.at[i, low], y_up) for i in items]
    c_down_top = [copy(down.at[i, top], from_above.at[i, top], y_down) for i in items]
    c_up_top = [copy(up.at[i, top], from_below.at[i, top], y_up) for i in items]
    c_down_low = [copy(down.at[i, low], from_above.at[i, low], y_down) for i in items]

    @staged
    def left_item(i):
        m, h = divmod(i, H)

        def tile(j, _):
            cols = pl.ds(pl.multiple_of(j * 256, 256), 256)
            b = jnp.concatenate(
                [blocks[h, :, j * 2].reshape(1024, 128), blocks[h, :, j * 2 + 1].reshape(1024, 128)],
                axis=1,
            )
            value = matmul(left_t[m], b)
            far[i, :, cols] = value[384:576].astype(BF16)
            up_own[i, :, cols] = value[192:288]
            up[i, low, cols] = value[288:384].astype(BF16)
            down[i, top, cols] = value[576:672].astype(BF16)
            down_own[i, :, cols] = value[672:768]
            here[i, :, cols] = value[:192]
            return 0

        lax.fori_loop(0, 2, tile, 0)
        c_far_up[i].start()
        c_far_down[i].start()

    @staged
    def start_direct(i):
        c_up_low[i].start()
        c_down_top[i].start()

    @staged
    def pass_far(i):
        c_far_up[i].wait_recv()
        up[i, top] = (up_own[i] + up_far[i].astype(F32)).astype(BF16)
        c_up_top[i].start()
        c_far_down[i].wait_recv()
        down[i, low] = (down_own[i] + down_far[i].astype(F32)).astype(BF16)
        c_down_low[i].start()

    @staged
    def mix(i):
        m, h = divmod(i, H)
        for item in (c_up_low[i], c_down_top[i], c_up_top[i], c_down_low[i]):
            item.wait_recv()

        def rows_of(k, _):
            start = pl.multiple_of(k * 16, 16)
            parts = []
            for w in range(3):
                for s in range(4):
                    at_ws = (i, pl.ds(w * 64 + start, 16), slice(s * 128, (s + 1) * 128))
                    part = here[at_ws] + from_below[at_ws].astype(F32) + from_above[at_ws].astype(F32)
                    parts.append(part.reshape(2, 8, 128))
            for v in range(3):
                for t in range(4):
                    total = None
                    for w in range(3):
                        for s in range(4):
                            term = pair[((w * 3 + v) * 4 + s) * 4 + t][None] * parts[w * 4 + s]
                            total = term if total is None else total + term
                    k = v * 4 + h
                    mixed[m, pl.ds(t * 64 + start, 16), k * 128 : (k + 1) * 128] = total.reshape(
                        16, 128
                    ).astype(BF16)
            return 0

        lax.fori_loop(0, 4, rows_of, 0)

    pieces = [pl.ds(c * 6 + 2 * k, 2) for k in range(3)]
    q_lo, q_hi = pl.ds(c * 6, 3), pl.ds(c * 6 + 3, 3)
    r_up = [copy(envs.at[0, p], envs.at[3, p], x_up) for p in pieces]
    r_down = [copy(envs.at[0, p], envs.at[1, p], x_down) for p in pieces]
    rp_below = [copy(envs.at[3, p], envs.at[3, p], partner) for p in pieces]
    rp_above = [copy(envs.at[1, p], envs.at[1, p], partner) for p in pieces]
    rf_up = copy(envs.at[3, q_lo], envs.at[2, q_lo], x_up)
    rf_down = copy(envs.at[1, q_hi], envs.at[2, q_hi], x_down)
    rp_lo = copy(envs.at[2, q_lo], envs.at[2, q_lo], partner)
    rp_hi = copy(envs.at[2, q_hi], envs.at[2, q_hi], partner)

    @staged
    def start_envs():
        local[H].wait()
        for k in range(3):
            r_up[k].start()
            r_down[k].start()

    @staged
    def pass_envs(k):
        r_up[k].wait_recv()
        rp_below[k].start()
        r_down[k].wait_recv()
        rp_above[k].start()
        if k == 2:
            rf_up.start()
            rf_down.start()

    @staged
    def pass_far_envs():
        rf_up.wait_recv()
        rp_lo.start()
        rf_down.wait_recv()
        rp_hi.start()

    def zmod(k):
        return lax.rem(z + k, Z)

    first, second = pl.ds(0, 128), pl.ds(128, 128)
    rings = []
    for u in range(8):
        ring = {}
        ring[1] = (
            copy(image.at[u, zmod(4), first], ring_half.at[u, 0], z_up),
            copy(image.at[u, zmod(4), second], ring_half.at[u, 1], z_down),
        )
        for k in (2, 3, 4):
            ring[k] = (
                copy(image.at[u, zmod(5 - k)], ring_full.at[u, 0, k - 2], z_up),
                copy(image.at[u, zmod(3 + k)], ring_full.at[u, 1, k - 2], z_down),
            )
        rings.append(ring)

    waited = set()

    @staged
    def contract(u):
        m, i = UNITS[u]
        for item in {0: [], 1: rp_above, 3: rp_below, 2: [rp_lo, rp_hi]}[i]:
            if id(item) not in waited:
                waited.add(id(item))
                item.wait_recv()

        def tile(j, _):
            cols = pl.ds(pl.multiple_of(j * 256, 256), 256)
            value = matmul(mixed[m], envs[i, :, :, cols].reshape(1536, 256)).astype(BF16)
            image[u, j * 2] = value[:, :128]
            image[u, j * 2 + 1] = value[:, 128:]
            return 0

        lax.fori_loop(0, 4, tile, 0)
        hop(u, 1)

    def add_into(u, k, rows, term):
        image[u, k, rows] = (image[u, k, rows].astype(F32) + term.astype(F32)).astype(BF16)

    @staged
    def hop(u, k):
        for side in range(2):
            if k > 1:
                rings[u][k - 1][side].wait_recv()
                owner = zmod(5 - k) if side == 0 else zmod(3 + k)
                if k == 2:
                    add_into(u, owner, (first, second)[side], ring_half[u, side])
                else:
                    add_into(u, owner, pl.ds(0, 256), ring_full[u, side, k - 3])
            rings[u][k][side].start()

    zero = jnp.zeros((8, 128), F32)

    def folded(value):
        return jnp.sum(value.reshape(-1, 8, 128), axis=0)

    @staged
    def finish(u, sums):
        rings[u][4][0].wait_recv()
        rings[u][4][1].wait_recv()
        m, i = UNITS[u]
        h = lax.rem(x + i, X)

        def piece(s, sums):
            squares, crossed, images = sums
            rows = pl.ds(pl.multiple_of(s * 64, 64), 64)
            value = (
                image[u, z, rows].astype(F32)
                + ring_full[u, 0, 2, rows].astype(F32)
                + ring_full[u, 1, 2, rows].astype(F32)
            )
            out[h * 4 + s, pl.ds(m * 64, 64)] = value
            start = state[h * 4 + s, pl.ds(m * 64, 64)].astype(F32)
            return (
                squares + folded(start * start),
                crossed + folded(start * value),
                images + folded(value * value),
            )

        return lax.fori_loop(0, 4, piece, sums)

    @staged
    def turn(k):
        if k == 0:
            load_left.wait()
            for item in a_swap:
                item.start()
            lax.fori_loop(0, 12, transpose_own, 0)
        if k == 1:
            for item in a_swap:
                item.wait_recv()
        if k == 2:
            lax.fori_loop(0, 12, transpose_other, 0)

    state_sums = (zero, zero, zero)
    stages = {
        "own": start_own,
        "near": pass_near,
        "rest": pass_rest,
        "turn": turn,
        "blocks": get_blocks,
        "left": left_item,
        "direct": start_direct,
        "far": pass_far,
        "mix": mix,
        "envs": start_envs,
        "penvs": pass_envs,
        "fenvs": pass_far_envs,
        "con": contract,
        "hop": hop,
    }
    for line in ORDER:
        name, *numbers = line.split(".")
        numbers = [int(n) for n in numbers]
        if name == "fin":
            state_sums = finish(numbers[0], state_sums)
        else:
            stages[name](*numbers)

    @staged
    def all_sum(phase, values, slots, me, targets):
        slots[me] = values
        sends = [copy(slots.at[me], slots.at[me], target) for target in targets]
        for item in sends:
            item.start()
        for item in sends:
            item.wait_recv()
        return jnp.sum(slots[...], axis=0)

    lane = lax.broadcasted_iota(jnp.int32, (1, 128), 1)
    packed = jnp.zeros((1, 128), F32)
    for k, value in enumerate(state_sums):
        packed = jnp.where(lane == k, jnp.sum(value, keepdims=True), packed)
    packed = all_sum(0, packed, sums_z, z, z_peers)
    packed = all_sum(1, packed, sums_xy, (x * Y + y) * 2 + c, xy_peers)
    square, projection, image_square = (
        jnp.sum(jnp.where(lane == k, packed, 0.0), keepdims=True) * (1.0 / ENTRIES) for k in range(3)
    )
    norm_sq = square + EPSILON
    alpha = projection / norm_sq
    residual_sq = (image_square - 2.0 * alpha * projection + alpha * alpha * square) / norm_sq
    beta = jnp.sqrt(residual_sq + EPSILON)
    scale = 1.0 / (jnp.sqrt(norm_sq) * beta)
    coef[0] = alpha[0, 0]
    coef[1] = beta[0, 0]

    def scaled(i, _):
        out[i] = (out[i] - alpha * state[i].astype(F32)) * scale
        return 0

    with jax.named_scope("scaled"):
        lax.fori_loop(0, 16, scaled, 0)
    with jax.named_scope("drain"):
        for item in used:
            item.wait_send()


def kernel(*refs):
    pl.run_scoped(
        functools.partial(step, *refs),
        pltpu.SemaphoreType.DMA((N_SEMS,)),
        pltpu.SemaphoreType.DMA((N_SEMS,)),
        pltpu.SemaphoreType.DMA((H + 3,)),
    )


def body(state, left_env, right_env, site_one, site_two):
    vmem = pl.BlockSpec(memory_space=pltpu.VMEM)
    smem = pl.BlockSpec(memory_space=pltpu.SMEM)
    anywhere = pl.BlockSpec(memory_space=pl.ANY)
    out, coef = pl.pallas_call(
        kernel,
        out_shape=(
            jax.ShapeDtypeStruct((16, 128, 128), F32),
            jax.ShapeDtypeStruct((2,), F32),
        ),
        in_specs=[smem, smem, anywhere, anywhere, anywhere],
        out_specs=(vmem, smem),
        scratch_shapes=[
            pltpu.VMEM((16, 128, 128), BF16),
            pltpu.VMEM((12, 128, 1024), BF16),
            pltpu.VMEM((144, 8, 128), F32),
            pltpu.VMEM((4, 8, 4, 128, 128), BF16),
            pltpu.VMEM((4, 12, 128, 128), BF16),
            pltpu.VMEM((2, 768, 1024), BF16),
            pltpu.VMEM((ITEMS, 192, 512), BF16),
            pltpu.VMEM((ITEMS, 192, 512), BF16),
            pltpu.VMEM((ITEMS, 192, 512), BF16),
            pltpu.VMEM((ITEMS, 96, 512), F32),
            pltpu.VMEM((ITEMS, 96, 512), F32),
            pltpu.VMEM((ITEMS, 192, 512), F32),
            pltpu.VMEM((ITEMS, 96, 512), BF16),
            pltpu.VMEM((ITEMS, 96, 512), BF16),
            pltpu.VMEM((ITEMS, 192, 512), BF16),
            pltpu.VMEM((ITEMS, 192, 512), BF16),
            pltpu.VMEM((2, 256, 1536), BF16),
            pltpu.VMEM((4, 12, 128, 1024), BF16),
            pltpu.VMEM((8, 8, 256, 128), BF16),
            pltpu.VMEM((8, 2, 128, 128), BF16),
            pltpu.VMEM((8, 2, 3, 256, 128), BF16),
            pltpu.VMEM((8, 1, 128), F32),
            pltpu.VMEM((32, 1, 128), F32),
        ],
        compiler_params=pltpu.CompilerParams(
            collective_id=0, has_side_effects=True, vmem_limit_bytes=64_000_000
        ),
        name="lanczos",
    )(
        site_one.transpose(0, 2, 3, 1),
        site_two.transpose(0, 2, 3, 1),
        state.reshape(16, 128, 128),
        left_env.reshape(12, 128, 1024),
        right_env.reshape(12, 128, 1024),
    )
    return out.reshape(1, 4, 4, 128, 128), coef


def solution(mesh):
    torus = Mesh(
        mesh.devices.reshape(4, 2, mesh.shape["rb"], mesh.shape["wa"]), ("lb_0", "lb_1", "rb", "wa")
    )
    in_specs = (
        P("wa", None, None, LB, "rb"),
        P(None, None, LB, "wa", None),
        P(None, None, "rb", "wa", None),
        P(),
        P(),
    )
    out_specs = (P("wa", None, None, LB, "rb"), P())
    return jax.shard_map(body, mesh=torus, in_specs=in_specs, out_specs=out_specs, check_vma=False)
```

```python
import functools

import jax
import jax.numpy as jnp
from jax import lax
from jax.experimental import pallas as pl
from jax.experimental.pallas import tpu as pltpu
from jax.sharding import Mesh
from jax.sharding import PartitionSpec as P

LB = ("lb_0", "lb_1")
EPSILON = 1e-06
ENTRIES = 4.0 * 4 * 4 * 1024 * 1024
F32, BF16 = jnp.float32, jnp.bfloat16
X, Y, Z, H = 4, 4, 8, 4
N_SEMS = 240
ITEMS = 8
UNITS = tuple((m, i) for m in range(2) for i in (0, 1, 3, 2))


ORDER = (
    "own.1", "own.0", "near.1", "turn.3", "own.2", "turn.0", "near.0", "own.3", "rest.1", "turn.1", "turn.2",
    "rest.0", "blocks.1", "left.5", "near.2", "left.1", "near.3", "direct.1", "envs.0", "blocks.0", "rest.3",
    "left.4", "rest.2", "blocks.2", "far.1", "left.2", "envs.1", "blocks.3", "left.3", "left.0", "direct.0",
    "far.3", "far.0", "penvs.0", "far.2", "direct.3", "direct.2", "far.4", "mix.1", "envs.2", "left.7",
    "direct.4", "mix.3", "left.6", "mix.0", "mix.2", "far.5", "direct.7", "penvs.1", "con.0", "penvs.2",
    "hop.0.2", "mix.4", "far.7", "direct.5", "con.1", "far.6", "direct.6", "hop.0.3", "con.2", "hop.1.2",
    "mix.7", "hop.2.2", "mix.5", "hop.0.4", "hop.1.3", "mix.6", "con.4", "hop.2.3", "con.5", "hop.1.4",
    "con.6", "hop.4.2", "hop.2.4", "fenvs", "hop.5.2", "hop.6.2", "con.3", "hop.4.3", "con.7", "fin.0",
    "hop.5.3", "hop.3.2", "fin.2", "hop.7.2", "hop.6.3", "hop.5.4", "hop.3.3", "hop.7.3", "hop.6.4",
    "hop.4.4", "fin.5", "hop.3.4", "fin.1", "hop.7.4", "fin.6", "fin.4", "fin.3", "fin.7",
)


def staged(f):
    def run(*args):
        with jax.named_scope(f"{f.__name__}#" + "_".join(str(a) for a in args if isinstance(a, int))):
            return f(*args)

    return run


def matmul(a, b):
    return lax.dot_general(a, b, (((1,), (0,)), ((), ())), preferred_element_type=F32)


def step(
    one_in,
    two_in,
    state_in,
    left_in,
    right_in,
    out,
    coef,
    applied,
    one,
    two,
    state,
    left,
    pair,
    blocks,
    left_other,
    left_t,
    far,
    up,
    down,
    up_own,
    down_own,
    here,
    up_far,
    down_far,
    from_below,
    from_above,
    mixed,
    envs,
    image,
    ring_half,
    ring_full,
    sums_z,
    sums_xy,
    send_sems,
    recv_sems,
    local_sems,
):
    y, c, z, x = (lax.axis_index(a) for a in ("lb_0", "lb_1", "rb", "wa"))
    other = 1 - c

    def at(dx=0, dy=0, dz=0, core=None):
        return (
            lax.rem(y + dy, Y),
            c if core is None else core,
            lax.rem(z + dz, Z),
            lax.rem(x + dx, X),
        )

    used = []

    def copy(src, dst, device):
        k = len(used)
        used.append(
            pltpu.make_async_remote_copy(
                src_ref=src,
                dst_ref=dst,
                send_sem=send_sems.at[k],
                recv_sem=recv_sems.at[k],
                device_id=device,
                device_id_type=pl.DeviceIdType.MESH,
            )
        )
        return used[-1]

    partner = at(core=other)
    x_up, x_down = at(dx=1), at(dx=X - 1)
    y_up, y_down = at(dy=1), at(dy=Y - 1)
    z_up, z_down = at(dz=1), at(dz=Z - 1)
    z_peers = [at(dz=k) for k in range(1, Z)]
    xy_peers = [
        at(dx=i, dy=j, core=core)
        for i in range(X)
        for j in range(Y)
        for core in (c, other)
        if not (i == 0 and j == 0 and core is c)
    ]

    barrier = pltpu.get_barrier_semaphore()
    peers = [partner, x_up, x_down, y_up, y_down, z_up, z_down]
    for peer in peers:
        pl.semaphore_signal(barrier, inc=1, device_id=peer, device_id_type=pl.DeviceIdType.MESH)

    own = x * 2 + c
    load_state = pltpu.make_async_copy(state_in, state, local_sems.at[H + 1])
    load_left = pltpu.make_async_copy(left_in, left, local_sems.at[H + 2])
    load_sites = [
        pltpu.make_async_copy(one_in, one, local_sems.at[H + 3]),
        pltpu.make_async_copy(two_in, two, local_sems.at[H + 4]),
    ]
    local = [
        pltpu.make_async_copy(state_in.at[pl.ds(h * 4, 4)], blocks.at[h, own], local_sems.at[h])
        for h in range(H)
    ]
    local.append(pltpu.make_async_copy(right_in, envs.at[0], local_sems.at[H]))
    for item in load_sites + [load_state, load_left] + local:
        item.start()

    def fill_pairs():
        for w in range(3):
            for v in range(3):
                for s in range(4):
                    for t in range(4):
                        total = sum(
                            one[w, s // 2, t // 2, u] * two[u, s % 2, t % 2, v] for u in range(3)
                        )
                        k = ((w * 3 + v) * 4 + s) * 4 + t
                        pair[k] = jnp.full((8, 128), total, F32)

    with jax.named_scope("entry"):
        load_state.wait()
        pl.semaphore_wait(barrier, len(peers))

    g_below = lax.rem(x + X - 1, X) * 2 + c
    g_above = lax.rem(x + 1, X) * 2 + c
    g_far = lax.rem(x + 2, X) * 2 + c
    lo, hi = pl.ds(0, 2), pl.ds(2, 2)
    mine = [state.at[pl.ds(h * 4, 4)] for h in range(H)]

    def send_mine(h, parts, device):
        return [copy(mine[h].at[part], blocks.at[h, own, part], device) for part in parts]

    b_up = [send_mine(h, (lo, hi), x_up) for h in range(H)]
    b_down = [send_mine(h, (hi, lo), x_down) for h in range(H)]
    b_own = [copy(mine[h], blocks.at[h, own], partner) for h in range(H)]
    bf_up = [copy(blocks.at[h, g_below, lo], blocks.at[h, g_below, lo], x_up) for h in range(H)]
    bf_down = [copy(blocks.at[h, g_above, hi], blocks.at[h, g_above, hi], x_down) for h in range(H)]
    b_pass = [
        [
            copy(blocks.at[h, g_below], blocks.at[h, g_below], partner),
            copy(blocks.at[h, g_above], blocks.at[h, g_above], partner),
            copy(blocks.at[h, g_far, lo], blocks.at[h, g_far, lo], partner),
            copy(blocks.at[h, g_far, hi], blocks.at[h, g_far, hi], partner),
        ]
        for h in range(H)
    ]

    @staged
    def start_own(h):
        for pair_of in zip(b_up[h], b_down[h]):
            for item in pair_of:
                item.start()
        b_own[h].start()

    @staged
    def pass_near(h):
        b_up[h][0].wait_recv()
        bf_up[h].start()
        b_down[h][0].wait_recv()
        bf_down[h].start()

    @staged
    def pass_rest(h):
        for item in b_up[h][1:]:
            item.wait_recv()
        b_pass[h][0].start()
        for item in b_down[h][1:]:
            item.wait_recv()
        b_pass[h][1].start()

    @staged
    def get_blocks(h):
        bf_up[h].wait_recv()
        b_pass[h][2].start()
        bf_down[h].wait_recv()
        b_pass[h][3].start()
        local[h].wait()
        b_own[h].wait_recv()
        for item in b_pass[h]:
            item.wait_recv()

    a_swap = [
        copy(
            left.at[:, :, pl.ds(pl.multiple_of(k * 256 + other * 128, 128), 128)],
            left_other.at[k],
            partner,
        )
        for k in range(Y)
    ]

    def put_left(r, w, g, core, tile):
        cols = pl.ds(pl.multiple_of((g * 2 + core) * 128, 128), 128)
        rows = pl.ds(pl.multiple_of(r * 192 + w * 64, 64), 64)
        turned = tile.T
        left_t[0, rows, cols] = turned[:64]
        left_t[1, rows, cols] = turned[64:]

    def transpose_own(i, _):
        for r in range(Y):
            cols = pl.ds(pl.multiple_of(lax.rem(y + r, Y) * 256 + c * 128, 128), 128)
            put_left(r, i // 4, lax.rem(i, 4), c, left[i, :, cols])
        return 0

    def transpose_other(i, _):
        for r in range(Y):
            put_left(r, i // 4, lax.rem(i, 4), other, left_other[lax.rem(y + r, Y), i])
        return 0

    top, low = pl.ds(0, 96), pl.ds(96, 96)
    items = range(ITEMS)
    c_far_up = [copy(far.at[i, top], up_far.at[i], y_up) for i in items]
    c_far_down = [copy(far.at[i, low], down_far.at[i], y_down) for i in items]
    c_up_low = [copy(up.at[i, low], from_below.at[i, low], y_up) for i in items]
    c_down_top = [copy(down.at[i, top], from_above.at[i, top], y_down) for i in items]
    c_up_top = [copy(up.at[i, top], from_below.at[i, top], y_up) for i in items]
    c_down_low = [copy(down.at[i, low], from_above.at[i, low], y_down) for i in items]

    @staged
    def left_item(i):
        m, h = divmod(i, H)

        def tile(j, _):
            cols = pl.ds(pl.multiple_of(j * 256, 256), 256)
            b = jnp.concatenate(
                [blocks[h, :, j * 2].reshape(1024, 128), blocks[h, :, j * 2 + 1].reshape(1024, 128)],
                axis=1,
            )
            value = matmul(left_t[m], b)
            far[i, :, cols] = value[384:576].astype(BF16)
            up_own[i, :, cols] = value[192:288]
            up[i, low, cols] = value[288:384].astype(BF16)
            down[i, top, cols] = value[576:672].astype(BF16)
            down_own[i, :, cols] = value[672:768]
            here[i, :, cols] = value[:192]
            return 0

        lax.fori_loop(0, 2, tile, 0)
        c_far_up[i].start()
        c_far_down[i].start()

    @staged
    def start_direct(i):
        c_up_low[i].start()
        c_down_top[i].start()

    @staged
    def pass_far(i):
        c_far_up[i].wait_recv()
        up[i, top] = (up_own[i] + up_far[i].astype(F32)).astype(BF16)
        c_up_top[i].start()
        c_far_down[i].wait_recv()
        down[i, low] = (down_own[i] + down_far[i].astype(F32)).astype(BF16)
        c_down_low[i].start()

    @staged
    def mix(i):
        m, h = divmod(i, H)
        for item in (c_up_low[i], c_down_top[i], c_up_top[i], c_down_low[i]):
            item.wait_recv()

        def rows_of(k, _):
            start = pl.multiple_of(k * 16, 16)
            parts = []
            for w in range(3):
                for s in range(4):
                    at_ws = (i, pl.ds(w * 64 + start, 16), slice(s * 128, (s + 1) * 128))
                    part = here[at_ws] + from_below[at_ws].astype(F32) + from_above[at_ws].astype(F32)
                    parts.append(part.reshape(2, 8, 128))
            for v in range(3):
                for t in range(4):
                    total = None
                    for w in range(3):
                        for s in range(4):
                            term = pair[((w * 3 + v) * 4 + s) * 4 + t][None] * parts[w * 4 + s]
                            total = term if total is None else total + term
                    k = v * 4 + h
                    mixed[m, pl.ds(t * 64 + start, 16), k * 128 : (k + 1) * 128] = total.reshape(
                        16, 128
                    ).astype(BF16)
            return 0

        lax.fori_loop(0, 4, rows_of, 0)

    pieces = [pl.ds(c * 6 + 2 * k, 2) for k in range(3)]
    q_lo, q_hi = pl.ds(c * 6, 3), pl.ds(c * 6 + 3, 3)
    r_up = [copy(envs.at[0, p], envs.at[3, p], x_up) for p in pieces]
    r_down = [copy(envs.at[0, p], envs.at[1, p], x_down) for p in pieces]
    rp_below = [copy(envs.at[3, p], envs.at[3, p], partner) for p in pieces]
    rp_above = [copy(envs.at[1, p], envs.at[1, p], partner) for p in pieces]
    rf_up = copy(envs.at[3, q_lo], envs.at[2, q_lo], x_up)
    rf_down = copy(envs.at[1, q_hi], envs.at[2, q_hi], x_down)
    rp_lo = copy(envs.at[2, q_lo], envs.at[2, q_lo], partner)
    rp_hi = copy(envs.at[2, q_hi], envs.at[2, q_hi], partner)

    @staged
    def start_envs(k):
        if k == 0:
            local[H].wait()
        r_up[k].start()
        r_down[k].start()

    @staged
    def pass_envs(k):
        r_up[k].wait_recv()
        rp_below[k].start()
        r_down[k].wait_recv()
        rp_above[k].start()
        if k == 2:
            rf_up.start()
            rf_down.start()

    @staged
    def pass_far_envs():
        rf_up.wait_recv()
        rp_lo.start()
        rf_down.wait_recv()
        rp_hi.start()

    def zmod(k):
        return lax.rem(z + k, Z)

    first, second = pl.ds(0, 128), pl.ds(128, 128)
    rings = []
    for u in range(8):
        ring = {}
        ring[1] = (
            copy(image.at[u, zmod(4), first], ring_half.at[u, 0], z_up),
            copy(image.at[u, zmod(4), second], ring_half.at[u, 1], z_down),
        )
        for k in (2, 3, 4):
            ring[k] = (
                copy(image.at[u, zmod(5 - k)], ring_full.at[u, 0, k - 2], z_up),
                copy(image.at[u, zmod(3 + k)], ring_full.at[u, 1, k - 2], z_down),
            )
        rings.append(ring)

    waited = set()

    @staged
    def contract(u):
        m, i = UNITS[u]
        for item in {0: [], 1: rp_above, 3: rp_below, 2: [rp_lo, rp_hi]}[i]:
            if id(item) not in waited:
                waited.add(id(item))
                item.wait_recv()

        def tile(j, _):
            cols = pl.ds(pl.multiple_of(j * 256, 256), 256)
            value = matmul(mixed[m], envs[i, :, :, cols].reshape(1536, 256)).astype(BF16)
            image[u, j * 2] = value[:, :128]
            image[u, j * 2 + 1] = value[:, 128:]
            return 0

        lax.fori_loop(0, 4, tile, 0)
        hop(u, 1)

    def add_into(u, k, rows, term):
        image[u, k, rows] = (image[u, k, rows].astype(F32) + term.astype(F32)).astype(BF16)

    @staged
    def hop(u, k):
        for side in range(2):
            if k > 1:
                rings[u][k - 1][side].wait_recv()
                owner = zmod(5 - k) if side == 0 else zmod(3 + k)
                if k == 2:
                    add_into(u, owner, (first, second)[side], ring_half[u, side])
                else:
                    add_into(u, owner, pl.ds(0, 256), ring_full[u, side, k - 3])
            rings[u][k][side].start()

    zero = jnp.zeros((8, 128), F32)

    def folded(value):
        return jnp.sum(value.reshape(-1, 8, 128), axis=0)

    @staged
    def finish(u, sums):
        rings[u][4][0].wait_recv()
        rings[u][4][1].wait_recv()
        m, i = UNITS[u]
        h = lax.rem(x + i, X)

        def piece(s, sums):
            squares, crossed, images = sums
            rows = pl.ds(pl.multiple_of(s * 64, 64), 64)
            value = (
                image[u, z, rows].astype(F32)
                + ring_full[u, 0, 2, rows].astype(F32)
                + ring_full[u, 1, 2, rows].astype(F32)
            )
            applied[h * 4 + s, pl.ds(m * 64, 64)] = value
            start = state[h * 4 + s, pl.ds(m * 64, 64)].astype(F32)
            return (
                squares + folded(start * start),
                crossed + folded(start * value),
                images + folded(value * value),
            )

        sums = lax.fori_loop(0, 4, piece, sums)
        done = (pl.ds(h * 4, 4), pl.ds(m * 64, 64))
        local.append(pltpu.make_async_copy(applied.at[done], out.at[done], local_sems.at[H + 5 + u]))
        local[-1].start()
        return sums

    @staged
    def turn(k):
        if k == 0:
            load_left.wait()
            for item in a_swap:
                item.start()
            lax.fori_loop(0, 12, transpose_own, 0)
        if k == 1:
            for item in a_swap:
                item.wait_recv()
        if k == 2:
            lax.fori_loop(0, 12, transpose_other, 0)
        if k == 3:
            for item in load_sites:
                item.wait()
            fill_pairs()

    state_sums = (zero, zero, zero)
    stages = {
        "own": start_own,
        "near": pass_near,
        "rest": pass_rest,
        "turn": turn,
        "blocks": get_blocks,
        "left": left_item,
        "direct": start_direct,
        "far": pass_far,
        "mix": mix,
        "envs": start_envs,
        "penvs": pass_envs,
        "fenvs": pass_far_envs,
        "con": contract,
        "hop": hop,
    }
    for line in ORDER:
        name, *numbers = line.split(".")
        numbers = [int(n) for n in numbers]
        if name == "fin":
            state_sums = finish(numbers[0], state_sums)
        else:
            stages[name](*numbers)

    @staged
    def all_sum(phase, values, slots, me, targets):
        slots[me] = values
        sends = [copy(slots.at[me], slots.at[me], target) for target in targets]
        for item in sends:
            item.start()
        for item in sends:
            item.wait_recv()
        return jnp.sum(slots[...], axis=0)

    lane = lax.broadcasted_iota(jnp.int32, (1, 128), 1)
    packed = jnp.zeros((1, 128), F32)
    for k, value in enumerate(state_sums):
        packed = jnp.where(lane == k, jnp.sum(value, keepdims=True), packed)
    packed = all_sum(0, packed, sums_z, z, z_peers)
    packed = all_sum(1, packed, sums_xy, (x * Y + y) * 2 + c, xy_peers)
    square, projection, image_square = (
        jnp.sum(jnp.where(lane == k, packed, 0.0), keepdims=True) * (1.0 / ENTRIES) for k in range(3)
    )
    norm_sq = square + EPSILON
    alpha = projection / norm_sq
    residual_sq = (image_square - 2.0 * alpha * projection + alpha * alpha * square) / norm_sq
    beta = jnp.sqrt(residual_sq + EPSILON)
    scale = 1.0 / (jnp.sqrt(norm_sq) * beta)
    for k, value in enumerate((alpha, beta, scale)):
        coef[k] = value[0, 0]
    with jax.named_scope("drain"):
        for item in used:
            item.wait_send()
        for item in local[H + 1 :]:
            item.wait()


def kernel(*refs):
    pl.run_scoped(
        functools.partial(step, *refs),
        pltpu.SemaphoreType.DMA((N_SEMS,)),
        pltpu.SemaphoreType.DMA((N_SEMS,)),
        pltpu.SemaphoreType.DMA((H + 13,)),
    )


def normalize(applied_in, state_in, terms_in, out, coef, applied, state, result, terms, sems):
    load_terms = pltpu.make_async_copy(terms_in, terms, sems.at[0])
    load_terms.start()
    parts = [pl.ds(4 * k, 4) for k in range(4)]
    loads, stores = [], []
    for k, part in enumerate(parts):
        loads.append(pltpu.make_async_copy(applied_in.at[part], applied.at[part], sems.at[1 + k]))
        loads.append(pltpu.make_async_copy(state_in.at[part], state.at[part], sems.at[5 + k]))
        stores.append(pltpu.make_async_copy(result.at[part], out.at[part], sems.at[9 + k]))
    for item in loads:
        item.start()
    load_terms.wait()
    alpha, beta, scale = (terms[k] for k in range(3))
    coef[0] = alpha
    coef[1] = beta
    for k in range(4):
        loads[2 * k].wait()
        loads[2 * k + 1].wait()

        def rows_of(i, _):
            result[i] = (applied[i] - alpha * state[i].astype(F32)) * scale
            return 0

        lax.fori_loop(4 * k, 4 * k + 4, rows_of, 0)
        stores[k].start()
    for item in stores:
        item.wait()


def body(state, left_env, right_env, site_one, site_two):
    smem = pl.BlockSpec(memory_space=pltpu.SMEM)
    anywhere = pl.BlockSpec(memory_space=pl.ANY)
    state = state.reshape(16, 128, 128)
    applied, terms = pl.pallas_call(
        kernel,
        out_shape=(
            jax.ShapeDtypeStruct((16, 128, 128), F32),
            jax.ShapeDtypeStruct((3,), F32),
        ),
        in_specs=[anywhere] * 5,
        out_specs=(anywhere, smem),
        scratch_shapes=[
            pltpu.VMEM((16, 128, 128), F32),
            pltpu.SMEM((3, 2, 2, 3), F32),
            pltpu.SMEM((3, 2, 2, 3), F32),
            pltpu.VMEM((16, 128, 128), BF16),
            pltpu.VMEM((12, 128, 1024), BF16),
            pltpu.VMEM((144, 8, 128), F32),
            pltpu.VMEM((4, 8, 4, 128, 128), BF16),
            pltpu.VMEM((4, 12, 128, 128), BF16),
            pltpu.VMEM((2, 768, 1024), BF16),
            pltpu.VMEM((ITEMS, 192, 512), BF16),
            pltpu.VMEM((ITEMS, 192, 512), BF16),
            pltpu.VMEM((ITEMS, 192, 512), BF16),
            pltpu.VMEM((ITEMS, 96, 512), F32),
            pltpu.VMEM((ITEMS, 96, 512), F32),
            pltpu.VMEM((ITEMS, 192, 512), F32),
            pltpu.VMEM((ITEMS, 96, 512), BF16),
            pltpu.VMEM((ITEMS, 96, 512), BF16),
            pltpu.VMEM((ITEMS, 192, 512), BF16),
            pltpu.VMEM((ITEMS, 192, 512), BF16),
            pltpu.VMEM((2, 256, 1536), BF16),
            pltpu.VMEM((4, 12, 128, 1024), BF16),
            pltpu.VMEM((8, 8, 256, 128), BF16),
            pltpu.VMEM((8, 2, 128, 128), BF16),
            pltpu.VMEM((8, 2, 3, 256, 128), BF16),
            pltpu.VMEM((8, 1, 128), F32),
            pltpu.VMEM((32, 1, 128), F32),
        ],
        compiler_params=pltpu.CompilerParams(
            collective_id=0, has_side_effects=True, vmem_limit_bytes=64_000_000
        ),
        name="lanczos",
    )(
        site_one.transpose(0, 2, 3, 1),
        site_two.transpose(0, 2, 3, 1),
        state,
        left_env.reshape(12, 128, 1024),
        right_env.reshape(12, 128, 1024),
    )
    out, coef = pl.pallas_call(
        normalize,
        out_shape=(
            jax.ShapeDtypeStruct((16, 128, 128), F32),
            jax.ShapeDtypeStruct((2,), F32),
        ),
        in_specs=[anywhere] * 3,
        out_specs=(anywhere, smem),
        scratch_shapes=[
            pltpu.VMEM((16, 128, 128), F32),
            pltpu.VMEM((16, 128, 128), BF16),
            pltpu.VMEM((16, 128, 128), F32),
            pltpu.SMEM((3,), F32),
            pltpu.SemaphoreType.DMA((13,)),
        ],
        compiler_params=pltpu.CompilerParams(vmem_limit_bytes=64_000_000),
        name="normalize",
    )(applied, state, terms)
    return out.reshape(1, 4, 4, 128, 128), coef


def solution(mesh):
    torus = Mesh(
        mesh.devices.reshape(4, 2, mesh.shape["rb"], mesh.shape["wa"]), ("lb_0", "lb_1", "rb", "wa")
    )
    in_specs = (
        P("wa", None, None, LB, "rb"),
        P(None, None, LB, "wa", None),
        P(None, None, "rb", "wa", None),
        P(),
        P(),
    )
    out_specs = (P("wa", None, None, LB, "rb"), P())
    return jax.shard_map(body, mesh=torus, in_specs=in_specs, out_specs=out_specs, check_vma=False)
```

```python
import functools

import jax
import jax.numpy as jnp
from jax import lax
from jax.experimental import pallas as pl
from jax.experimental.pallas import tpu as pltpu
from jax.sharding import Mesh
from jax.sharding import PartitionSpec as P

LB = ("lb_0", "lb_1")
EPSILON = 1e-06
ENTRIES = 4.0 * 4 * 4 * 1024 * 1024
F32, BF16 = jnp.float32, jnp.bfloat16
X, Y, Z, H = 4, 4, 8, 4
N_SEMS = 300
ITEMS = 8
UNITS = tuple((m, i, p) for m in range(2) for i in (0, 1, 3, 2) for p in range(2))


ORDER = (
    "own.3", "own.0", "turn.0", "near.3", "turn.1", "turn.2", "own.1", "rest.3", "near.0", "own.2",
    "blocks.3", "near.1", "left.7", "left.3", "rest.0", "direct.7", "envs.0", "rest.1", "blocks.0", "near.2",
    "left.0", "envs.1", "envs.2", "blocks.1", "rest.2", "left.1", "direct.0", "far.0", "direct.1", "direct.3",
    "blocks.2", "left.2", "envs.3", "far.1", "direct.2", "turn.3", "far.2", "mix.0", "penvs.0", "far.3",
    "mix.1", "left.6", "left.4", "penvs.1", "left.5", "far.7", "mix.2", "penvs.2", "mix.3", "direct.4",
    "con.1", "rf.0", "direct.5", "con.0", "con.4", "hop.0.2", "con.2", "far.5", "hop.4.2", "far.4", "hop.2.2",
    "penvs.3", "mix.7", "hop.1.2", "hop.0.3", "hop.4.3", "hop.2.3", "direct.6", "con.3", "con.5", "hop.1.3",
    "hop.3.2", "far.6", "rf.1", "hop.0.4", "fenvs.0", "mix.5", "hop.5.2", "hop.1.4", "hop.4.4", "mix.4",
    "hop.2.4", "con.6", "hop.3.3", "mix.6", "con.12", "hop.5.3", "con.8", "con.14", "hop.6.2", "con.10",
    "hop.3.4", "con.11", "fin.4", "con.9", "hop.5.4", "hop.6.3", "fenvs.1", "fin.0", "con.13", "hop.8.2",
    "hop.11.2", "hop.12.2", "hop.9.2", "con.15", "hop.13.2", "fin.3", "con.7", "hop.14.2", "hop.8.3",
    "hop.15.2", "hop.7.2", "fin.2", "hop.12.3", "hop.14.3", "hop.10.2", "hop.9.3", "fin.5", "fin.1",
    "hop.11.3", "hop.6.4", "hop.13.3", "hop.15.3", "hop.7.3", "hop.14.4", "hop.10.3", "hop.11.4", "hop.9.4",
    "hop.8.4", "hop.15.4", "hop.12.4", "hop.13.4", "hop.10.4", "fin.6", "fin.9", "hop.7.4", "fin.13",
    "fin.15", "fin.14", "fin.11", "fin.12", "fin.8", "fin.7", "fin.10",
)


def staged(f):
    def run(*args):
        with jax.named_scope(f"{f.__name__}#" + "_".join(str(a) for a in args if isinstance(a, int))):
            return f(*args)

    return run


def matmul(a, b):
    return lax.dot_general(a, b, (((1,), (0,)), ((), ())), preferred_element_type=F32)


def step(
    one_in,
    two_in,
    state_in,
    left_in,
    right_in,
    out,
    coef,
    applied,
    one,
    two,
    state,
    left,
    pair,
    blocks,
    left_other,
    left_t,
    far,
    up,
    down,
    up_own,
    down_own,
    here,
    up_far,
    down_far,
    from_below,
    from_above,
    mixed,
    envs,
    image,
    ring,
    totals,
    sums_z,
    sums_xy,
    send_sems,
    recv_sems,
    local_sems,
):
    y, c, z, x = (lax.axis_index(a) for a in ("lb_0", "lb_1", "rb", "wa"))
    other = 1 - c

    def at(dx=0, dy=0, dz=0, core=None):
        return (
            lax.rem(y + dy, Y),
            c if core is None else core,
            lax.rem(z + dz, Z),
            lax.rem(x + dx, X),
        )

    used = []

    def copy(src, dst, device):
        k = len(used)
        used.append(
            pltpu.make_async_remote_copy(
                src_ref=src,
                dst_ref=dst,
                send_sem=send_sems.at[k],
                recv_sem=recv_sems.at[k],
                device_id=device,
                device_id_type=pl.DeviceIdType.MESH,
            )
        )
        return used[-1]

    partner = at(core=other)
    x_up, x_down = at(dx=1), at(dx=X - 1)
    y_up, y_down = at(dy=1), at(dy=Y - 1)
    z_up, z_down = at(dz=1), at(dz=Z - 1)
    z_peers = [at(dz=k) for k in range(1, Z)]
    xy_peers = [
        at(dx=i, dy=j, core=core)
        for i in range(X)
        for j in range(Y)
        for core in (c, other)
        if not (i == 0 and j == 0 and core is c)
    ]

    barrier = pltpu.get_barrier_semaphore()
    peers = [partner, x_up, x_down, y_up, y_down, z_up, z_down]
    for peer in peers:
        pl.semaphore_signal(barrier, inc=1, device_id=peer, device_id_type=pl.DeviceIdType.MESH)

    own = x * 2 + c
    load_state = pltpu.make_async_copy(state_in, state, local_sems.at[H + 1])
    load_left = pltpu.make_async_copy(left_in, left, local_sems.at[H + 2])
    load_sites = [
        pltpu.make_async_copy(one_in, one, local_sems.at[H + 3]),
        pltpu.make_async_copy(two_in, two, local_sems.at[H + 4]),
    ]
    local = [
        pltpu.make_async_copy(state_in.at[pl.ds(h * 4, 4)], blocks.at[h, own], local_sems.at[h])
        for h in range(H)
    ]
    load_right = [
        pltpu.make_async_copy(
            right_in.at[:, :, pl.ds(b * 128, 128)],
            envs.at[0, b % 2 * 4 + b // 2],
            local_sems.at[H + 5 + b],
        )
        for b in range(Z)
    ]
    for item in load_sites + [load_state, load_left] + local + load_right:
        item.start()

    def fill_pairs():
        for w in range(3):
            for v in range(3):
                for s in range(4):
                    for t in range(4):
                        total = sum(
                            one[w, s // 2, t // 2, u] * two[u, s % 2, t % 2, v] for u in range(3)
                        )
                        k = ((w * 3 + v) * 4 + s) * 4 + t
                        pair[k] = jnp.full((8, 128), total, F32)

    with jax.named_scope("entry"):
        load_state.wait()
        pl.semaphore_wait(barrier, len(peers))

    g_below = lax.rem(x + X - 1, X) * 2 + c
    g_above = lax.rem(x + 1, X) * 2 + c
    g_far = lax.rem(x + 2, X) * 2 + c
    lo, hi = pl.ds(0, 2), pl.ds(2, 2)
    mine = [state.at[pl.ds(h * 4, 4)] for h in range(H)]

    def send_mine(h, parts, device):
        return [copy(mine[h].at[part], blocks.at[h, own, part], device) for part in parts]

    b_up = [send_mine(h, (lo, hi), x_up) for h in range(H)]
    b_down = [send_mine(h, (hi, lo), x_down) for h in range(H)]
    b_own = [copy(mine[h], blocks.at[h, own], partner) for h in range(H)]
    bf_up = [copy(blocks.at[h, g_below, lo], blocks.at[h, g_below, lo], x_up) for h in range(H)]
    bf_down = [copy(blocks.at[h, g_above, hi], blocks.at[h, g_above, hi], x_down) for h in range(H)]
    b_pass = [
        [
            copy(blocks.at[h, g_below], blocks.at[h, g_below], partner),
            copy(blocks.at[h, g_above], blocks.at[h, g_above], partner),
            copy(blocks.at[h, g_far, lo], blocks.at[h, g_far, lo], partner),
            copy(blocks.at[h, g_far, hi], blocks.at[h, g_far, hi], partner),
        ]
        for h in range(H)
    ]

    @staged
    def start_own(h):
        for pair_of in zip(b_up[h], b_down[h]):
            for item in pair_of:
                item.start()
        b_own[h].start()

    @staged
    def pass_near(h):
        b_up[h][0].wait_recv()
        bf_up[h].start()
        b_down[h][0].wait_recv()
        bf_down[h].start()

    @staged
    def pass_rest(h):
        for item in b_up[h][1:]:
            item.wait_recv()
        b_pass[h][0].start()
        for item in b_down[h][1:]:
            item.wait_recv()
        b_pass[h][1].start()

    @staged
    def get_blocks(h):
        bf_up[h].wait_recv()
        b_pass[h][2].start()
        bf_down[h].wait_recv()
        b_pass[h][3].start()
        local[h].wait()
        b_own[h].wait_recv()
        for item in b_pass[h]:
            item.wait_recv()

    a_swap = [
        copy(
            left.at[:, :, pl.ds(pl.multiple_of(k * 256 + other * 128, 128), 128)],
            left_other.at[k],
            partner,
        )
        for k in range(Y)
    ]

    def put_left(r, w, g, core, tile):
        cols = pl.ds(pl.multiple_of((g * 2 + core) * 128, 128), 128)
        rows = pl.ds(pl.multiple_of(r * 192 + w * 64, 64), 64)
        turned = tile.T
        left_t[0, rows, cols] = turned[:64]
        left_t[1, rows, cols] = turned[64:]

    def transpose_own(i, _):
        for r in range(Y):
            cols = pl.ds(pl.multiple_of(lax.rem(y + r, Y) * 256 + c * 128, 128), 128)
            put_left(r, i // 4, lax.rem(i, 4), c, left[i, :, cols])
        return 0

    def transpose_other(i, _):
        for r in range(Y):
            put_left(r, i // 4, lax.rem(i, 4), other, left_other[lax.rem(y + r, Y), i])
        return 0

    top, low = pl.ds(0, 96), pl.ds(96, 96)
    items = range(ITEMS)
    c_far_up = [copy(far.at[i, top], up_far.at[i], y_up) for i in items]
    c_far_down = [copy(far.at[i, low], down_far.at[i], y_down) for i in items]
    c_up_low = [copy(up.at[i, low], from_below.at[i, low], y_up) for i in items]
    c_down_top = [copy(down.at[i, top], from_above.at[i, top], y_down) for i in items]
    c_up_top = [copy(up.at[i, top], from_below.at[i, top], y_up) for i in items]
    c_down_low = [copy(down.at[i, low], from_above.at[i, low], y_down) for i in items]

    @staged
    def left_item(i):
        m, h = divmod(i, H)

        def tile(j, _):
            cols = pl.ds(pl.multiple_of(j * 256, 256), 256)
            b = jnp.concatenate(
                [blocks[h, :, j * 2].reshape(1024, 128), blocks[h, :, j * 2 + 1].reshape(1024, 128)],
                axis=1,
            )
            value = matmul(left_t[m], b)
            far[i, :, cols] = value[384:576].astype(BF16)
            up_own[i, :, cols] = value[192:288]
            up[i, low, cols] = value[288:384].astype(BF16)
            down[i, top, cols] = value[576:672].astype(BF16)
            down_own[i, :, cols] = value[672:768]
            here[i, :, cols] = value[:192]
            return 0

        lax.fori_loop(0, 2, tile, 0)
        c_far_up[i].start()
        c_far_down[i].start()

    @staged
    def start_direct(i):
        c_up_low[i].start()
        c_down_top[i].start()

    @staged
    def pass_far(i):
        c_far_up[i].wait_recv()
        up[i, top] = (up_own[i] + up_far[i].astype(F32)).astype(BF16)
        c_up_top[i].start()
        c_far_down[i].wait_recv()
        down[i, low] = (down_own[i] + down_far[i].astype(F32)).astype(BF16)
        c_down_low[i].start()

    @staged
    def mix(i):
        m, h = divmod(i, H)
        for item in (c_up_low[i], c_down_top[i], c_up_top[i], c_down_low[i]):
            item.wait_recv()

        def rows_of(k, _):
            start = pl.multiple_of(k * 16, 16)
            parts = []
            for w in range(3):
                for s in range(4):
                    at_ws = (i, pl.ds(w * 64 + start, 16), slice(s * 128, (s + 1) * 128))
                    part = here[at_ws] + from_below[at_ws].astype(F32) + from_above[at_ws].astype(F32)
                    parts.append(part.reshape(2, 8, 128))
            for v in range(3):
                for t in range(4):
                    total = None
                    for w in range(3):
                        for s in range(4):
                            term = pair[((w * 3 + v) * 4 + s) * 4 + t][None] * parts[w * 4 + s]
                            total = term if total is None else total + term
                    k = v * 4 + h
                    mixed[m, pl.ds(t * 64 + start, 16), k * 128 : (k + 1) * 128] = total.reshape(
                        16, 128
                    ).astype(BF16)
            return 0

        lax.fori_loop(0, 4, rows_of, 0)

    half = pl.ds(c * 6, 6)
    q_lo, q_hi = pl.ds(c * 6, 3), pl.ds(c * 6 + 3, 3)
    pieces = [(pl.ds(2 * k, 2), half) for k in range(4)]
    r_up = [copy(envs.at[0, *q], envs.at[3, *q], x_up) for q in pieces]
    r_down = [copy(envs.at[0, *q], envs.at[1, *q], x_down) for q in pieces]
    rp_below = [copy(envs.at[3, *q], envs.at[3, *q], partner) for q in pieces]
    rp_above = [copy(envs.at[1, *q], envs.at[1, *q], partner) for q in pieces]
    group = [pl.ds(4 * p, 4) for p in range(2)]
    rf_up = [copy(envs.at[3, g, q_lo], envs.at[2, g, q_lo], x_up) for g in group]
    rf_down = [copy(envs.at[1, g, q_hi], envs.at[2, g, q_hi], x_down) for g in group]
    rp_lo = [copy(envs.at[2, g, q_lo], envs.at[2, g, q_lo], partner) for g in group]
    rp_hi = [copy(envs.at[2, g, q_hi], envs.at[2, g, q_hi], partner) for g in group]

    @staged
    def start_envs(k):
        if k == 0:
            for item in load_right:
                item.wait()
        r_up[k].start()
        r_down[k].start()

    @staged
    def pass_envs(k):
        r_up[k].wait_recv()
        rp_below[k].start()
        r_down[k].wait_recv()
        rp_above[k].start()

    @staged
    def start_far_envs(p):
        rf_up[p].start()
        rf_down[p].start()

    @staged
    def pass_far_envs(p):
        rf_up[p].wait_recv()
        rp_lo[p].start()
        rf_down[p].wait_recv()
        rp_hi[p].start()

    def zmod(k):
        return lax.rem(z + k, Z)

    parity = lax.rem(z, 2)

    def has_role(p, hop):
        return parity == (p if hop % 2 == 1 else 1 - p)

    first, second, every = pl.ds(0, 128), pl.ds(128, 128), pl.ds(0, 256)
    places = {1: None, 2: 0, 3: 0, 4: 1}
    hops = []
    for u in range(len(UNITS)):
        sends = {}
        sends[1] = (
            copy(image.at[u, zmod(4) // 2, first], ring.at[u, 0, 1, first], z_up),
            copy(image.at[u, zmod(4) // 2, second], ring.at[u, 1, 1, first], z_down),
        )
        for k in (2, 3, 4):
            sends[k] = (
                copy(image.at[u, zmod(5 - k) // 2], ring.at[u, 0, places[k]], z_up),
                copy(image.at[u, zmod(3 + k) // 2], ring.at[u, 1, places[k]], z_down),
            )
        hops.append(sends)
    hop_copies = {id(item) for sends in hops for k in sends for item in sends[k]}

    waited = set()

    @staged
    def contract(u):
        m, i, p = UNITS[u]
        needed = {
            0: [],
            1: rp_above[2 * p : 2 * p + 2],
            3: rp_below[2 * p : 2 * p + 2],
            2: [rp_lo[p], rp_hi[p]],
        }[i]
        for item in needed:
            if id(item) not in waited:
                waited.add(id(item))
                item.wait_recv()

        def tile(j, _):
            b = jnp.concatenate(
                [envs[i, p * 4 + j * 2 + k].reshape(1536, 128) for k in range(2)], axis=1
            )
            value = matmul(mixed[m], b).astype(BF16)
            image[u, j * 2] = value[:, :128]
            image[u, j * 2 + 1] = value[:, 128:]
            return 0

        lax.fori_loop(0, 2, tile, 0)

        @pl.when(has_role(p, 1))
        def _():
            for item in hops[u][1]:
                item.start()

    @staged
    def hop(u, k):
        @pl.when(has_role(UNITS[u][2], k))
        def _():
            for side in range(2):
                hops[u][k - 1][side].wait_recv()
                e = (zmod(5 - k) if side == 0 else zmod(3 + k)) // 2
                if k == 2:
                    rows, term = (first, second)[side], ring[u, side, 1, first]
                else:
                    rows, term = every, ring[u, side, places[k - 1]]
                image[u, e, rows] = (image[u, e, rows].astype(F32) + term.astype(F32)).astype(BF16)
                hops[u][k][side].start()

    def folded(value):
        return jnp.sum(value.reshape(-1, 8, 128), axis=0)

    stores = []

    @staged
    def finish(u):
        m, i, p = UNITS[u]
        h = lax.rem(x + i, X)
        done = (pl.ds(h * 4, 4), pl.ds(m * 64, 64))
        stores.append(
            (p, pltpu.make_async_copy(applied.at[done], out.at[done], local_sems.at[H + 13 + u]))
        )

        @pl.when(has_role(p, 1))
        def _():
            for side in range(2):
                hops[u][4][side].wait_recv()

            def piece(s, sums):
                squares, crossed, images = sums
                rows = pl.ds(pl.multiple_of(s * 64, 64), 64)
                value = (
                    image[u, z // 2, rows].astype(F32)
                    + ring[u, 0, 1, rows].astype(F32)
                    + ring[u, 1, 1, rows].astype(F32)
                )
                applied[h * 4 + s, pl.ds(m * 64, 64)] = value
                start = state[h * 4 + s, pl.ds(m * 64, 64)].astype(F32)
                return (
                    squares + folded(start * start),
                    crossed + folded(start * value),
                    images + folded(value * value),
                )

            sums = lax.fori_loop(0, 4, piece, (totals[0], totals[1], totals[2]))
            for k in range(3):
                totals[k] = sums[k]
            stores[-1][1].start()

    @staged
    def turn(k):
        if k == 0:
            load_left.wait()
            for item in a_swap:
                item.start()
            lax.fori_loop(0, 12, transpose_own, 0)
        if k == 1:
            for item in a_swap:
                item.wait_recv()
        if k == 2:
            lax.fori_loop(0, 12, transpose_other, 0)
        if k == 3:
            for item in load_sites:
                item.wait()
            fill_pairs()

    totals[...] = jnp.zeros((3, 8, 128), F32)
    stages = {
        "own": start_own,
        "near": pass_near,
        "rest": pass_rest,
        "turn": turn,
        "blocks": get_blocks,
        "left": left_item,
        "direct": start_direct,
        "far": pass_far,
        "mix": mix,
        "envs": start_envs,
        "penvs": pass_envs,
        "rf": start_far_envs,
        "fenvs": pass_far_envs,
        "fin": finish,
        "con": contract,
        "hop": hop,
    }
    for line in ORDER:
        name, *numbers = line.split(".")
        numbers = [int(n) for n in numbers]
        stages[name](*numbers)

    @staged
    def all_sum(phase, values, slots, me, targets):
        slots[me] = values
        sends = [copy(slots.at[me], slots.at[me], target) for target in targets]
        for item in sends:
            item.start()
        for item in sends:
            item.wait_recv()
        return jnp.sum(slots[...], axis=0)

    lane = lax.broadcasted_iota(jnp.int32, (1, 128), 1)
    packed = jnp.zeros((1, 128), F32)
    for k in range(3):
        packed = jnp.where(lane == k, jnp.sum(totals[k], keepdims=True), packed)
    packed = all_sum(0, packed, sums_z, z, z_peers)
    packed = all_sum(1, packed, sums_xy, (x * Y + y) * 2 + c, xy_peers)
    square, projection, image_square = (
        jnp.sum(jnp.where(lane == k, packed, 0.0), keepdims=True) * (1.0 / ENTRIES) for k in range(3)
    )
    norm_sq = square + EPSILON
    alpha = projection / norm_sq
    residual_sq = (image_square - 2.0 * alpha * projection + alpha * alpha * square) / norm_sq
    beta = jnp.sqrt(residual_sq + EPSILON)
    scale = 1.0 / (jnp.sqrt(norm_sq) * beta)
    for k, value in enumerate((alpha, beta, scale)):
        coef[k] = value[0, 0]
    with jax.named_scope("drain"):
        for item in used:
            if id(item) not in hop_copies:
                item.wait_send()
        for p in range(2):

            @pl.when(has_role(p, 1))
            def _():
                for (_, _, q), sends in zip(UNITS, hops):
                    for k in (1, 3) if q == p else (2, 4):
                        for item in sends[k]:
                            item.wait_send()
                for q, item in stores:
                    if q == p:
                        item.wait()


def kernel(*refs):
    pl.run_scoped(
        functools.partial(step, *refs),
        pltpu.SemaphoreType.DMA((N_SEMS,)),
        pltpu.SemaphoreType.DMA((N_SEMS,)),
        pltpu.SemaphoreType.DMA((H + 29,)),
    )


def normalize(applied_in, state_in, terms_in, out, coef, applied, state, result, terms, sems):
    load_terms = pltpu.make_async_copy(terms_in, terms, sems.at[0])
    load_terms.start()
    parts = [pl.ds(4 * k, 4) for k in range(4)]
    loads, stores = [], []
    for k, part in enumerate(parts):
        loads.append(pltpu.make_async_copy(applied_in.at[part], applied.at[part], sems.at[1 + k]))
        loads.append(pltpu.make_async_copy(state_in.at[part], state.at[part], sems.at[5 + k]))
        stores.append(pltpu.make_async_copy(result.at[part], out.at[part], sems.at[9 + k]))
    for item in loads:
        item.start()
    load_terms.wait()
    alpha, beta, scale = (terms[k] for k in range(3))
    coef[0] = alpha
    coef[1] = beta
    for k in range(4):
        loads[2 * k].wait()
        loads[2 * k + 1].wait()

        def rows_of(i, _):
            result[i] = (applied[i] - alpha * state[i].astype(F32)) * scale
            return 0

        lax.fori_loop(4 * k, 4 * k + 4, rows_of, 0)
        stores[k].start()
    for item in stores:
        item.wait()


def body(state, left_env, right_env, site_one, site_two):
    smem = pl.BlockSpec(memory_space=pltpu.SMEM)
    anywhere = pl.BlockSpec(memory_space=pl.ANY)
    state = state.reshape(16, 128, 128)
    applied, terms = pl.pallas_call(
        kernel,
        out_shape=(
            jax.ShapeDtypeStruct((16, 128, 128), F32),
            jax.ShapeDtypeStruct((3,), F32),
        ),
        in_specs=[anywhere] * 5,
        out_specs=(anywhere, smem),
        scratch_shapes=[
            pltpu.VMEM((16, 128, 128), F32),
            pltpu.SMEM((3, 2, 2, 3), F32),
            pltpu.SMEM((3, 2, 2, 3), F32),
            pltpu.VMEM((16, 128, 128), BF16),
            pltpu.VMEM((12, 128, 1024), BF16),
            pltpu.VMEM((144, 8, 128), F32),
            pltpu.VMEM((4, 8, 4, 128, 128), BF16),
            pltpu.VMEM((4, 12, 128, 128), BF16),
            pltpu.VMEM((2, 768, 1024), BF16),
            pltpu.VMEM((ITEMS, 192, 512), BF16),
            pltpu.VMEM((ITEMS, 192, 512), BF16),
            pltpu.VMEM((ITEMS, 192, 512), BF16),
            pltpu.VMEM((ITEMS, 96, 512), F32),
            pltpu.VMEM((ITEMS, 96, 512), F32),
            pltpu.VMEM((ITEMS, 192, 512), F32),
            pltpu.VMEM((ITEMS, 96, 512), BF16),
            pltpu.VMEM((ITEMS, 96, 512), BF16),
            pltpu.VMEM((ITEMS, 192, 512), BF16),
            pltpu.VMEM((ITEMS, 192, 512), BF16),
            pltpu.VMEM((2, 256, 1536), BF16),
            pltpu.VMEM((4, 8, 12, 128, 128), BF16),
            pltpu.VMEM((16, 4, 256, 128), BF16),
            pltpu.VMEM((16, 2, 2, 256, 128), BF16),
            pltpu.VMEM((3, 8, 128), F32),
            pltpu.VMEM((8, 1, 128), F32),
            pltpu.VMEM((32, 1, 128), F32),
        ],
        compiler_params=pltpu.CompilerParams(
            collective_id=0, has_side_effects=True, vmem_limit_bytes=64_000_000
        ),
        name="lanczos",
    )(
        site_one.transpose(0, 2, 3, 1),
        site_two.transpose(0, 2, 3, 1),
        state,
        left_env.reshape(12, 128, 1024),
        right_env.reshape(12, 128, 1024),
    )
    out, coef = pl.pallas_call(
        normalize,
        out_shape=(
            jax.ShapeDtypeStruct((16, 128, 128), F32),
            jax.ShapeDtypeStruct((2,), F32),
        ),
        in_specs=[anywhere] * 3,
        out_specs=(anywhere, smem),
        scratch_shapes=[
            pltpu.VMEM((16, 128, 128), F32),
            pltpu.VMEM((16, 128, 128), BF16),
            pltpu.VMEM((16, 128, 128), F32),
            pltpu.SMEM((3,), F32),
            pltpu.SemaphoreType.DMA((13,)),
        ],
        compiler_params=pltpu.CompilerParams(vmem_limit_bytes=64_000_000),
        name="normalize",
    )(applied, state, terms)
    return out.reshape(1, 4, 4, 128, 128), coef


def solution(mesh):
    torus = Mesh(
        mesh.devices.reshape(4, 2, mesh.shape["rb"], mesh.shape["wa"]), ("lb_0", "lb_1", "rb", "wa")
    )
    in_specs = (
        P("wa", None, None, LB, "rb"),
        P(None, None, LB, "wa", None),
        P(None, None, "rb", "wa", None),
        P(),
        P(),
    )
    out_specs = (P("wa", None, None, LB, "rb"), P())
    return jax.shard_map(body, mesh=torus, in_specs=in_specs, out_specs=out_specs, check_vma=False)
```

```python
import functools

import jax
import jax.numpy as jnp
from jax import lax
from jax.experimental import pallas as pl
from jax.experimental.pallas import tpu as pltpu
from jax.sharding import Mesh
from jax.sharding import PartitionSpec as P

LB = ("lb_0", "lb_1")
EPSILON = 1e-06
ENTRIES = 4.0 * 4 * 4 * 1024 * 1024
F32, BF16 = jnp.float32, jnp.bfloat16
X, Y, Z, H = 4, 4, 8, 4
N_SEMS = 440
ROWS = (64, 32, 32)
STARTS = tuple(sum(ROWS[:m]) for m in range(len(ROWS)))
TOPS = tuple((3 * r // 16 + (m + 1) % 2) // 2 * 16 for m, r in enumerate(ROWS))
TOP_STARTS = tuple(sum(TOPS[:m]) for m in range(len(ROWS)))
TOP_ROWS = sum(TOPS)
ITEMS = 4 * len(ROWS)
UNITS = tuple((m, i, p) for m in range(len(ROWS)) for i in (0, 1, 3, 2) for p in range(2))


OWN, TURN, NEAR, REST, BLOCKS, LEFT, DIRECT, FAR, MIX, ENVS, PENVS, RF, FENVS, CON, HOP, FIN = range(16)
ORDER = (
    (OWN, 1), (TURN, 0), (OWN, 3), (NEAR, 1), (TURN, 1), (OWN, 0), (TURN, 2), (REST, 1), (TURN, 3), (OWN, 2),
    (NEAR, 3), (BLOCKS, 1), (LEFT, 1), (LEFT, 9), (DIRECT, 1), (NEAR, 0), (REST, 3), (NEAR, 2), (REST, 2),
    (ENVS, 0), (ENVS, 1), (FAR, 1), (REST, 0), (ENVS, 2), (BLOCKS, 3), (DIRECT, 9), (LEFT, 3), (DIRECT, 3),
    (BLOCKS, 2), (LEFT, 2), (DIRECT, 2), (BLOCKS, 0), (LEFT, 0), (DIRECT, 0), (PENVS, 0), (FAR, 2), (FAR, 3),
    (MIX, 1), (FAR, 0), (ENVS, 3), (PENVS, 1), (LEFT, 8), (RF, 0), (LEFT, 11), (MIX, 2), (LEFT, 10),
    (DIRECT, 8), (MIX, 3), (MIX, 0), (FAR, 9), (CON, 0), (FAR, 8), (CON, 1), (DIRECT, 11), (CON, 2), (CON, 4),
    (FAR, 11), (HOP, 0, 2), (DIRECT, 10), (HOP, 1, 2), (FAR, 10), (MIX, 9), (LEFT, 6), (LEFT, 7), (MIX, 8),
    (LEFT, 5), (HOP, 4, 2), (PENVS, 2), (DIRECT, 6), (LEFT, 4), (MIX, 11), (HOP, 2, 2), (PENVS, 3),
    (HOP, 1, 3), (HOP, 0, 3), (MIX, 10), (CON, 16), (DIRECT, 5), (CON, 20), (CON, 18), (HOP, 4, 3), (FAR, 6),
    (RF, 1), (CON, 17), (CON, 5), (HOP, 2, 3), (CON, 19), (CON, 21), (HOP, 16, 2), (FAR, 5), (HOP, 1, 4),
    (DIRECT, 4), (CON, 3), (HOP, 18, 2), (HOP, 20, 2), (FAR, 4), (FAR, 7), (HOP, 2, 4), (HOP, 17, 2),
    (HOP, 5, 2), (HOP, 19, 2), (HOP, 0, 4), (HOP, 21, 2), (DIRECT, 7), (FENVS, 0), (HOP, 3, 2), (MIX, 5),
    (HOP, 4, 4), (MIX, 6), (CON, 22), (MIX, 4), (HOP, 20, 3), (HOP, 17, 3), (CON, 6), (HOP, 5, 3),
    (HOP, 16, 3), (MIX, 7), (CON, 8), (CON, 13), (CON, 12), (HOP, 21, 3), (HOP, 19, 3), (CON, 10),
    (HOP, 18, 3), (HOP, 17, 4), (CON, 9), (CON, 14), (HOP, 3, 3), (HOP, 5, 4), (FENVS, 1), (HOP, 13, 2),
    (HOP, 21, 4), (CON, 11), (HOP, 9, 2), (HOP, 3, 4), (HOP, 22, 2), (HOP, 8, 2), (HOP, 12, 2), (FIN, 1),
    (CON, 7), (HOP, 11, 2), (CON, 23), (HOP, 10, 2), (HOP, 20, 4), (HOP, 22, 3), (HOP, 7, 2), (HOP, 23, 2),
    (CON, 15), (HOP, 14, 2), (HOP, 12, 3), (HOP, 6, 2), (HOP, 16, 4), (HOP, 13, 3), (FIN, 4), (HOP, 15, 2),
    (HOP, 10, 3), (HOP, 14, 3), (HOP, 6, 3), (FIN, 16), (HOP, 9, 3), (HOP, 18, 4), (HOP, 13, 4), (FIN, 2),
    (FIN, 17), (HOP, 11, 3), (FIN, 0), (HOP, 23, 3), (HOP, 9, 4), (HOP, 7, 3), (HOP, 8, 3), (HOP, 15, 3),
    (HOP, 11, 4), (HOP, 12, 4), (HOP, 23, 4), (FIN, 20), (FIN, 5), (FIN, 18), (HOP, 7, 4), (HOP, 15, 4),
    (HOP, 22, 4), (HOP, 10, 4), (HOP, 14, 4), (HOP, 6, 4), (HOP, 8, 4), (FIN, 11), (HOP, 19, 4), (FIN, 22),
    (FIN, 14), (FIN, 21), (FIN, 12), (FIN, 10), (FIN, 9), (FIN, 3), (FIN, 6), (FIN, 23), (FIN, 7), (FIN, 8),
    (FIN, 19), (FIN, 13), (FIN, 15),
)


def staged(f):
    def run(*args):
        with jax.named_scope(f"{f.__name__}#" + "_".join(str(a) for a in args if isinstance(a, int))):
            return f(*args)

    return run


def matmul(a, b):
    return lax.dot_general(a, b, (((1,), (0,)), ((), ())), preferred_element_type=F32)


def step(
    one_in,
    two_in,
    state_in,
    left_in,
    right_in,
    out,
    coef,
    applied,
    one,
    two,
    state,
    left,
    pair,
    blocks,
    left_other,
    left_t,
    far,
    up,
    down,
    up_own,
    down_own,
    here,
    up_far,
    down_far,
    from_below,
    from_above,
    mixed,
    envs,
    image,
    ring,
    totals,
    sums_z,
    sums_xy,
    send_sems,
    recv_sems,
    local_sems,
):
    y, c, z, x = (lax.axis_index(a) for a in ("lb_0", "lb_1", "rb", "wa"))
    other = 1 - c

    def at(dx=0, dy=0, dz=0, core=None):
        return (
            lax.rem(y + dy, Y),
            c if core is None else core,
            lax.rem(z + dz, Z),
            lax.rem(x + dx, X),
        )

    used = []

    def copy(src, dst, device):
        k = len(used)
        used.append(
            pltpu.make_async_remote_copy(
                src_ref=src,
                dst_ref=dst,
                send_sem=send_sems.at[k],
                recv_sem=recv_sems.at[k],
                device_id=device,
                device_id_type=pl.DeviceIdType.MESH,
            )
        )
        return used[-1]

    partner = at(core=other)
    x_up, x_down = at(dx=1), at(dx=X - 1)
    y_up, y_down = at(dy=1), at(dy=Y - 1)
    z_up, z_down = at(dz=1), at(dz=Z - 1)
    z_peers = [at(dz=k) for k in range(1, Z)]
    xy_peers = [
        at(dx=i, dy=j, core=core)
        for i in range(X)
        for j in range(Y)
        for core in (c, other)
        if not (i == 0 and j == 0 and core is c)
    ]

    barrier = pltpu.get_barrier_semaphore()
    peers = [partner, x_up, x_down, y_up, y_down, z_up, z_down]
    for peer in peers:
        pl.semaphore_signal(barrier, inc=1, device_id=peer, device_id_type=pl.DeviceIdType.MESH)

    own = x * 2 + c
    load_state = pltpu.make_async_copy(state_in, state, local_sems.at[H + 1])
    load_left = pltpu.make_async_copy(left_in, left, local_sems.at[H + 2])
    load_sites = [
        pltpu.make_async_copy(one_in, one, local_sems.at[H + 3]),
        pltpu.make_async_copy(two_in, two, local_sems.at[H + 4]),
    ]
    local = [
        pltpu.make_async_copy(state_in.at[pl.ds(h * 4, 4)], blocks.at[h, own], local_sems.at[h])
        for h in range(H)
    ]
    load_right = [
        pltpu.make_async_copy(
            right_in.at[:, :, pl.ds(b * 128, 128)],
            envs.at[0, b % 2 * 4 + b // 2],
            local_sems.at[H + 5 + b],
        )
        for b in range(Z)
    ]
    for item in load_sites + [load_state, load_left] + local + load_right:
        item.start()

    def fill_pairs():
        for w in range(3):
            for v in range(3):
                for s in range(4):
                    for t in range(4):
                        total = sum(
                            one[w, s // 2, t // 2, u] * two[u, s % 2, t % 2, v] for u in range(3)
                        )
                        k = ((w * 3 + v) * 4 + s) * 4 + t
                        pair[k] = jnp.full((8, 128), total, F32)

    with jax.named_scope("entry"):
        load_state.wait()
        pl.semaphore_wait(barrier, len(peers))

    g_below = lax.rem(x + X - 1, X) * 2 + c
    g_above = lax.rem(x + 1, X) * 2 + c
    g_far = lax.rem(x + 2, X) * 2 + c
    lo, hi = pl.ds(0, 2), pl.ds(2, 2)
    mine = [state.at[pl.ds(h * 4, 4)] for h in range(H)]

    def send_mine(h, parts, device):
        return [copy(mine[h].at[part], blocks.at[h, own, part], device) for part in parts]

    b_up = [send_mine(h, (lo, hi), x_up) for h in range(H)]
    b_down = [send_mine(h, (hi, lo), x_down) for h in range(H)]
    b_own = [copy(mine[h], blocks.at[h, own], partner) for h in range(H)]
    bf_up = [copy(blocks.at[h, g_below, lo], blocks.at[h, g_below, lo], x_up) for h in range(H)]
    bf_down = [copy(blocks.at[h, g_above, hi], blocks.at[h, g_above, hi], x_down) for h in range(H)]
    b_pass = [
        [
            copy(blocks.at[h, g_below], blocks.at[h, g_below], partner),
            copy(blocks.at[h, g_above], blocks.at[h, g_above], partner),
            copy(blocks.at[h, g_far, lo], blocks.at[h, g_far, lo], partner),
            copy(blocks.at[h, g_far, hi], blocks.at[h, g_far, hi], partner),
        ]
        for h in range(H)
    ]

    @staged
    def start_own(h):
        for pair_of in zip(b_up[h], b_down[h]):
            for item in pair_of:
                item.start()
        b_own[h].start()

    @staged
    def pass_near(h):
        b_up[h][0].wait_recv()
        bf_up[h].start()
        b_down[h][0].wait_recv()
        bf_down[h].start()

    @staged
    def pass_rest(h):
        for item in b_up[h][1:]:
            item.wait_recv()
        b_pass[h][0].start()
        for item in b_down[h][1:]:
            item.wait_recv()
        b_pass[h][1].start()

    @staged
    def get_blocks(h):
        bf_up[h].wait_recv()
        b_pass[h][2].start()
        bf_down[h].wait_recv()
        b_pass[h][3].start()
        local[h].wait()
        b_own[h].wait_recv()
        for item in b_pass[h]:
            item.wait_recv()

    a_swap = [
        copy(
            left.at[:, :, pl.ds(pl.multiple_of(k * 256 + other * 128, 128), 128)],
            left_other.at[k],
            partner,
        )
        for k in range(Y)
    ]

    def put_left(r, w, g, core, tile):
        cols = pl.ds(pl.multiple_of((g * 2 + core) * 128, 128), 128)
        turned = tile.T
        for start, count in zip(STARTS, ROWS):
            row = pl.multiple_of(12 * start + 3 * r * count + w * count, 16)
            left_t[pl.ds(row, count), cols] = turned[start : start + count]

    def transpose_own(i, _):
        for r in range(Y):
            cols = pl.ds(pl.multiple_of(lax.rem(y + r, Y) * 256 + c * 128, 128), 128)
            put_left(r, i // 4, lax.rem(i, 4), c, left[i, :, cols])
        return 0

    def transpose_other(i, _):
        for r in range(Y):
            put_left(r, i // 4, lax.rem(i, 4), other, left_other[lax.rem(y + r, Y), i])
        return 0

    items = [divmod(i, H) for i in range(ITEMS)]
    full = [pl.ds(3 * start, 3 * count) for start, count in zip(STARTS, ROWS)]
    top = [pl.ds(3 * start, size) for start, size in zip(STARTS, TOPS)]
    low = [
        pl.ds(3 * start + size, 3 * count - size) for start, size, count in zip(STARTS, TOPS, ROWS)
    ]
    top_own = [pl.ds(start, size) for start, size in zip(TOP_STARTS, TOPS)]
    low_own = [
        pl.ds(3 * start - before, 3 * count - size)
        for start, before, size, count in zip(STARTS, TOP_STARTS, TOPS, ROWS)
    ]
    c_far_up = [copy(far.at[h, top[m]], up_far.at[h, top_own[m]], y_up) for m, h in items]
    c_far_down = [copy(far.at[h, low[m]], down_far.at[h, low_own[m]], y_down) for m, h in items]
    c_up_low = [copy(up.at[h, low[m]], from_below.at[h, low[m]], y_up) for m, h in items]
    c_down_top = [copy(down.at[h, top[m]], from_above.at[h, top[m]], y_down) for m, h in items]
    c_up_top = [copy(up.at[h, top[m]], from_below.at[h, top[m]], y_up) for m, h in items]
    c_down_low = [copy(down.at[h, low[m]], from_above.at[h, low[m]], y_down) for m, h in items]

    @staged
    def left_item(i):
        m, h = items[i]
        n, size = 3 * ROWS[m], TOPS[m]

        def tile(j, _):
            cols = pl.ds(pl.multiple_of(j * 256, 256), 256)
            b = jnp.concatenate(
                [blocks[h, :, j * 2].reshape(1024, 128), blocks[h, :, j * 2 + 1].reshape(1024, 128)],
                axis=1,
            )
            value = matmul(left_t[pl.ds(12 * STARTS[m], 4 * n)], b)
            here[h, full[m], cols] = value[:n]
            up_own[h, top_own[m], cols] = value[n : n + size]
            up[h, low[m], cols] = value[n + size : 2 * n].astype(BF16)
            far[h, full[m], cols] = value[2 * n : 3 * n].astype(BF16)
            down[h, top[m], cols] = value[3 * n : 3 * n + size].astype(BF16)
            down_own[h, low_own[m], cols] = value[3 * n + size :]
            return 0

        lax.fori_loop(0, 2, tile, 0)
        c_far_up[i].start()
        c_far_down[i].start()

    @staged
    def start_direct(i):
        c_up_low[i].start()
        c_down_top[i].start()

    @staged
    def pass_far(i):
        m, h = items[i]
        mine_up, mine_down = (h, top_own[m]), (h, low_own[m])
        c_far_up[i].wait_recv()
        up[h, top[m]] = (up_own[mine_up] + up_far[mine_up].astype(F32)).astype(BF16)
        c_up_top[i].start()
        c_far_down[i].wait_recv()
        down[h, low[m]] = (down_own[mine_down] + down_far[mine_down].astype(F32)).astype(BF16)
        c_down_low[i].start()

    @staged
    def mix(i):
        m, h = items[i]
        for item in (c_up_low[i], c_down_top[i], c_up_top[i], c_down_low[i]):
            item.wait_recv()

        def rows_of(k, _):
            start = pl.multiple_of(k * 16, 16)
            parts = []
            for w in range(3):
                for s in range(4):
                    row = 3 * STARTS[m] + w * ROWS[m] + start
                    at_ws = (h, pl.ds(row, 16), slice(s * 128, (s + 1) * 128))
                    part = here[at_ws] + from_below[at_ws].astype(F32) + from_above[at_ws].astype(F32)
                    parts.append(part.reshape(2, 8, 128))
            for v in range(3):
                for t in range(4):
                    total = None
                    for w in range(3):
                        for s in range(4):
                            term = pair[((w * 3 + v) * 4 + s) * 4 + t][None] * parts[w * 4 + s]
                            total = term if total is None else total + term
                    k = v * 4 + h
                    row = 4 * STARTS[m] + t * ROWS[m] + start
                    mixed[pl.ds(row, 16), k * 128 : (k + 1) * 128] = total.reshape(16, 128).astype(BF16)
            return 0

        lax.fori_loop(0, ROWS[m] // 16, rows_of, 0)

    half = pl.ds(c * 6, 6)
    q_lo, q_hi = pl.ds(c * 6, 3), pl.ds(c * 6 + 3, 3)
    pieces = [(pl.ds(2 * k, 2), half) for k in range(4)]
    r_up = [copy(envs.at[0, *q], envs.at[3, *q], x_up) for q in pieces]
    r_down = [copy(envs.at[0, *q], envs.at[1, *q], x_down) for q in pieces]
    rp_below = [copy(envs.at[3, *q], envs.at[3, *q], partner) for q in pieces]
    rp_above = [copy(envs.at[1, *q], envs.at[1, *q], partner) for q in pieces]
    group = [pl.ds(4 * p, 4) for p in range(2)]
    rf_up = [copy(envs.at[3, g, q_lo], envs.at[2, g, q_lo], x_up) for g in group]
    rf_down = [copy(envs.at[1, g, q_hi], envs.at[2, g, q_hi], x_down) for g in group]
    rp_lo = [copy(envs.at[2, g, q_lo], envs.at[2, g, q_lo], partner) for g in group]
    rp_hi = [copy(envs.at[2, g, q_hi], envs.at[2, g, q_hi], partner) for g in group]

    @staged
    def start_envs(k):
        if k == 0:
            for item in load_right:
                item.wait()
        r_up[k].start()
        r_down[k].start()

    @staged
    def pass_envs(k):
        r_up[k].wait_recv()
        rp_below[k].start()
        r_down[k].wait_recv()
        rp_above[k].start()

    @staged
    def start_far_envs(p):
        rf_up[p].start()
        rf_down[p].start()

    @staged
    def pass_far_envs(p):
        rf_up[p].wait_recv()
        rp_lo[p].start()
        rf_down[p].wait_recv()
        rp_hi[p].start()

    def zmod(k):
        return lax.rem(z + k, Z)

    parity = lax.rem(z, 2)

    def has_role(p, hop):
        return parity == (p if hop % 2 == 1 else 1 - p)

    first = [pl.ds(4 * start, 2 * count) for start, count in zip(STARTS, ROWS)]
    second = [pl.ds(4 * start + 2 * count, 2 * count) for start, count in zip(STARTS, ROWS)]
    every = [pl.ds(4 * start, 4 * count) for start, count in zip(STARTS, ROWS)]
    places = {1: None, 2: 0, 3: 0, 4: 1}
    hops = []
    for u in range(len(UNITS)):
        m, v = UNITS[u][0], u % 8
        sends = {}
        sends[1] = (
            copy(image.at[v, zmod(4) // 2, first[m]], ring.at[v, 0, 1, first[m]], z_up),
            copy(image.at[v, zmod(4) // 2, second[m]], ring.at[v, 1, 1, first[m]], z_down),
        )
        for k in (2, 3, 4):
            sends[k] = tuple(
                copy(
                    image.at[v, zmod(owner) // 2, every[m]],
                    ring.at[v, side, places[k], every[m]],
                    device,
                )
                for side, owner, device in ((0, 5 - k, z_up), (1, 3 + k, z_down))
            )
        hops.append(sends)
    hop_copies = {id(item) for sends in hops for k in sends for item in sends[k]}

    waited = set()

    @staged
    def contract(u):
        m, i, p = UNITS[u]
        needed = {
            0: [],
            1: rp_above[2 * p : 2 * p + 2],
            3: rp_below[2 * p : 2 * p + 2],
            2: [rp_lo[p], rp_hi[p]],
        }[i]
        for item in needed:
            if id(item) not in waited:
                waited.add(id(item))
                item.wait_recv()

        def tile(j, _):
            b = jnp.concatenate(
                [envs[i, p * 4 + j * 2 + k].reshape(1536, 128) for k in range(2)], axis=1
            )
            value = matmul(mixed[every[m]], b).astype(BF16)
            image[u % 8, j * 2, every[m]] = value[:, :128]
            image[u % 8, j * 2 + 1, every[m]] = value[:, 128:]
            return 0

        lax.fori_loop(0, 2, tile, 0)

        @pl.when(has_role(p, 1))
        def _():
            for item in hops[u][1]:
                item.start()

    @staged
    def hop(u, k):
        m, v = UNITS[u][0], u % 8

        @pl.when(has_role(UNITS[u][2], k))
        def _():
            for side in range(2):
                hops[u][k - 1][side].wait_recv()
                e = (zmod(5 - k) if side == 0 else zmod(3 + k)) // 2
                if k == 2:
                    rows, term = (first, second)[side][m], ring[v, side, 1, first[m]]
                else:
                    rows, term = every[m], ring[v, side, places[k - 1], every[m]]
                image[v, e, rows] = (image[v, e, rows].astype(F32) + term.astype(F32)).astype(BF16)
                hops[u][k][side].start()

    def folded(value):
        return jnp.sum(value.reshape(-1, 8, 128), axis=0)

    stores = []

    @staged
    def finish(u):
        m, i, p = UNITS[u]
        h = lax.rem(x + i, X)
        v, count, rows_here = u % 8, ROWS[m], pl.ds(STARTS[m], ROWS[m])
        done = (pl.ds(h * 4, 4), rows_here)
        stores.append(
            (p, pltpu.make_async_copy(applied.at[done], out.at[done], local_sems.at[H + 13 + u]))
        )

        @pl.when(has_role(p, 1))
        def _():
            for side in range(2):
                hops[u][4][side].wait_recv()

            def piece(s, sums):
                squares, crossed, images = sums
                rows = pl.ds(pl.multiple_of(4 * STARTS[m] + s * count, 16), count)
                value = (
                    image[v, z // 2, rows].astype(F32)
                    + ring[v, 0, 1, rows].astype(F32)
                    + ring[v, 1, 1, rows].astype(F32)
                )
                applied[h * 4 + s, rows_here] = value
                start = state[h * 4 + s, rows_here].astype(F32)
                return (
                    squares + folded(start * start),
                    crossed + folded(start * value),
                    images + folded(value * value),
                )

            sums = lax.fori_loop(0, 4, piece, (totals[0], totals[1], totals[2]))
            for k in range(3):
                totals[k] = sums[k]
            stores[-1][1].start()

    @staged
    def turn(k):
        if k == 0:
            load_left.wait()
            for item in a_swap:
                item.start()
            lax.fori_loop(0, 12, transpose_own, 0)
        if k == 1:
            for item in a_swap:
                item.wait_recv()
        if k == 2:
            lax.fori_loop(0, 12, transpose_other, 0)
        if k == 3:
            for item in load_sites:
                item.wait()
            fill_pairs()

    totals[...] = jnp.zeros((3, 8, 128), F32)
    stages = {
        OWN: start_own,
        TURN: turn,
        NEAR: pass_near,
        REST: pass_rest,
        BLOCKS: get_blocks,
        LEFT: left_item,
        DIRECT: start_direct,
        FAR: pass_far,
        MIX: mix,
        ENVS: start_envs,
        PENVS: pass_envs,
        RF: start_far_envs,
        FENVS: pass_far_envs,
        CON: contract,
        HOP: hop,
        FIN: finish,
    }
    for name, *numbers in ORDER:
        stages[name](*numbers)

    @staged
    def all_sum(phase, values, slots, me, targets):
        slots[me] = values
        sends = [copy(slots.at[me], slots.at[me], target) for target in targets]
        for item in sends:
            item.start()
        for item in sends:
            item.wait_recv()
        return jnp.sum(slots[...], axis=0)

    lane = lax.broadcasted_iota(jnp.int32, (1, 128), 1)
    packed = jnp.zeros((1, 128), F32)
    for k in range(3):
        packed = jnp.where(lane == k, jnp.sum(totals[k], keepdims=True), packed)
    packed = all_sum(0, packed, sums_z, z, z_peers)
    packed = all_sum(1, packed, sums_xy, (x * Y + y) * 2 + c, xy_peers)
    square, projection, image_square = (
        jnp.sum(jnp.where(lane == k, packed, 0.0), keepdims=True) * (1.0 / ENTRIES) for k in range(3)
    )
    norm_sq = square + EPSILON
    alpha = projection / norm_sq
    residual_sq = (image_square - 2.0 * alpha * projection + alpha * alpha * square) / norm_sq
    beta = jnp.sqrt(residual_sq + EPSILON)
    scale = 1.0 / (jnp.sqrt(norm_sq) * beta)
    for k, value in enumerate((alpha, beta, scale)):
        coef[k] = value[0, 0]
    with jax.named_scope("drain"):
        for item in used:
            if id(item) not in hop_copies:
                item.wait_send()
        for p in range(2):

            @pl.when(has_role(p, 1))
            def _():
                for (_, _, q), sends in zip(UNITS, hops):
                    for k in (1, 3) if q == p else (2, 4):
                        for item in sends[k]:
                            item.wait_send()
                for q, item in stores:
                    if q == p:
                        item.wait()


def kernel(*refs):
    pl.run_scoped(
        functools.partial(step, *refs),
        pltpu.SemaphoreType.DMA((N_SEMS,)),
        pltpu.SemaphoreType.DMA((N_SEMS,)),
        pltpu.SemaphoreType.DMA((H + 13 + len(UNITS),)),
    )


def normalize(applied_in, state_in, terms_in, out, coef, applied, state, result, terms, sems):
    load_terms = pltpu.make_async_copy(terms_in, terms, sems.at[0])
    load_terms.start()
    parts = [pl.ds(4 * k, 4) for k in range(4)]
    loads, stores = [], []
    for k, part in enumerate(parts):
        loads.append(pltpu.make_async_copy(applied_in.at[part], applied.at[part], sems.at[1 + k]))
        loads.append(pltpu.make_async_copy(state_in.at[part], state.at[part], sems.at[5 + k]))
        stores.append(pltpu.make_async_copy(result.at[part], out.at[part], sems.at[9 + k]))
    for item in loads:
        item.start()
    load_terms.wait()
    alpha, beta, scale = (terms[k] for k in range(3))
    coef[0] = alpha
    coef[1] = beta
    for k in range(4):
        loads[2 * k].wait()
        loads[2 * k + 1].wait()

        def rows_of(i, _):
            result[i] = (applied[i] - alpha * state[i].astype(F32)) * scale
            return 0

        lax.fori_loop(4 * k, 4 * k + 4, rows_of, 0)
        stores[k].start()
    for item in stores:
        item.wait()


def body(state, left_env, right_env, site_one, site_two):
    smem = pl.BlockSpec(memory_space=pltpu.SMEM)
    anywhere = pl.BlockSpec(memory_space=pl.ANY)
    state = state.reshape(16, 128, 128)
    applied, terms = pl.pallas_call(
        kernel,
        out_shape=(
            jax.ShapeDtypeStruct((16, 128, 128), F32),
            jax.ShapeDtypeStruct((3,), F32),
        ),
        in_specs=[anywhere] * 5,
        out_specs=(anywhere, smem),
        scratch_shapes=[
            pltpu.VMEM((16, 128, 128), F32),
            pltpu.SMEM((3, 2, 2, 3), F32),
            pltpu.SMEM((3, 2, 2, 3), F32),
            pltpu.VMEM((16, 128, 128), BF16),
            pltpu.VMEM((12, 128, 1024), BF16),
            pltpu.VMEM((144, 8, 128), F32),
            pltpu.VMEM((4, 8, 4, 128, 128), BF16),
            pltpu.VMEM((4, 12, 128, 128), BF16),
            pltpu.VMEM((1536, 1024), BF16),
            pltpu.VMEM((H, 384, 512), BF16),
            pltpu.VMEM((H, 384, 512), BF16),
            pltpu.VMEM((H, 384, 512), BF16),
            pltpu.VMEM((H, TOP_ROWS, 512), F32),
            pltpu.VMEM((H, 384 - TOP_ROWS, 512), F32),
            pltpu.VMEM((H, 384, 512), F32),
            pltpu.VMEM((H, TOP_ROWS, 512), BF16),
            pltpu.VMEM((H, 384 - TOP_ROWS, 512), BF16),
            pltpu.VMEM((H, 384, 512), BF16),
            pltpu.VMEM((H, 384, 512), BF16),
            pltpu.VMEM((512, 1536), BF16),
            pltpu.VMEM((4, 8, 12, 128, 128), BF16),
            pltpu.VMEM((8, 4, 512, 128), BF16),
            pltpu.VMEM((8, 2, 2, 512, 128), BF16),
            pltpu.VMEM((3, 8, 128), F32),
            pltpu.VMEM((8, 1, 128), F32),
            pltpu.VMEM((32, 1, 128), F32),
        ],
        compiler_params=pltpu.CompilerParams(
            collective_id=0, has_side_effects=True, vmem_limit_bytes=64_000_000
        ),
        name="lanczos",
    )(
        site_one.transpose(0, 2, 3, 1),
        site_two.transpose(0, 2, 3, 1),
        state,
        left_env.reshape(12, 128, 1024),
        right_env.reshape(12, 128, 1024),
    )
    out, coef = pl.pallas_call(
        normalize,
        out_shape=(
            jax.ShapeDtypeStruct((16, 128, 128), F32),
            jax.ShapeDtypeStruct((2,), F32),
        ),
        in_specs=[anywhere] * 3,
        out_specs=(anywhere, smem),
        scratch_shapes=[
            pltpu.VMEM((16, 128, 128), F32),
            pltpu.VMEM((16, 128, 128), BF16),
            pltpu.VMEM((16, 128, 128), F32),
            pltpu.SMEM((3,), F32),
            pltpu.SemaphoreType.DMA((13,)),
        ],
        compiler_params=pltpu.CompilerParams(vmem_limit_bytes=64_000_000),
        name="normalize",
    )(applied, state, terms)
    return out.reshape(1, 4, 4, 128, 128), coef


def solution(mesh):
    torus = Mesh(
        mesh.devices.reshape(4, 2, mesh.shape["rb"], mesh.shape["wa"]), ("lb_0", "lb_1", "rb", "wa")
    )
    in_specs = (
        P("wa", None, None, LB, "rb"),
        P(None, None, LB, "wa", None),
        P(None, None, "rb", "wa", None),
        P(),
        P(),
    )
    out_specs = (P("wa", None, None, LB, "rb"), P())
    return jax.shard_map(body, mesh=torus, in_specs=in_specs, out_specs=out_specs, check_vma=False)
```

```python
import functools

import jax
import jax.numpy as jnp
from jax import lax
from jax.experimental import pallas as pl
from jax.experimental.pallas import tpu as pltpu
from jax.sharding import Mesh
from jax.sharding import PartitionSpec as P

LB = ("lb_0", "lb_1")
EPSILON = 1e-06
ENTRIES = 4.0 * 4 * 4 * 1024 * 1024
F32, BF16 = jnp.float32, jnp.bfloat16
X, Y, Z, H = 4, 4, 8, 4
N_SEMS = 440
ROWS = (64, 32, 32)
STARTS = tuple(sum(ROWS[:m]) for m in range(len(ROWS)))
TOPS = tuple((3 * r // 16 + (m + 1) % 2) // 2 * 16 for m, r in enumerate(ROWS))
TOP_STARTS = tuple(sum(TOPS[:m]) for m in range(len(ROWS)))
TOP_ROWS = sum(TOPS)
ITEMS = 4 * len(ROWS)
UNITS = tuple((m, i, p) for m in range(len(ROWS)) for i in (0, 1, 3, 2) for p in range(2))


OWN, TURN, NEAR, REST, BLOCKS, LEFT, DIRECT, FAR, MIX, ENVS, PENVS, RF, FENVS, CON, HOP, FIN = range(16)
ORDER = (
    (OWN, 1), (TURN, 0), (OWN, 3), (NEAR, 1), (TURN, 1), (OWN, 0), (TURN, 2), (REST, 1), (TURN, 3), (OWN, 2),
    (NEAR, 3), (BLOCKS, 1), (LEFT, 1), (LEFT, 9), (DIRECT, 1), (NEAR, 0), (REST, 3), (NEAR, 2), (REST, 2),
    (ENVS, 0), (ENVS, 1), (FAR, 1), (REST, 0), (ENVS, 2), (BLOCKS, 3), (DIRECT, 9), (LEFT, 3), (DIRECT, 3),
    (BLOCKS, 2), (LEFT, 2), (DIRECT, 2), (BLOCKS, 0), (LEFT, 0), (DIRECT, 0), (PENVS, 0), (FAR, 2), (FAR, 3),
    (MIX, 1), (FAR, 0), (ENVS, 3), (PENVS, 1), (LEFT, 8), (RF, 0), (LEFT, 11), (MIX, 2), (LEFT, 10),
    (DIRECT, 8), (MIX, 3), (MIX, 0), (FAR, 9), (CON, 0), (FAR, 8), (CON, 1), (DIRECT, 11), (CON, 2), (CON, 4),
    (FAR, 11), (HOP, 0, 2), (DIRECT, 10), (HOP, 1, 2), (FAR, 10), (MIX, 9), (LEFT, 6), (LEFT, 7), (MIX, 8),
    (LEFT, 5), (HOP, 4, 2), (PENVS, 2), (DIRECT, 6), (LEFT, 4), (MIX, 11), (HOP, 2, 2), (PENVS, 3),
    (HOP, 1, 3), (HOP, 0, 3), (MIX, 10), (CON, 16), (DIRECT, 5), (CON, 20), (CON, 18), (HOP, 4, 3), (FAR, 6),
    (RF, 1), (CON, 17), (CON, 5), (HOP, 2, 3), (CON, 19), (CON, 21), (HOP, 16, 2), (FAR, 5), (HOP, 1, 4),
    (DIRECT, 4), (CON, 3), (HOP, 18, 2), (HOP, 20, 2), (FAR, 4), (FAR, 7), (HOP, 2, 4), (HOP, 17, 2),
    (HOP, 5, 2), (HOP, 19, 2), (HOP, 0, 4), (HOP, 21, 2), (DIRECT, 7), (FENVS, 0), (HOP, 3, 2), (MIX, 5),
    (HOP, 4, 4), (MIX, 6), (CON, 22), (MIX, 4), (HOP, 20, 3), (HOP, 17, 3), (CON, 6), (HOP, 5, 3),
    (HOP, 16, 3), (MIX, 7), (CON, 8), (CON, 13), (CON, 12), (HOP, 21, 3), (HOP, 19, 3), (CON, 10),
    (HOP, 18, 3), (HOP, 17, 4), (CON, 9), (CON, 14), (HOP, 3, 3), (HOP, 5, 4), (FENVS, 1), (HOP, 13, 2),
    (HOP, 21, 4), (CON, 11), (HOP, 9, 2), (HOP, 3, 4), (HOP, 22, 2), (HOP, 8, 2), (HOP, 12, 2), (FIN, 1),
    (CON, 7), (HOP, 11, 2), (CON, 23), (HOP, 10, 2), (HOP, 20, 4), (HOP, 22, 3), (HOP, 7, 2), (HOP, 23, 2),
    (CON, 15), (HOP, 14, 2), (HOP, 12, 3), (HOP, 6, 2), (HOP, 16, 4), (HOP, 13, 3), (FIN, 4), (HOP, 15, 2),
    (HOP, 10, 3), (HOP, 14, 3), (HOP, 6, 3), (FIN, 16), (HOP, 9, 3), (HOP, 18, 4), (HOP, 13, 4), (FIN, 2),
    (FIN, 17), (HOP, 11, 3), (FIN, 0), (HOP, 23, 3), (HOP, 9, 4), (HOP, 7, 3), (HOP, 8, 3), (HOP, 15, 3),
    (HOP, 11, 4), (HOP, 12, 4), (HOP, 23, 4), (FIN, 20), (FIN, 5), (FIN, 18), (HOP, 7, 4), (HOP, 15, 4),
    (HOP, 22, 4), (HOP, 10, 4), (HOP, 14, 4), (HOP, 6, 4), (HOP, 8, 4), (FIN, 11), (HOP, 19, 4), (FIN, 22),
    (FIN, 14), (FIN, 21), (FIN, 12), (FIN, 10), (FIN, 9), (FIN, 3), (FIN, 6), (FIN, 23), (FIN, 7), (FIN, 8),
    (FIN, 19), (FIN, 13), (FIN, 15),
)


def staged(f):
    def run(*args):
        with jax.named_scope(f"{f.__name__}#" + "_".join(str(a) for a in args if isinstance(a, int))):
            return f(*args)

    return run


def matmul(a, b):
    return lax.dot_general(a, b, (((1,), (0,)), ((), ())), preferred_element_type=F32)


def step(
    one_in,
    two_in,
    state_in,
    left_in,
    right_in,
    applied,
    terms,
    one,
    two,
    state,
    left,
    pair,
    blocks,
    left_other,
    left_t,
    far,
    up,
    down,
    up_own,
    down_own,
    here,
    up_far,
    down_far,
    from_below,
    from_above,
    mixed,
    envs,
    image,
    ring,
    totals,
    sums_z,
    sums_xy,
    send_sems,
    recv_sems,
    local_sems,
):
    y, c, z, x = (lax.axis_index(a) for a in ("lb_0", "lb_1", "rb", "wa"))
    other = 1 - c

    def at(dx=0, dy=0, dz=0, core=None):
        return (
            lax.rem(y + dy, Y),
            c if core is None else core,
            lax.rem(z + dz, Z),
            lax.rem(x + dx, X),
        )

    used = []

    def copy(src, dst, device):
        k = len(used)
        used.append(
            pltpu.make_async_remote_copy(
                src_ref=src,
                dst_ref=dst,
                send_sem=send_sems.at[k],
                recv_sem=recv_sems.at[k],
                device_id=device,
                device_id_type=pl.DeviceIdType.MESH,
            )
        )
        return used[-1]

    partner = at(core=other)
    x_up, x_down = at(dx=1), at(dx=X - 1)
    y_up, y_down = at(dy=1), at(dy=Y - 1)
    z_up, z_down = at(dz=1), at(dz=Z - 1)
    z_peers = [at(dz=k) for k in range(1, Z)]
    xy_peers = [
        at(dx=i, dy=j, core=core)
        for i in range(X)
        for j in range(Y)
        for core in (c, other)
        if not (i == 0 and j == 0 and core is c)
    ]

    barrier = pltpu.get_barrier_semaphore()
    peers = [partner, x_up, x_down, y_up, y_down, z_up, z_down]
    for peer in peers:
        pl.semaphore_signal(barrier, inc=1, device_id=peer, device_id_type=pl.DeviceIdType.MESH)

    own = x * 2 + c
    load_state = pltpu.make_async_copy(state_in, state, local_sems.at[H + 1])
    load_left = pltpu.make_async_copy(left_in, left, local_sems.at[H + 2])
    load_sites = [
        pltpu.make_async_copy(one_in, one, local_sems.at[H + 3]),
        pltpu.make_async_copy(two_in, two, local_sems.at[H + 4]),
    ]
    local = [
        pltpu.make_async_copy(state_in.at[pl.ds(h * 4, 4)], blocks.at[h, own], local_sems.at[h])
        for h in range(H)
    ]
    load_right = [
        pltpu.make_async_copy(
            right_in.at[:, :, pl.ds(b * 128, 128)],
            envs.at[0, b % 2 * 4 + b // 2],
            local_sems.at[H + 5 + b],
        )
        for b in range(Z)
    ]
    for item in load_sites + [load_state, load_left] + local + load_right:
        item.start()

    def fill_pairs():
        for w in range(3):
            for v in range(3):
                for s in range(4):
                    for t in range(4):
                        total = sum(
                            one[w, s // 2, t // 2, u] * two[u, s % 2, t % 2, v] for u in range(3)
                        )
                        k = ((w * 3 + v) * 4 + s) * 4 + t
                        pair[k] = jnp.full((8, 128), total, F32)

    with jax.named_scope("entry"):
        load_state.wait()
        pl.semaphore_wait(barrier, len(peers))

    g_below = lax.rem(x + X - 1, X) * 2 + c
    g_above = lax.rem(x + 1, X) * 2 + c
    g_far = lax.rem(x + 2, X) * 2 + c
    lo, hi = pl.ds(0, 2), pl.ds(2, 2)
    mine = [state.at[pl.ds(h * 4, 4)] for h in range(H)]

    def send_mine(h, parts, device):
        return [copy(mine[h].at[part], blocks.at[h, own, part], device) for part in parts]

    b_up = [send_mine(h, (lo, hi), x_up) for h in range(H)]
    b_down = [send_mine(h, (hi, lo), x_down) for h in range(H)]
    b_own = [copy(mine[h], blocks.at[h, own], partner) for h in range(H)]
    bf_up = [copy(blocks.at[h, g_below, lo], blocks.at[h, g_below, lo], x_up) for h in range(H)]
    bf_down = [copy(blocks.at[h, g_above, hi], blocks.at[h, g_above, hi], x_down) for h in range(H)]
    b_pass = [
        [
            copy(blocks.at[h, g_below], blocks.at[h, g_below], partner),
            copy(blocks.at[h, g_above], blocks.at[h, g_above], partner),
            copy(blocks.at[h, g_far, lo], blocks.at[h, g_far, lo], partner),
            copy(blocks.at[h, g_far, hi], blocks.at[h, g_far, hi], partner),
        ]
        for h in range(H)
    ]

    @staged
    def start_own(h):
        for pair_of in zip(b_up[h], b_down[h]):
            for item in pair_of:
                item.start()
        b_own[h].start()

    @staged
    def pass_near(h):
        b_up[h][0].wait_recv()
        bf_up[h].start()
        b_down[h][0].wait_recv()
        bf_down[h].start()

    @staged
    def pass_rest(h):
        for item in b_up[h][1:]:
            item.wait_recv()
        b_pass[h][0].start()
        for item in b_down[h][1:]:
            item.wait_recv()
        b_pass[h][1].start()

    @staged
    def get_blocks(h):
        bf_up[h].wait_recv()
        b_pass[h][2].start()
        bf_down[h].wait_recv()
        b_pass[h][3].start()
        local[h].wait()
        b_own[h].wait_recv()
        for item in b_pass[h]:
            item.wait_recv()

    a_swap = [
        copy(
            left.at[:, :, pl.ds(pl.multiple_of(k * 256 + other * 128, 128), 128)],
            left_other.at[k],
            partner,
        )
        for k in range(Y)
    ]

    def put_left(r, w, g, core, tile):
        cols = pl.ds(pl.multiple_of((g * 2 + core) * 128, 128), 128)
        turned = tile.T
        for start, count in zip(STARTS, ROWS):
            row = pl.multiple_of(12 * start + 3 * r * count + w * count, 16)
            left_t[pl.ds(row, count), cols] = turned[start : start + count]

    def transpose_own(i, _):
        for r in range(Y):
            cols = pl.ds(pl.multiple_of(lax.rem(y + r, Y) * 256 + c * 128, 128), 128)
            put_left(r, i // 4, lax.rem(i, 4), c, left[i, :, cols])
        return 0

    def transpose_other(i, _):
        for r in range(Y):
            put_left(r, i // 4, lax.rem(i, 4), other, left_other[lax.rem(y + r, Y), i])
        return 0

    items = [divmod(i, H) for i in range(ITEMS)]
    full = [pl.ds(3 * start, 3 * count) for start, count in zip(STARTS, ROWS)]
    top = [pl.ds(3 * start, size) for start, size in zip(STARTS, TOPS)]
    low = [
        pl.ds(3 * start + size, 3 * count - size) for start, size, count in zip(STARTS, TOPS, ROWS)
    ]
    top_own = [pl.ds(start, size) for start, size in zip(TOP_STARTS, TOPS)]
    low_own = [
        pl.ds(3 * start - before, 3 * count - size)
        for start, before, size, count in zip(STARTS, TOP_STARTS, TOPS, ROWS)
    ]
    c_far_up = [copy(far.at[h, top[m]], up_far.at[h, top_own[m]], y_up) for m, h in items]
    c_far_down = [copy(far.at[h, low[m]], down_far.at[h, low_own[m]], y_down) for m, h in items]
    c_up_low = [copy(up.at[h, low[m]], from_below.at[h, low[m]], y_up) for m, h in items]
    c_down_top = [copy(down.at[h, top[m]], from_above.at[h, top[m]], y_down) for m, h in items]
    c_up_top = [copy(up.at[h, top[m]], from_below.at[h, top[m]], y_up) for m, h in items]
    c_down_low = [copy(down.at[h, low[m]], from_above.at[h, low[m]], y_down) for m, h in items]

    @staged
    def left_item(i):
        m, h = items[i]
        n, size = 3 * ROWS[m], TOPS[m]

        def tile(j, _):
            cols = pl.ds(pl.multiple_of(j * 256, 256), 256)
            b = jnp.concatenate(
                [blocks[h, :, j * 2].reshape(1024, 128), blocks[h, :, j * 2 + 1].reshape(1024, 128)],
                axis=1,
            )
            value = matmul(left_t[pl.ds(12 * STARTS[m], 4 * n)], b)
            here[h, full[m], cols] = value[:n]
            up_own[h, top_own[m], cols] = value[n : n + size]
            up[h, low[m], cols] = value[n + size : 2 * n].astype(BF16)
            far[h, full[m], cols] = value[2 * n : 3 * n].astype(BF16)
            down[h, top[m], cols] = value[3 * n : 3 * n + size].astype(BF16)
            down_own[h, low_own[m], cols] = value[3 * n + size :]
            return 0

        lax.fori_loop(0, 2, tile, 0)
        c_far_up[i].start()
        c_far_down[i].start()

    @staged
    def start_direct(i):
        c_up_low[i].start()
        c_down_top[i].start()

    @staged
    def pass_far(i):
        m, h = items[i]
        mine_up, mine_down = (h, top_own[m]), (h, low_own[m])
        c_far_up[i].wait_recv()
        up[h, top[m]] = (up_own[mine_up] + up_far[mine_up].astype(F32)).astype(BF16)
        c_up_top[i].start()
        c_far_down[i].wait_recv()
        down[h, low[m]] = (down_own[mine_down] + down_far[mine_down].astype(F32)).astype(BF16)
        c_down_low[i].start()

    @staged
    def mix(i):
        m, h = items[i]
        for item in (c_up_low[i], c_down_top[i], c_up_top[i], c_down_low[i]):
            item.wait_recv()

        def rows_of(k, _):
            start = pl.multiple_of(k * 16, 16)
            parts = []
            for w in range(3):
                for s in range(4):
                    row = 3 * STARTS[m] + w * ROWS[m] + start
                    at_ws = (h, pl.ds(row, 16), slice(s * 128, (s + 1) * 128))
                    part = here[at_ws] + from_below[at_ws].astype(F32) + from_above[at_ws].astype(F32)
                    parts.append(part.reshape(2, 8, 128))
            for v in range(3):
                for t in range(4):
                    total = None
                    for w in range(3):
                        for s in range(4):
                            term = pair[((w * 3 + v) * 4 + s) * 4 + t][None] * parts[w * 4 + s]
                            total = term if total is None else total + term
                    k = v * 4 + h
                    row = 4 * STARTS[m] + t * ROWS[m] + start
                    mixed[pl.ds(row, 16), k * 128 : (k + 1) * 128] = total.reshape(16, 128).astype(BF16)
            return 0

        lax.fori_loop(0, ROWS[m] // 16, rows_of, 0)

    half = pl.ds(c * 6, 6)
    q_lo, q_hi = pl.ds(c * 6, 3), pl.ds(c * 6 + 3, 3)
    pieces = [(pl.ds(2 * k, 2), half) for k in range(4)]
    r_up = [copy(envs.at[0, *q], envs.at[3, *q], x_up) for q in pieces]
    r_down = [copy(envs.at[0, *q], envs.at[1, *q], x_down) for q in pieces]
    rp_below = [copy(envs.at[3, *q], envs.at[3, *q], partner) for q in pieces]
    rp_above = [copy(envs.at[1, *q], envs.at[1, *q], partner) for q in pieces]
    group = [pl.ds(4 * p, 4) for p in range(2)]
    rf_up = [copy(envs.at[3, g, q_lo], envs.at[2, g, q_lo], x_up) for g in group]
    rf_down = [copy(envs.at[1, g, q_hi], envs.at[2, g, q_hi], x_down) for g in group]
    rp_lo = [copy(envs.at[2, g, q_lo], envs.at[2, g, q_lo], partner) for g in group]
    rp_hi = [copy(envs.at[2, g, q_hi], envs.at[2, g, q_hi], partner) for g in group]

    @staged
    def start_envs(k):
        if k == 0:
            for item in load_right:
                item.wait()
        r_up[k].start()
        r_down[k].start()

    @staged
    def pass_envs(k):
        r_up[k].wait_recv()
        rp_below[k].start()
        r_down[k].wait_recv()
        rp_above[k].start()

    @staged
    def start_far_envs(p):
        rf_up[p].start()
        rf_down[p].start()

    @staged
    def pass_far_envs(p):
        rf_up[p].wait_recv()
        rp_lo[p].start()
        rf_down[p].wait_recv()
        rp_hi[p].start()

    def zmod(k):
        return lax.rem(z + k, Z)

    parity = lax.rem(z, 2)

    def has_role(p, hop):
        return parity == (p if hop % 2 == 1 else 1 - p)

    first = [pl.ds(4 * start, 2 * count) for start, count in zip(STARTS, ROWS)]
    second = [pl.ds(4 * start + 2 * count, 2 * count) for start, count in zip(STARTS, ROWS)]
    every = [pl.ds(4 * start, 4 * count) for start, count in zip(STARTS, ROWS)]
    places = {1: None, 2: 0, 3: 0, 4: 1}
    hops = []
    for u in range(len(UNITS)):
        m, v = UNITS[u][0], u % 8
        sends = {}
        sends[1] = (
            copy(image.at[v, zmod(4) // 2, first[m]], ring.at[v, 0, 1, first[m]], z_up),
            copy(image.at[v, zmod(4) // 2, second[m]], ring.at[v, 1, 1, first[m]], z_down),
        )
        for k in (2, 3, 4):
            sends[k] = tuple(
                copy(
                    image.at[v, zmod(owner) // 2, every[m]],
                    ring.at[v, side, places[k], every[m]],
                    device,
                )
                for side, owner, device in ((0, 5 - k, z_up), (1, 3 + k, z_down))
            )
        hops.append(sends)
    hop_copies = {id(item) for sends in hops for k in sends for item in sends[k]}

    waited = set()

    @staged
    def contract(u):
        m, i, p = UNITS[u]
        needed = {
            0: [],
            1: rp_above[2 * p : 2 * p + 2],
            3: rp_below[2 * p : 2 * p + 2],
            2: [rp_lo[p], rp_hi[p]],
        }[i]
        for item in needed:
            if id(item) not in waited:
                waited.add(id(item))
                item.wait_recv()

        def tile(j, _):
            b = jnp.concatenate(
                [envs[i, p * 4 + j * 2 + k].reshape(1536, 128) for k in range(2)], axis=1
            )
            value = matmul(mixed[every[m]], b).astype(BF16)
            image[u % 8, j * 2, every[m]] = value[:, :128]
            image[u % 8, j * 2 + 1, every[m]] = value[:, 128:]
            return 0

        lax.fori_loop(0, 2, tile, 0)

        @pl.when(has_role(p, 1))
        def _():
            for item in hops[u][1]:
                item.start()

    @staged
    def hop(u, k):
        m, v = UNITS[u][0], u % 8

        @pl.when(has_role(UNITS[u][2], k))
        def _():
            for side in range(2):
                hops[u][k - 1][side].wait_recv()
                e = (zmod(5 - k) if side == 0 else zmod(3 + k)) // 2
                if k == 2:
                    rows, term = (first, second)[side][m], ring[v, side, 1, first[m]]
                else:
                    rows, term = every[m], ring[v, side, places[k - 1], every[m]]
                image[v, e, rows] = (image[v, e, rows].astype(F32) + term.astype(F32)).astype(BF16)
                hops[u][k][side].start()

    def folded(value):
        return jnp.sum(value.reshape(-1, 8, 128), axis=0)

    @staged
    def finish(u):
        m, i, p = UNITS[u]
        h = lax.rem(x + i, X)
        v, count, rows_here = u % 8, ROWS[m], pl.ds(STARTS[m], ROWS[m])

        @pl.when(has_role(p, 1))
        def _():
            for side in range(2):
                hops[u][4][side].wait_recv()

            def piece(s, sums):
                squares, crossed, images = sums
                rows = pl.ds(pl.multiple_of(4 * STARTS[m] + s * count, 16), count)
                value = (
                    image[v, z // 2, rows].astype(F32)
                    + ring[v, 0, 1, rows].astype(F32)
                    + ring[v, 1, 1, rows].astype(F32)
                )
                applied[h * 4 + s, rows_here] = value
                start = state[h * 4 + s, rows_here].astype(F32)
                return (
                    squares + folded(start * start),
                    crossed + folded(start * value),
                    images + folded(value * value),
                )

            sums = lax.fori_loop(0, 4, piece, (totals[0], totals[1], totals[2]))
            for k in range(3):
                totals[k] = sums[k]

    @staged
    def turn(k):
        if k == 0:
            load_left.wait()
            for item in a_swap:
                item.start()
            lax.fori_loop(0, 12, transpose_own, 0)
        if k == 1:
            for item in a_swap:
                item.wait_recv()
        if k == 2:
            lax.fori_loop(0, 12, transpose_other, 0)
        if k == 3:
            for item in load_sites:
                item.wait()
            fill_pairs()

    totals[...] = jnp.zeros((3, 8, 128), F32)
    stages = {
        OWN: start_own,
        TURN: turn,
        NEAR: pass_near,
        REST: pass_rest,
        BLOCKS: get_blocks,
        LEFT: left_item,
        DIRECT: start_direct,
        FAR: pass_far,
        MIX: mix,
        ENVS: start_envs,
        PENVS: pass_envs,
        RF: start_far_envs,
        FENVS: pass_far_envs,
        CON: contract,
        HOP: hop,
        FIN: finish,
    }
    for name, *numbers in ORDER:
        stages[name](*numbers)

    n_before = len(used)

    def drain():
        for item in used[:n_before]:
            if id(item) not in hop_copies:
                item.wait_send()
        for p in range(2):

            @pl.when(has_role(p, 1))
            def _():
                for (_, _, q), sends in zip(UNITS, hops):
                    for k in (1, 3) if q == p else (2, 4):
                        for item in sends[k]:
                            item.wait_send()

    @staged
    def all_sum(phase, values, slots, me, targets):
        slots[me] = values
        sends = [copy(slots.at[me], slots.at[me], target) for target in targets]
        for item in sends:
            item.start()
        if phase == 0:
            drain()
        for item in sends:
            item.wait_recv()
        return jnp.sum(slots[...], axis=0)

    lane = lax.broadcasted_iota(jnp.int32, (1, 128), 1)
    packed = jnp.zeros((1, 128), F32)
    for k in range(3):
        packed = jnp.where(lane == k, jnp.sum(totals[k], keepdims=True), packed)
    packed = all_sum(0, packed, sums_z, z, z_peers)
    packed = all_sum(1, packed, sums_xy, (x * Y + y) * 2 + c, xy_peers)
    square, projection, image_square = (
        jnp.sum(jnp.where(lane == k, packed, 0.0), keepdims=True) * (1.0 / ENTRIES) for k in range(3)
    )
    norm_sq = square + EPSILON
    alpha = projection / norm_sq
    residual_sq = (image_square - 2.0 * alpha * projection + alpha * alpha * square) / norm_sq
    beta = jnp.sqrt(residual_sq + EPSILON)
    scale = 1.0 / (jnp.sqrt(norm_sq) * beta)
    for k, value in enumerate((alpha, beta, scale)):
        terms[k : k + 1] = jnp.broadcast_to(value, (1, 128))
    with jax.named_scope("drain"):
        for item in used[n_before:]:
            item.wait_send()


def kernel(*refs):
    pl.run_scoped(
        functools.partial(step, *refs),
        pltpu.SemaphoreType.DMA((N_SEMS,)),
        pltpu.SemaphoreType.DMA((N_SEMS,)),
        pltpu.SemaphoreType.DMA((H + 13,)),
    )


def normalize(applied, state, terms, out, coef, result, sems):
    alpha, scale = terms[0:1], terms[2:3]
    coef[0] = terms[0, 0]
    coef[1] = terms[1, 0]
    stores = []
    for k in range(4):

        def rows_of(i, _):
            result[i] = (applied[i] - alpha * state[i].astype(F32)) * scale
            return 0

        lax.fori_loop(4 * k, 4 * k + 4, rows_of, 0)
        part = pl.ds(4 * k, 4)
        stores.append(pltpu.make_async_copy(result.at[part], out.at[part], sems.at[k]))
        stores[k].start()
    for item in stores:
        item.wait()


def body(state, left_env, right_env, site_one, site_two):
    smem = pl.BlockSpec(memory_space=pltpu.SMEM)
    anywhere = pl.BlockSpec(memory_space=pl.ANY)
    vmem = pl.BlockSpec(memory_space=pltpu.VMEM)
    state = state.reshape(16, 128, 128)
    applied, terms = pl.pallas_call(
        kernel,
        out_shape=(
            pltpu.VMEM((16, 128, 128), F32),
            pltpu.VMEM((8, 128), F32),
        ),
        in_specs=[anywhere] * 5,
        out_specs=(vmem, vmem),
        scratch_shapes=[
            pltpu.SMEM((3, 2, 2, 3), F32),
            pltpu.SMEM((3, 2, 2, 3), F32),
            pltpu.VMEM((16, 128, 128), BF16),
            pltpu.VMEM((12, 128, 1024), BF16),
            pltpu.VMEM((144, 8, 128), F32),
            pltpu.VMEM((4, 8, 4, 128, 128), BF16),
            pltpu.VMEM((4, 12, 128, 128), BF16),
            pltpu.VMEM((1536, 1024), BF16),
            pltpu.VMEM((H, 384, 512), BF16),
            pltpu.VMEM((H, 384, 512), BF16),
            pltpu.VMEM((H, 384, 512), BF16),
            pltpu.VMEM((H, TOP_ROWS, 512), F32),
            pltpu.VMEM((H, 384 - TOP_ROWS, 512), F32),
            pltpu.VMEM((H, 384, 512), F32),
            pltpu.VMEM((H, TOP_ROWS, 512), BF16),
            pltpu.VMEM((H, 384 - TOP_ROWS, 512), BF16),
            pltpu.VMEM((H, 384, 512), BF16),
            pltpu.VMEM((H, 384, 512), BF16),
            pltpu.VMEM((512, 1536), BF16),
            pltpu.VMEM((4, 8, 12, 128, 128), BF16),
            pltpu.VMEM((8, 4, 512, 128), BF16),
            pltpu.VMEM((8, 2, 2, 512, 128), BF16),
            pltpu.VMEM((3, 8, 128), F32),
            pltpu.VMEM((8, 1, 128), F32),
            pltpu.VMEM((32, 1, 128), F32),
        ],
        compiler_params=pltpu.CompilerParams(
            collective_id=0, has_side_effects=True, vmem_limit_bytes=58_500_000
        ),
        name="lanczos",
    )(
        site_one.transpose(0, 2, 3, 1),
        site_two.transpose(0, 2, 3, 1),
        state,
        left_env.reshape(12, 128, 1024),
        right_env.reshape(12, 128, 1024),
    )
    out, coef = pl.pallas_call(
        normalize,
        out_shape=(
            jax.ShapeDtypeStruct((16, 128, 128), F32),
            jax.ShapeDtypeStruct((2,), F32),
        ),
        in_specs=[vmem, vmem, vmem],
        out_specs=(anywhere, smem),
        scratch_shapes=[
            pltpu.VMEM((16, 128, 128), F32),
            pltpu.SemaphoreType.DMA((4,)),
        ],
        compiler_params=pltpu.CompilerParams(vmem_limit_bytes=8_000_000),
        name="normalize",
    )(applied, state, terms)
    return out.reshape(1, 4, 4, 128, 128), coef


def solution(mesh):
    torus = Mesh(
        mesh.devices.reshape(4, 2, mesh.shape["rb"], mesh.shape["wa"]), ("lb_0", "lb_1", "rb", "wa")
    )
    in_specs = (
        P("wa", None, None, LB, "rb"),
        P(None, None, LB, "wa", None),
        P(None, None, "rb", "wa", None),
        P(),
        P(),
    )
    out_specs = (P("wa", None, None, LB, "rb"), P())
    return jax.shard_map(body, mesh=torus, in_specs=in_specs, out_specs=out_specs, check_vma=False)
```

```python
import functools

import jax
import jax.numpy as jnp
from jax import lax
from jax.experimental import pallas as pl
from jax.experimental.pallas import tpu as pltpu
from jax.sharding import Mesh
from jax.sharding import PartitionSpec as P

LB = ("lb_0", "lb_1")
EPSILON = 1e-06
ENTRIES = 4.0 * 4 * 4 * 1024 * 1024
F32, BF16 = jnp.float32, jnp.bfloat16
X, Y, Z, H = 4, 4, 8, 4
N_SEMS = 440
ROWS = (64, 32, 32)
STARTS = tuple(sum(ROWS[:m]) for m in range(len(ROWS)))
TOPS = tuple((3 * r // 16 + (m + 1) % 2) // 2 * 16 for m, r in enumerate(ROWS))
TOP_STARTS = tuple(sum(TOPS[:m]) for m in range(len(ROWS)))
TOP_ROWS = sum(TOPS)
ITEMS = 4 * len(ROWS)
UNITS = tuple((m, i, p) for m in range(len(ROWS)) for i in (0, 1, 3, 2) for p in range(2))


OWN, TURN, NEAR, REST, BLOCKS, LEFT, DIRECT, FAR, MIX, ENVS, PENVS, RF, FENVS, CON, HOP, FIN = range(16)
ORDER = (
    (OWN, 3), (TURN, 0), (OWN, 0), (NEAR, 3), (OWN, 2), (NEAR, 0), (OWN, 1), (REST, 0), (TURN, 1), (REST, 3),
    (TURN, 2), (BLOCKS, 3), (NEAR, 2), (LEFT, 11), (LEFT, 3), (ENVS, 0), (DIRECT, 3), (TURN, 3), (BLOCKS, 0),
    (LEFT, 0), (REST, 2), (NEAR, 1), (FAR, 3), (ENVS, 1), (DIRECT, 0), (BLOCKS, 2), (FAR, 0), (LEFT, 2),
    (REST, 1), (DIRECT, 2), (BLOCKS, 1), (ENVS, 2), (LEFT, 1), (DIRECT, 1), (FAR, 2), (MIX, 0), (PENVS, 0),
    (FAR, 1), (LEFT, 9), (LEFT, 10), (ENVS, 3), (LEFT, 8), (MIX, 3), (DIRECT, 11), (PENVS, 1), (FAR, 11),
    (MIX, 2), (DIRECT, 9), (MIX, 1), (DIRECT, 10), (CON, 2), (CON, 1), (DIRECT, 8), (CON, 4), (RF, 0),
    (CON, 0), (FAR, 8), (HOP, 1, 2), (FAR, 9), (HOP, 2, 2), (FAR, 10), (HOP, 4, 2), (LEFT, 6), (PENVS, 2),
    (HOP, 0, 2), (LEFT, 4), (LEFT, 7), (HOP, 2, 3), (MIX, 11), (MIX, 8), (LEFT, 5), (HOP, 4, 3), (MIX, 9),
    (HOP, 1, 3), (PENVS, 3), (RF, 1), (MIX, 10), (CON, 17), (DIRECT, 4), (CON, 18), (CON, 20), (HOP, 2, 4),
    (HOP, 0, 3), (FAR, 4), (DIRECT, 7), (DIRECT, 6), (CON, 16), (CON, 5), (CON, 3), (FAR, 7), (FAR, 6),
    (HOP, 17, 2), (CON, 21), (HOP, 1, 4), (HOP, 5, 2), (HOP, 20, 2), (HOP, 18, 2), (FAR, 5), (DIRECT, 5),
    (CON, 19), (HOP, 0, 4), (HOP, 21, 2), (MIX, 4), (FENVS, 0), (HOP, 16, 2), (HOP, 17, 3), (HOP, 3, 2),
    (HOP, 20, 3), (MIX, 7), (HOP, 19, 2), (HOP, 4, 4), (HOP, 18, 3), (HOP, 5, 3), (MIX, 6), (CON, 6),
    (CON, 22), (HOP, 21, 3), (HOP, 17, 4), (MIX, 5), (CON, 11), (CON, 9), (HOP, 16, 3), (HOP, 3, 3),
    (CON, 12), (CON, 14), (HOP, 5, 4), (HOP, 19, 3), (HOP, 6, 2), (HOP, 21, 4), (CON, 10), (FENVS, 1),
    (HOP, 9, 2), (CON, 8), (HOP, 3, 4), (HOP, 20, 4), (HOP, 11, 2), (CON, 13), (HOP, 6, 3), (HOP, 12, 2),
    (HOP, 14, 2), (CON, 7), (CON, 23), (FIN, 2), (HOP, 13, 2), (CON, 15), (HOP, 7, 2), (HOP, 22, 2),
    (HOP, 16, 4), (HOP, 23, 2), (HOP, 9, 3), (HOP, 8, 2), (HOP, 11, 3), (HOP, 12, 3), (HOP, 10, 2),
    (HOP, 15, 2), (HOP, 19, 4), (FIN, 0), (HOP, 22, 3), (HOP, 14, 3), (HOP, 18, 4), (HOP, 11, 4),
    (HOP, 10, 3), (HOP, 6, 4), (FIN, 20), (HOP, 8, 3), (HOP, 23, 3), (HOP, 9, 4), (HOP, 7, 3), (FIN, 17),
    (FIN, 6), (HOP, 23, 4), (HOP, 15, 3), (FIN, 21), (HOP, 13, 3), (HOP, 22, 4), (HOP, 7, 4), (HOP, 12, 4),
    (HOP, 15, 4), (FIN, 5), (HOP, 14, 4), (HOP, 13, 4), (FIN, 12), (FIN, 14), (FIN, 22), (FIN, 18),
    (HOP, 10, 4), (FIN, 3), (FIN, 10), (FIN, 4), (FIN, 19), (HOP, 8, 4), (FIN, 11), (FIN, 16), (FIN, 1),
    (FIN, 9), (FIN, 23), (FIN, 7), (FIN, 15), (FIN, 13), (FIN, 8),
)


def staged(f):
    def run(*args):
        with jax.named_scope(f"{f.__name__}#" + "_".join(str(a) for a in args if isinstance(a, int))):
            return f(*args)

    return run


def matmul(a, b):
    return lax.dot_general(a, b, (((1,), (0,)), ((), ())), preferred_element_type=F32)


def step(
    one_in,
    two_in,
    state_in,
    left_in,
    right_in,
    applied,
    terms,
    one,
    two,
    state,
    left,
    pair,
    blocks,
    left_other,
    left_t,
    far,
    up,
    down,
    up_own,
    down_own,
    here,
    up_far,
    down_far,
    from_below,
    from_above,
    mixed,
    envs,
    image,
    ring,
    totals,
    sums_z,
    sums_xy,
    send_sems,
    recv_sems,
    local_sems,
):
    y, c, z, x = (lax.axis_index(a) for a in ("lb_0", "lb_1", "rb", "wa"))
    other = 1 - c

    def at(dx=0, dy=0, dz=0, core=None):
        return (
            lax.rem(y + dy, Y),
            c if core is None else core,
            lax.rem(z + dz, Z),
            lax.rem(x + dx, X),
        )

    used = []

    def copy(src, dst, device):
        k = len(used)
        used.append(
            pltpu.make_async_remote_copy(
                src_ref=src,
                dst_ref=dst,
                send_sem=send_sems.at[k],
                recv_sem=recv_sems.at[k],
                device_id=device,
                device_id_type=pl.DeviceIdType.MESH,
            )
        )
        return used[-1]

    partner = at(core=other)
    x_up, x_down = at(dx=1), at(dx=X - 1)
    y_up, y_down = at(dy=1), at(dy=Y - 1)
    z_up, z_down = at(dz=1), at(dz=Z - 1)
    z_peers = [at(dz=k) for k in (4, 3, 5, 2, 6, 1, 7)]
    distance = (0, 1, 2, 1)
    xy_peers = [
        at(dx=i, dy=j, core=core)
        for i, j in sorted(
            ((i, j) for i in range(X) for j in range(Y)),
            key=lambda ij: -distance[ij[0]] - distance[ij[1]],
        )
        for core in (other, c)
        if not (i == 0 and j == 0 and core is c)
    ]

    barrier = pltpu.get_barrier_semaphore()
    peers = [partner, x_up, x_down, y_up, y_down, z_up, z_down]
    for peer in peers:
        pl.semaphore_signal(barrier, inc=1, device_id=peer, device_id_type=pl.DeviceIdType.MESH)

    own = x * 2 + c
    load_state = pltpu.make_async_copy(state_in, state, local_sems.at[H + 1])
    load_left = pltpu.make_async_copy(left_in, left, local_sems.at[H + 2])
    load_sites = [
        pltpu.make_async_copy(one_in, one, local_sems.at[H + 3]),
        pltpu.make_async_copy(two_in, two, local_sems.at[H + 4]),
    ]
    local = [
        pltpu.make_async_copy(state_in.at[pl.ds(h * 4, 4)], blocks.at[h, own], local_sems.at[h])
        for h in range(H)
    ]
    load_right = [
        pltpu.make_async_copy(
            right_in.at[:, :, pl.ds(b * 128, 128)],
            envs.at[0, b % 2 * 4 + b // 2],
            local_sems.at[H + 5 + b],
        )
        for b in range(Z)
    ]
    for item in load_sites + [load_state, load_left] + local + load_right:
        item.start()

    def fill_pairs():
        for w in range(3):
            for v in range(3):
                for s in range(4):
                    for t in range(4):
                        total = sum(
                            one[w, s // 2, t // 2, u] * two[u, s % 2, t % 2, v] for u in range(3)
                        )
                        k = ((w * 3 + v) * 4 + s) * 4 + t
                        pair[k] = jnp.full((8, 128), total, F32)

    with jax.named_scope("entry"):
        load_state.wait()
        pl.semaphore_wait(barrier, len(peers))

    g_below = lax.rem(x + X - 1, X) * 2 + c
    g_above = lax.rem(x + 1, X) * 2 + c
    g_far = lax.rem(x + 2, X) * 2 + c
    lo, hi = pl.ds(0, 2), pl.ds(2, 2)
    mine = [state.at[pl.ds(h * 4, 4)] for h in range(H)]

    def send_mine(h, parts, device):
        return [copy(mine[h].at[part], blocks.at[h, own, part], device) for part in parts]

    b_up = [send_mine(h, (lo, hi), x_up) for h in range(H)]
    b_down = [send_mine(h, (hi, lo), x_down) for h in range(H)]
    b_own = [copy(mine[h], blocks.at[h, own], partner) for h in range(H)]
    bf_up = [copy(blocks.at[h, g_below, lo], blocks.at[h, g_below, lo], x_up) for h in range(H)]
    bf_down = [copy(blocks.at[h, g_above, hi], blocks.at[h, g_above, hi], x_down) for h in range(H)]
    b_pass = [
        [
            copy(blocks.at[h, g_below], blocks.at[h, g_below], partner),
            copy(blocks.at[h, g_above], blocks.at[h, g_above], partner),
            copy(blocks.at[h, g_far, lo], blocks.at[h, g_far, lo], partner),
            copy(blocks.at[h, g_far, hi], blocks.at[h, g_far, hi], partner),
        ]
        for h in range(H)
    ]

    @staged
    def start_own(h):
        for pair_of in zip(b_up[h], b_down[h]):
            for item in pair_of:
                item.start()
        b_own[h].start()

    @staged
    def pass_near(h):
        b_up[h][0].wait_recv()
        bf_up[h].start()
        b_down[h][0].wait_recv()
        bf_down[h].start()

    @staged
    def pass_rest(h):
        for item in b_up[h][1:]:
            item.wait_recv()
        b_pass[h][0].start()
        for item in b_down[h][1:]:
            item.wait_recv()
        b_pass[h][1].start()

    @staged
    def get_blocks(h):
        bf_up[h].wait_recv()
        b_pass[h][2].start()
        bf_down[h].wait_recv()
        b_pass[h][3].start()
        local[h].wait()
        b_own[h].wait_recv()
        for item in b_pass[h]:
            item.wait_recv()

    a_swap = [
        copy(
            left.at[:, :, pl.ds(pl.multiple_of(k * 256 + other * 128, 128), 128)],
            left_other.at[k],
            partner,
        )
        for k in range(Y)
    ]

    def put_left(r, w, g, core, tile):
        cols = pl.ds(pl.multiple_of((g * 2 + core) * 128, 128), 128)
        turned = tile.T
        for start, count in zip(STARTS, ROWS):
            row = pl.multiple_of(12 * start + 3 * r * count + w * count, 16)
            left_t[pl.ds(row, count), cols] = turned[start : start + count]

    def transpose_own(i, _):
        for r in range(Y):
            cols = pl.ds(pl.multiple_of(lax.rem(y + r, Y) * 256 + c * 128, 128), 128)
            put_left(r, i // 4, lax.rem(i, 4), c, left[i, :, cols])
        return 0

    def transpose_other(i, _):
        for r in range(Y):
            put_left(r, i // 4, lax.rem(i, 4), other, left_other[lax.rem(y + r, Y), i])
        return 0

    items = [divmod(i, H) for i in range(ITEMS)]
    full = [pl.ds(3 * start, 3 * count) for start, count in zip(STARTS, ROWS)]
    top = [pl.ds(3 * start, size) for start, size in zip(STARTS, TOPS)]
    low = [
        pl.ds(3 * start + size, 3 * count - size) for start, size, count in zip(STARTS, TOPS, ROWS)
    ]
    top_own = [pl.ds(start, size) for start, size in zip(TOP_STARTS, TOPS)]
    low_own = [
        pl.ds(3 * start - before, 3 * count - size)
        for start, before, size, count in zip(STARTS, TOP_STARTS, TOPS, ROWS)
    ]
    c_far_up = [copy(far.at[h, top[m]], up_far.at[h, top_own[m]], y_up) for m, h in items]
    c_far_down = [copy(far.at[h, low[m]], down_far.at[h, low_own[m]], y_down) for m, h in items]
    c_up_low = [copy(up.at[h, low[m]], from_below.at[h, low[m]], y_up) for m, h in items]
    c_down_top = [copy(down.at[h, top[m]], from_above.at[h, top[m]], y_down) for m, h in items]
    c_up_top = [copy(up.at[h, top[m]], from_below.at[h, top[m]], y_up) for m, h in items]
    c_down_low = [copy(down.at[h, low[m]], from_above.at[h, low[m]], y_down) for m, h in items]

    @staged
    def left_item(i):
        m, h = items[i]
        n, size = 3 * ROWS[m], TOPS[m]

        def tile(j, _):
            cols = pl.ds(pl.multiple_of(j * 256, 256), 256)
            b = jnp.concatenate(
                [blocks[h, :, j * 2].reshape(1024, 128), blocks[h, :, j * 2 + 1].reshape(1024, 128)],
                axis=1,
            )
            value = matmul(left_t[pl.ds(12 * STARTS[m], 4 * n)], b)
            here[h, full[m], cols] = value[:n]
            up_own[h, top_own[m], cols] = value[n : n + size]
            up[h, low[m], cols] = value[n + size : 2 * n].astype(BF16)
            far[h, full[m], cols] = value[2 * n : 3 * n].astype(BF16)
            down[h, top[m], cols] = value[3 * n : 3 * n + size].astype(BF16)
            down_own[h, low_own[m], cols] = value[3 * n + size :]
            return 0

        lax.fori_loop(0, 2, tile, 0)
        c_far_up[i].start()
        c_far_down[i].start()

    @staged
    def start_direct(i):
        c_up_low[i].start()
        c_down_top[i].start()

    @staged
    def pass_far(i):
        m, h = items[i]
        mine_up, mine_down = (h, top_own[m]), (h, low_own[m])
        c_far_up[i].wait_recv()
        up[h, top[m]] = (up_own[mine_up] + up_far[mine_up].astype(F32)).astype(BF16)
        c_up_top[i].start()
        c_far_down[i].wait_recv()
        down[h, low[m]] = (down_own[mine_down] + down_far[mine_down].astype(F32)).astype(BF16)
        c_down_low[i].start()

    @staged
    def mix(i):
        m, h = items[i]
        for item in (c_up_low[i], c_down_top[i], c_up_top[i], c_down_low[i]):
            item.wait_recv()

        def rows_of(k, _):
            start = pl.multiple_of(k * 16, 16)
            parts = []
            for w in range(3):
                for s in range(4):
                    row = 3 * STARTS[m] + w * ROWS[m] + start
                    at_ws = (h, pl.ds(row, 16), slice(s * 128, (s + 1) * 128))
                    part = here[at_ws] + from_below[at_ws].astype(F32) + from_above[at_ws].astype(F32)
                    parts.append(part.reshape(2, 8, 128))
            for v in range(3):
                for t in range(4):
                    total = None
                    for w in range(3):
                        for s in range(4):
                            term = pair[((w * 3 + v) * 4 + s) * 4 + t][None] * parts[w * 4 + s]
                            total = term if total is None else total + term
                    k = v * 4 + h
                    row = 4 * STARTS[m] + t * ROWS[m] + start
                    mixed[pl.ds(row, 16), k * 128 : (k + 1) * 128] = total.reshape(16, 128).astype(BF16)
            return 0

        lax.fori_loop(0, ROWS[m] // 16, rows_of, 0)

    half = pl.ds(c * 6, 6)
    q_lo, q_hi = pl.ds(c * 6, 3), pl.ds(c * 6 + 3, 3)
    pieces = [(pl.ds(2 * k, 2), half) for k in range(4)]
    r_up = [copy(envs.at[0, *q], envs.at[3, *q], x_up) for q in pieces]
    r_down = [copy(envs.at[0, *q], envs.at[1, *q], x_down) for q in pieces]
    rp_below = [copy(envs.at[3, *q], envs.at[3, *q], partner) for q in pieces]
    rp_above = [copy(envs.at[1, *q], envs.at[1, *q], partner) for q in pieces]
    group = [pl.ds(4 * p, 4) for p in range(2)]
    rf_up = [copy(envs.at[3, g, q_lo], envs.at[2, g, q_lo], x_up) for g in group]
    rf_down = [copy(envs.at[1, g, q_hi], envs.at[2, g, q_hi], x_down) for g in group]
    rp_lo = [copy(envs.at[2, g, q_lo], envs.at[2, g, q_lo], partner) for g in group]
    rp_hi = [copy(envs.at[2, g, q_hi], envs.at[2, g, q_hi], partner) for g in group]

    @staged
    def start_envs(k):
        if k == 0:
            for item in load_right:
                item.wait()
        r_up[k].start()
        r_down[k].start()

    @staged
    def pass_envs(k):
        r_up[k].wait_recv()
        rp_below[k].start()
        r_down[k].wait_recv()
        rp_above[k].start()

    @staged
    def start_far_envs(p):
        rf_up[p].start()
        rf_down[p].start()

    @staged
    def pass_far_envs(p):
        rf_up[p].wait_recv()
        rp_lo[p].start()
        rf_down[p].wait_recv()
        rp_hi[p].start()

    def zmod(k):
        return lax.rem(z + k, Z)

    parity = lax.rem(z, 2)

    def has_role(p, hop):
        return parity == (p if hop % 2 == 1 else 1 - p)

    first = [pl.ds(4 * start, 2 * count) for start, count in zip(STARTS, ROWS)]
    second = [pl.ds(4 * start + 2 * count, 2 * count) for start, count in zip(STARTS, ROWS)]
    every = [pl.ds(4 * start, 4 * count) for start, count in zip(STARTS, ROWS)]
    places = {1: None, 2: 0, 3: 0, 4: 1}
    hops = []
    for u in range(len(UNITS)):
        m, v = UNITS[u][0], u % 8
        sends = {}
        sends[1] = (
            copy(image.at[v, zmod(4) // 2, first[m]], ring.at[v, 0, 1, first[m]], z_up),
            copy(image.at[v, zmod(4) // 2, second[m]], ring.at[v, 1, 1, first[m]], z_down),
        )
        for k in (2, 3, 4):
            sends[k] = tuple(
                copy(
                    image.at[v, zmod(owner) // 2, every[m]],
                    ring.at[v, side, places[k], every[m]],
                    device,
                )
                for side, owner, device in ((0, 5 - k, z_up), (1, 3 + k, z_down))
            )
        hops.append(sends)
    hop_copies = {id(item) for sends in hops for k in sends for item in sends[k]}

    waited = set()

    @staged
    def contract(u):
        m, i, p = UNITS[u]
        needed = {
            0: [],
            1: rp_above[2 * p : 2 * p + 2],
            3: rp_below[2 * p : 2 * p + 2],
            2: [rp_lo[p], rp_hi[p]],
        }[i]
        for item in needed:
            if id(item) not in waited:
                waited.add(id(item))
                item.wait_recv()

        def tile(j, _):
            b = jnp.concatenate(
                [envs[i, p * 4 + j * 2 + k].reshape(1536, 128) for k in range(2)], axis=1
            )
            value = matmul(mixed[every[m]], b).astype(BF16)
            image[u % 8, j * 2, every[m]] = value[:, :128]
            image[u % 8, j * 2 + 1, every[m]] = value[:, 128:]
            return 0

        lax.fori_loop(0, 2, tile, 0)

        @pl.when(has_role(p, 1))
        def _():
            for item in hops[u][1]:
                item.start()

    @staged
    def hop(u, k):
        m, v = UNITS[u][0], u % 8

        @pl.when(has_role(UNITS[u][2], k))
        def _():
            for side in range(2):
                hops[u][k - 1][side].wait_recv()
                e = (zmod(5 - k) if side == 0 else zmod(3 + k)) // 2
                if k == 2:
                    rows, term = (first, second)[side][m], ring[v, side, 1, first[m]]
                else:
                    rows, term = every[m], ring[v, side, places[k - 1], every[m]]
                image[v, e, rows] = (image[v, e, rows].astype(F32) + term.astype(F32)).astype(BF16)
                hops[u][k][side].start()

    def folded(value):
        return jnp.sum(value.reshape(-1, 8, 128), axis=0)

    @staged
    def finish(u):
        m, i, p = UNITS[u]
        h = lax.rem(x + i, X)
        v, count, rows_here = u % 8, ROWS[m], pl.ds(STARTS[m], ROWS[m])

        @pl.when(has_role(p, 1))
        def _():
            for side in range(2):
                hops[u][4][side].wait_recv()

            def piece(s, sums):
                squares, crossed, images = sums
                rows = pl.ds(pl.multiple_of(4 * STARTS[m] + s * count, 16), count)
                value = (
                    image[v, z // 2, rows].astype(F32)
                    + ring[v, 0, 1, rows].astype(F32)
                    + ring[v, 1, 1, rows].astype(F32)
                )
                applied[h * 4 + s, rows_here] = value
                start = state[h * 4 + s, rows_here].astype(F32)
                return (
                    squares + folded(start * start),
                    crossed + folded(start * value),
                    images + folded(value * value),
                )

            sums = lax.fori_loop(0, 4, piece, (totals[0], totals[1], totals[2]))
            for k in range(3):
                totals[k] = sums[k]

    @staged
    def turn(k):
        if k == 0:
            load_left.wait()
            for item in a_swap:
                item.start()
            lax.fori_loop(0, 12, transpose_own, 0)
        if k == 1:
            for item in a_swap:
                item.wait_recv()
        if k == 2:
            lax.fori_loop(0, 12, transpose_other, 0)
        if k == 3:
            for item in load_sites:
                item.wait()
            fill_pairs()

    totals[...] = jnp.zeros((3, 8, 128), F32)
    stages = {
        OWN: start_own,
        TURN: turn,
        NEAR: pass_near,
        REST: pass_rest,
        BLOCKS: get_blocks,
        LEFT: left_item,
        DIRECT: start_direct,
        FAR: pass_far,
        MIX: mix,
        ENVS: start_envs,
        PENVS: pass_envs,
        RF: start_far_envs,
        FENVS: pass_far_envs,
        CON: contract,
        HOP: hop,
        FIN: finish,
    }
    for name, *numbers in ORDER:
        stages[name](*numbers)

    n_before = len(used)

    def drain():
        for item in used[:n_before]:
            if id(item) not in hop_copies:
                item.wait_send()
        for p in range(2):

            @pl.when(has_role(p, 1))
            def _():
                for (_, _, q), sends in zip(UNITS, hops):
                    for k in (1, 3) if q == p else (2, 4):
                        for item in sends[k]:
                            item.wait_send()

    @staged
    def all_sum(phase, values, slots, me, targets):
        slots[me] = values
        sends = [copy(slots.at[me], slots.at[me], target) for target in targets]
        for item in sends:
            item.start()
        if phase == 0:
            drain()
        for item in sends:
            item.wait_recv()
        return jnp.sum(slots[...], axis=0)

    lane = lax.broadcasted_iota(jnp.int32, (1, 128), 1)
    packed = jnp.zeros((1, 128), F32)
    for k in range(3):
        packed = jnp.where(lane == k, jnp.sum(totals[k], keepdims=True), packed)
    packed = all_sum(0, packed, sums_z, z, z_peers)
    packed = all_sum(1, packed, sums_xy, (x * Y + y) * 2 + c, xy_peers)
    square, projection, image_square = (
        jnp.sum(jnp.where(lane == k, packed, 0.0), keepdims=True) * (1.0 / ENTRIES) for k in range(3)
    )
    norm_sq = square + EPSILON
    alpha = projection / norm_sq
    residual_sq = (image_square - 2.0 * alpha * projection + alpha * alpha * square) / norm_sq
    beta = jnp.sqrt(residual_sq + EPSILON)
    scale = 1.0 / (jnp.sqrt(norm_sq) * beta)
    for k, value in enumerate((alpha, beta, scale)):
        terms[k : k + 1] = jnp.broadcast_to(value, (1, 128))
    with jax.named_scope("drain"):
        for item in used[n_before:]:
            item.wait_send()


def kernel(*refs):
    pl.run_scoped(
        functools.partial(step, *refs),
        pltpu.SemaphoreType.DMA((N_SEMS,)),
        pltpu.SemaphoreType.DMA((N_SEMS,)),
        pltpu.SemaphoreType.DMA((H + 13,)),
    )


def normalize(applied, state, terms, out, coef, result, sems):
    alpha, scale = terms[0:1], terms[2:3]
    coef[0] = terms[0, 0]
    coef[1] = terms[1, 0]
    stores = []
    for k in range(4):

        def rows_of(i, _):
            result[i] = (applied[i] - alpha * state[i].astype(F32)) * scale
            return 0

        lax.fori_loop(4 * k, 4 * k + 4, rows_of, 0)
        part = pl.ds(4 * k, 4)
        stores.append(pltpu.make_async_copy(result.at[part], out.at[part], sems.at[k]))
        stores[k].start()
    for item in stores:
        item.wait()


def body(state, left_env, right_env, site_one, site_two):
    smem = pl.BlockSpec(memory_space=pltpu.SMEM)
    anywhere = pl.BlockSpec(memory_space=pl.ANY)
    vmem = pl.BlockSpec(memory_space=pltpu.VMEM)
    state = state.reshape(16, 128, 128)
    applied, terms = pl.pallas_call(
        kernel,
        out_shape=(
            pltpu.VMEM((16, 128, 128), F32),
            pltpu.VMEM((8, 128), F32),
        ),
        in_specs=[anywhere] * 5,
        out_specs=(vmem, vmem),
        scratch_shapes=[
            pltpu.SMEM((3, 2, 2, 3), F32),
            pltpu.SMEM((3, 2, 2, 3), F32),
            pltpu.VMEM((16, 128, 128), BF16),
            pltpu.VMEM((12, 128, 1024), BF16),
            pltpu.VMEM((144, 8, 128), F32),
            pltpu.VMEM((4, 8, 4, 128, 128), BF16),
            pltpu.VMEM((4, 12, 128, 128), BF16),
            pltpu.VMEM((1536, 1024), BF16),
            pltpu.VMEM((H, 384, 512), BF16),
            pltpu.VMEM((H, 384, 512), BF16),
            pltpu.VMEM((H, 384, 512), BF16),
            pltpu.VMEM((H, TOP_ROWS, 512), F32),
            pltpu.VMEM((H, 384 - TOP_ROWS, 512), F32),
            pltpu.VMEM((H, 384, 512), F32),
            pltpu.VMEM((H, TOP_ROWS, 512), BF16),
            pltpu.VMEM((H, 384 - TOP_ROWS, 512), BF16),
            pltpu.VMEM((H, 384, 512), BF16),
            pltpu.VMEM((H, 384, 512), BF16),
            pltpu.VMEM((512, 1536), BF16),
            pltpu.VMEM((4, 8, 12, 128, 128), BF16),
            pltpu.VMEM((8, 4, 512, 128), BF16),
            pltpu.VMEM((8, 2, 2, 512, 128), BF16),
            pltpu.VMEM((3, 8, 128), F32),
            pltpu.VMEM((8, 1, 128), F32),
            pltpu.VMEM((32, 1, 128), F32),
        ],
        compiler_params=pltpu.CompilerParams(
            collective_id=0, has_side_effects=True, vmem_limit_bytes=58_500_000
        ),
        name="lanczos",
    )(
        site_one.transpose(0, 2, 3, 1),
        site_two.transpose(0, 2, 3, 1),
        state,
        left_env.reshape(12, 128, 1024),
        right_env.reshape(12, 128, 1024),
    )
    out, coef = pl.pallas_call(
        normalize,
        out_shape=(
            jax.ShapeDtypeStruct((16, 128, 128), F32),
            jax.ShapeDtypeStruct((2,), F32),
        ),
        in_specs=[vmem, vmem, vmem],
        out_specs=(anywhere, smem),
        scratch_shapes=[
            pltpu.VMEM((16, 128, 128), F32),
            pltpu.SemaphoreType.DMA((4,)),
        ],
        compiler_params=pltpu.CompilerParams(vmem_limit_bytes=8_000_000),
        name="normalize",
    )(applied, state, terms)
    return out.reshape(1, 4, 4, 128, 128), coef


def solution(mesh):
    torus = Mesh(
        mesh.devices.reshape(4, 2, mesh.shape["rb"], mesh.shape["wa"]), ("lb_0", "lb_1", "rb", "wa")
    )
    in_specs = (
        P("wa", None, None, LB, "rb"),
        P(None, None, LB, "wa", None),
        P(None, None, "rb", "wa", None),
        P(),
        P(),
    )
    out_specs = (P("wa", None, None, LB, "rb"), P())
    return jax.shard_map(body, mesh=torus, in_specs=in_specs, out_specs=out_specs, check_vma=False)
```

```python
import functools

import jax
import jax.numpy as jnp
from jax import lax
from jax.experimental import pallas as pl
from jax.experimental.pallas import tpu as pltpu
from jax.sharding import Mesh
from jax.sharding import PartitionSpec as P

LB = ("lb_0", "lb_1")
EPSILON = 1e-06
ENTRIES = 4.0 * 4 * 4 * 1024 * 1024
F32, BF16 = jnp.float32, jnp.bfloat16
X, Y, Z, H = 4, 4, 8, 4
N_SEMS = 440
ROWS = (64, 32, 32)
STARTS = tuple(sum(ROWS[:m]) for m in range(len(ROWS)))
TOPS = tuple((3 * r // 16 + (m + 1) % 2) // 2 * 16 for m, r in enumerate(ROWS))
TOP_STARTS = tuple(sum(TOPS[:m]) for m in range(len(ROWS)))
TOP_ROWS = sum(TOPS)
ITEMS = 4 * len(ROWS)
UNITS = tuple((m, i, p) for m in range(len(ROWS)) for i in (0, 1, 3, 2) for p in range(2))


OWN, TURN, NEAR, REST, BLOCKS, LEFT, DIRECT, FAR, MIX, ENVS, PENVS, RF, FENVS, CON, HOP, FIN = range(16)
ORDER = (
    (OWN, 3), (TURN, 0), (OWN, 0), (NEAR, 3), (OWN, 2), (NEAR, 0), (OWN, 1), (REST, 0), (TURN, 1), (REST, 3),
    (TURN, 2), (BLOCKS, 3), (NEAR, 2), (LEFT, 11), (LEFT, 3), (ENVS, 0), (DIRECT, 3), (TURN, 3), (BLOCKS, 0),
    (LEFT, 0), (REST, 2), (NEAR, 1), (FAR, 3), (ENVS, 1), (DIRECT, 0), (BLOCKS, 2), (FAR, 0), (LEFT, 2),
    (REST, 1), (DIRECT, 2), (BLOCKS, 1), (ENVS, 2), (LEFT, 1), (DIRECT, 1), (FAR, 2), (MIX, 0), (PENVS, 0),
    (FAR, 1), (LEFT, 9), (LEFT, 10), (ENVS, 3), (LEFT, 8), (MIX, 3), (DIRECT, 11), (PENVS, 1), (FAR, 11),
    (MIX, 2), (DIRECT, 9), (MIX, 1), (DIRECT, 10), (CON, 2), (CON, 1), (DIRECT, 8), (CON, 4), (RF, 0),
    (CON, 0), (FAR, 8), (HOP, 1, 2), (FAR, 9), (HOP, 2, 2), (FAR, 10), (HOP, 4, 2), (LEFT, 6), (PENVS, 2),
    (HOP, 0, 2), (LEFT, 4), (LEFT, 7), (HOP, 2, 3), (MIX, 11), (MIX, 8), (LEFT, 5), (HOP, 4, 3), (MIX, 9),
    (HOP, 1, 3), (PENVS, 3), (RF, 1), (MIX, 10), (CON, 17), (DIRECT, 4), (CON, 18), (CON, 20), (HOP, 2, 4),
    (HOP, 0, 3), (FAR, 4), (DIRECT, 7), (DIRECT, 6), (CON, 16), (CON, 5), (CON, 3), (FAR, 7), (FAR, 6),
    (HOP, 17, 2), (CON, 21), (HOP, 1, 4), (HOP, 5, 2), (HOP, 20, 2), (HOP, 18, 2), (FAR, 5), (DIRECT, 5),
    (CON, 19), (HOP, 0, 4), (HOP, 21, 2), (MIX, 4), (FENVS, 0), (HOP, 16, 2), (HOP, 17, 3), (HOP, 3, 2),
    (HOP, 20, 3), (MIX, 7), (HOP, 19, 2), (HOP, 4, 4), (HOP, 18, 3), (HOP, 5, 3), (MIX, 6), (CON, 6),
    (CON, 22), (HOP, 21, 3), (HOP, 17, 4), (MIX, 5), (CON, 11), (CON, 9), (HOP, 16, 3), (HOP, 3, 3),
    (CON, 12), (CON, 14), (HOP, 5, 4), (HOP, 19, 3), (HOP, 6, 2), (HOP, 21, 4), (CON, 10), (FENVS, 1),
    (HOP, 9, 2), (CON, 8), (HOP, 3, 4), (HOP, 20, 4), (HOP, 11, 2), (CON, 13), (HOP, 6, 3), (HOP, 12, 2),
    (HOP, 14, 2), (CON, 7), (CON, 23), (FIN, 2), (HOP, 13, 2), (CON, 15), (HOP, 7, 2), (HOP, 22, 2),
    (HOP, 16, 4), (HOP, 23, 2), (HOP, 9, 3), (HOP, 8, 2), (HOP, 11, 3), (HOP, 12, 3), (HOP, 10, 2),
    (HOP, 15, 2), (HOP, 19, 4), (FIN, 0), (HOP, 22, 3), (HOP, 14, 3), (HOP, 18, 4), (HOP, 11, 4),
    (HOP, 10, 3), (HOP, 6, 4), (FIN, 20), (HOP, 8, 3), (HOP, 23, 3), (HOP, 9, 4), (HOP, 7, 3), (FIN, 17),
    (FIN, 6), (HOP, 23, 4), (HOP, 15, 3), (FIN, 21), (HOP, 13, 3), (HOP, 22, 4), (HOP, 7, 4), (HOP, 12, 4),
    (HOP, 15, 4), (FIN, 5), (HOP, 14, 4), (HOP, 13, 4), (FIN, 12), (FIN, 14), (FIN, 22), (FIN, 18),
    (HOP, 10, 4), (FIN, 3), (FIN, 10), (FIN, 4), (FIN, 19), (HOP, 8, 4), (FIN, 11), (FIN, 16), (FIN, 1),
    (FIN, 9), (FIN, 23), (FIN, 7), (FIN, 15), (FIN, 13), (FIN, 8),
)


def staged(f):
    def run(*args):
        with jax.named_scope(f"{f.__name__}#" + "_".join(str(a) for a in args if isinstance(a, int))):
            return f(*args)

    return run


def matmul(a, b):
    return lax.dot_general(a, b, (((1,), (0,)), ((), ())), preferred_element_type=F32)


def step(
    one_in,
    two_in,
    state_in,
    left_in,
    right_in,
    applied,
    terms,
    one,
    two,
    state,
    left,
    pair,
    blocks,
    left_other,
    left_t,
    far,
    up,
    down,
    up_own,
    down_own,
    here,
    up_far,
    down_far,
    from_below,
    from_above,
    mixed,
    envs,
    image,
    ring,
    totals,
    sums_z,
    sums_xy,
    send_sems,
    recv_sems,
    local_sems,
):
    y, c, z, x = (lax.axis_index(a) for a in ("lb_0", "lb_1", "rb", "wa"))
    other = 1 - c

    def at(dx=0, dy=0, dz=0, core=None):
        return (
            lax.rem(y + dy, Y),
            c if core is None else core,
            lax.rem(z + dz, Z),
            lax.rem(x + dx, X),
        )

    used = []

    def copy(src, dst, device):
        k = len(used)
        used.append(
            pltpu.make_async_remote_copy(
                src_ref=src,
                dst_ref=dst,
                send_sem=send_sems.at[k],
                recv_sem=recv_sems.at[k],
                device_id=device,
                device_id_type=pl.DeviceIdType.MESH,
            )
        )
        return used[-1]

    partner = at(core=other)
    x_up, x_down = at(dx=1), at(dx=X - 1)
    y_up, y_down = at(dy=1), at(dy=Y - 1)
    z_up, z_down = at(dz=1), at(dz=Z - 1)
    z_peers = [at(dz=k) for k in (4, 3, 5, 2, 6, 1, 7)]
    distance = (0, 1, 2, 1)
    xy_peers = [
        at(dx=i, dy=j, core=core)
        for i, j in sorted(
            ((i, j) for i in range(X) for j in range(Y)),
            key=lambda ij: -distance[ij[0]] - distance[ij[1]],
        )
        for core in (other, c)
        if not (i == 0 and j == 0 and core is c)
    ]

    barrier = pltpu.get_barrier_semaphore()
    peers = [partner, x_up, x_down, y_up, y_down, z_up, z_down]
    for peer in peers:
        pl.semaphore_signal(barrier, inc=1, device_id=peer, device_id_type=pl.DeviceIdType.MESH)

    own = x * 2 + c
    load_state = pltpu.make_async_copy(state_in, state, local_sems.at[H + 1])
    load_left = pltpu.make_async_copy(left_in, left, local_sems.at[H + 2])
    load_sites = [
        pltpu.make_async_copy(one_in, one, local_sems.at[H + 3]),
        pltpu.make_async_copy(two_in, two, local_sems.at[H + 4]),
    ]
    local = [
        pltpu.make_async_copy(state_in.at[pl.ds(h * 4, 4)], blocks.at[h, own], local_sems.at[h])
        for h in range(H)
    ]
    load_right = [
        pltpu.make_async_copy(
            right_in.at[:, :, pl.ds(b * 128, 128)],
            envs.at[0, b % 2 * 4 + b // 2],
            local_sems.at[H + 5 + b],
        )
        for b in range(Z)
    ]
    load_state.start()

    def fill_pairs():
        for w in range(3):
            for v in range(3):
                for s in range(4):
                    for t in range(4):
                        total = sum(
                            one[w, s // 2, t // 2, u] * two[u, s % 2, t % 2, v] for u in range(3)
                        )
                        k = ((w * 3 + v) * 4 + s) * 4 + t
                        pair[k] = jnp.full((8, 128), total, F32)

    with jax.named_scope("entry"):
        load_state.wait()
        for item in [load_left] + local + load_sites + load_right:
            item.start()
        pl.semaphore_wait(barrier, len(peers))

    g_below = lax.rem(x + X - 1, X) * 2 + c
    g_above = lax.rem(x + 1, X) * 2 + c
    g_far = lax.rem(x + 2, X) * 2 + c
    lo, hi = pl.ds(0, 2), pl.ds(2, 2)
    mine = [state.at[pl.ds(h * 4, 4)] for h in range(H)]

    def send_mine(h, parts, device):
        return [copy(mine[h].at[part], blocks.at[h, own, part], device) for part in parts]

    b_up = [send_mine(h, (lo, hi), x_up) for h in range(H)]
    b_down = [send_mine(h, (hi, lo), x_down) for h in range(H)]
    b_own = [copy(mine[h], blocks.at[h, own], partner) for h in range(H)]
    bf_up = [copy(blocks.at[h, g_below, lo], blocks.at[h, g_below, lo], x_up) for h in range(H)]
    bf_down = [copy(blocks.at[h, g_above, hi], blocks.at[h, g_above, hi], x_down) for h in range(H)]
    b_pass = [
        [
            copy(blocks.at[h, g_below], blocks.at[h, g_below], partner),
            copy(blocks.at[h, g_above], blocks.at[h, g_above], partner),
            copy(blocks.at[h, g_far, lo], blocks.at[h, g_far, lo], partner),
            copy(blocks.at[h, g_far, hi], blocks.at[h, g_far, hi], partner),
        ]
        for h in range(H)
    ]

    @staged
    def start_own(h):
        for pair_of in zip(b_up[h], b_down[h]):
            for item in pair_of:
                item.start()
        b_own[h].start()

    @staged
    def pass_near(h):
        b_up[h][0].wait_recv()
        bf_up[h].start()
        b_down[h][0].wait_recv()
        bf_down[h].start()

    @staged
    def pass_rest(h):
        for item in b_up[h][1:]:
            item.wait_recv()
        b_pass[h][0].start()
        for item in b_down[h][1:]:
            item.wait_recv()
        b_pass[h][1].start()

    @staged
    def get_blocks(h):
        bf_up[h].wait_recv()
        b_pass[h][2].start()
        bf_down[h].wait_recv()
        b_pass[h][3].start()
        local[h].wait()
        b_own[h].wait_recv()
        for item in b_pass[h]:
            item.wait_recv()

    a_swap = [
        copy(
            left.at[:, :, pl.ds(pl.multiple_of(k * 256 + other * 128, 128), 128)],
            left_other.at[k],
            partner,
        )
        for k in range(Y)
    ]

    def put_left(r, w, g, core, tile):
        cols = pl.ds(pl.multiple_of((g * 2 + core) * 128, 128), 128)
        turned = tile.T
        for start, count in zip(STARTS, ROWS):
            row = pl.multiple_of(12 * start + 3 * r * count + w * count, 16)
            left_t[pl.ds(row, count), cols] = turned[start : start + count]

    def transpose_own(i, _):
        for r in range(Y):
            cols = pl.ds(pl.multiple_of(lax.rem(y + r, Y) * 256 + c * 128, 128), 128)
            put_left(r, i // 4, lax.rem(i, 4), c, left[i, :, cols])
        return 0

    def transpose_other(i, _):
        for r in range(Y):
            put_left(r, i // 4, lax.rem(i, 4), other, left_other[lax.rem(y + r, Y), i])
        return 0

    items = [divmod(i, H) for i in range(ITEMS)]
    full = [pl.ds(3 * start, 3 * count) for start, count in zip(STARTS, ROWS)]
    top = [pl.ds(3 * start, size) for start, size in zip(STARTS, TOPS)]
    low = [
        pl.ds(3 * start + size, 3 * count - size) for start, size, count in zip(STARTS, TOPS, ROWS)
    ]
    top_own = [pl.ds(start, size) for start, size in zip(TOP_STARTS, TOPS)]
    low_own = [
        pl.ds(3 * start - before, 3 * count - size)
        for start, before, size, count in zip(STARTS, TOP_STARTS, TOPS, ROWS)
    ]
    c_far_up = [copy(far.at[h, top[m]], up_far.at[h, top_own[m]], y_up) for m, h in items]
    c_far_down = [copy(far.at[h, low[m]], down_far.at[h, low_own[m]], y_down) for m, h in items]
    c_up_low = [copy(up.at[h, low[m]], from_below.at[h, low[m]], y_up) for m, h in items]
    c_down_top = [copy(down.at[h, top[m]], from_above.at[h, top[m]], y_down) for m, h in items]
    c_up_top = [copy(up.at[h, top[m]], from_below.at[h, top[m]], y_up) for m, h in items]
    c_down_low = [copy(down.at[h, low[m]], from_above.at[h, low[m]], y_down) for m, h in items]

    @staged
    def left_item(i):
        m, h = items[i]
        n, size = 3 * ROWS[m], TOPS[m]

        def tile(j, _):
            cols = pl.ds(pl.multiple_of(j * 256, 256), 256)
            b = jnp.concatenate(
                [blocks[h, :, j * 2].reshape(1024, 128), blocks[h, :, j * 2 + 1].reshape(1024, 128)],
                axis=1,
            )
            value = matmul(left_t[pl.ds(12 * STARTS[m], 4 * n)], b)
            here[h, full[m], cols] = value[:n]
            up_own[h, top_own[m], cols] = value[n : n + size]
            up[h, low[m], cols] = value[n + size : 2 * n].astype(BF16)
            far[h, full[m], cols] = value[2 * n : 3 * n].astype(BF16)
            down[h, top[m], cols] = value[3 * n : 3 * n + size].astype(BF16)
            down_own[h, low_own[m], cols] = value[3 * n + size :]
            return 0

        lax.fori_loop(0, 2, tile, 0)
        c_far_up[i].start()
        c_far_down[i].start()

    @staged
    def start_direct(i):
        c_up_low[i].start()
        c_down_top[i].start()

    @staged
    def pass_far(i):
        m, h = items[i]
        mine_up, mine_down = (h, top_own[m]), (h, low_own[m])
        c_far_up[i].wait_recv()
        up[h, top[m]] = (up_own[mine_up] + up_far[mine_up].astype(F32)).astype(BF16)
        c_up_top[i].start()
        c_far_down[i].wait_recv()
        down[h, low[m]] = (down_own[mine_down] + down_far[mine_down].astype(F32)).astype(BF16)
        c_down_low[i].start()

    @staged
    def mix(i):
        m, h = items[i]
        for item in (c_up_low[i], c_down_top[i], c_up_top[i], c_down_low[i]):
            item.wait_recv()

        def rows_of(k, _):
            start = pl.multiple_of(k * 16, 16)
            parts = []
            for w in range(3):
                for s in range(4):
                    row = 3 * STARTS[m] + w * ROWS[m] + start
                    at_ws = (h, pl.ds(row, 16), slice(s * 128, (s + 1) * 128))
                    part = here[at_ws] + from_below[at_ws].astype(F32) + from_above[at_ws].astype(F32)
                    parts.append(part.reshape(2, 8, 128))
            for v in range(3):
                for t in range(4):
                    total = None
                    for w in range(3):
                        for s in range(4):
                            term = pair[((w * 3 + v) * 4 + s) * 4 + t][None] * parts[w * 4 + s]
                            total = term if total is None else total + term
                    k = v * 4 + h
                    row = 4 * STARTS[m] + t * ROWS[m] + start
                    mixed[pl.ds(row, 16), k * 128 : (k + 1) * 128] = total.reshape(16, 128).astype(BF16)
            return 0

        lax.fori_loop(0, ROWS[m] // 16, rows_of, 0)

    half = pl.ds(c * 6, 6)
    q_lo, q_hi = pl.ds(c * 6, 3), pl.ds(c * 6 + 3, 3)
    pieces = [(pl.ds(2 * k, 2), half) for k in range(4)]
    r_up = [copy(envs.at[0, *q], envs.at[3, *q], x_up) for q in pieces]
    r_down = [copy(envs.at[0, *q], envs.at[1, *q], x_down) for q in pieces]
    rp_below = [copy(envs.at[3, *q], envs.at[3, *q], partner) for q in pieces]
    rp_above = [copy(envs.at[1, *q], envs.at[1, *q], partner) for q in pieces]
    group = [pl.ds(4 * p, 4) for p in range(2)]
    rf_up = [copy(envs.at[3, g, q_lo], envs.at[2, g, q_lo], x_up) for g in group]
    rf_down = [copy(envs.at[1, g, q_hi], envs.at[2, g, q_hi], x_down) for g in group]
    rp_lo = [copy(envs.at[2, g, q_lo], envs.at[2, g, q_lo], partner) for g in group]
    rp_hi = [copy(envs.at[2, g, q_hi], envs.at[2, g, q_hi], partner) for g in group]

    @staged
    def start_envs(k):
        if k == 0:
            for item in load_right:
                item.wait()
        r_up[k].start()
        r_down[k].start()

    @staged
    def pass_envs(k):
        r_up[k].wait_recv()
        rp_below[k].start()
        r_down[k].wait_recv()
        rp_above[k].start()

    @staged
    def start_far_envs(p):
        rf_up[p].start()
        rf_down[p].start()

    @staged
    def pass_far_envs(p):
        rf_up[p].wait_recv()
        rp_lo[p].start()
        rf_down[p].wait_recv()
        rp_hi[p].start()

    def zmod(k):
        return lax.rem(z + k, Z)

    parity = lax.rem(z, 2)

    def has_role(p, hop):
        return parity == (p if hop % 2 == 1 else 1 - p)

    first = [pl.ds(4 * start, 2 * count) for start, count in zip(STARTS, ROWS)]
    second = [pl.ds(4 * start + 2 * count, 2 * count) for start, count in zip(STARTS, ROWS)]
    every = [pl.ds(4 * start, 4 * count) for start, count in zip(STARTS, ROWS)]
    places = {1: None, 2: 0, 3: 0, 4: 1}
    hops = []
    for u in range(len(UNITS)):
        m, v = UNITS[u][0], u % 8
        sends = {}
        sends[1] = (
            copy(image.at[v, zmod(4) // 2, first[m]], ring.at[v, 0, 1, first[m]], z_up),
            copy(image.at[v, zmod(4) // 2, second[m]], ring.at[v, 1, 1, first[m]], z_down),
        )
        for k in (2, 3, 4):
            sends[k] = tuple(
                copy(
                    image.at[v, zmod(owner) // 2, every[m]],
                    ring.at[v, side, places[k], every[m]],
                    device,
                )
                for side, owner, device in ((0, 5 - k, z_up), (1, 3 + k, z_down))
            )
        hops.append(sends)
    hop_copies = {id(item) for sends in hops for k in sends for item in sends[k]}

    waited = set()

    @staged
    def contract(u):
        m, i, p = UNITS[u]
        needed = {
            0: [],
            1: rp_above[2 * p : 2 * p + 2],
            3: rp_below[2 * p : 2 * p + 2],
            2: [rp_lo[p], rp_hi[p]],
        }[i]
        for item in needed:
            if id(item) not in waited:
                waited.add(id(item))
                item.wait_recv()

        def tile(j, _):
            b = jnp.concatenate(
                [envs[i, p * 4 + j * 2 + k].reshape(1536, 128) for k in range(2)], axis=1
            )
            value = matmul(mixed[every[m]], b).astype(BF16)
            image[u % 8, j * 2, every[m]] = value[:, :128]
            image[u % 8, j * 2 + 1, every[m]] = value[:, 128:]
            return 0

        lax.fori_loop(0, 2, tile, 0)

        @pl.when(has_role(p, 1))
        def _():
            for item in hops[u][1]:
                item.start()

    @staged
    def hop(u, k):
        m, v = UNITS[u][0], u % 8

        @pl.when(has_role(UNITS[u][2], k))
        def _():
            for side in range(2):
                hops[u][k - 1][side].wait_recv()
                e = (zmod(5 - k) if side == 0 else zmod(3 + k)) // 2
                if k == 2:
                    rows, term = (first, second)[side][m], ring[v, side, 1, first[m]]
                else:
                    rows, term = every[m], ring[v, side, places[k - 1], every[m]]
                image[v, e, rows] = (image[v, e, rows].astype(F32) + term.astype(F32)).astype(BF16)
                hops[u][k][side].start()

    def folded(value):
        return jnp.sum(value.reshape(-1, 8, 128), axis=0)

    @staged
    def finish(u):
        m, i, p = UNITS[u]
        h = lax.rem(x + i, X)
        v, count, rows_here = u % 8, ROWS[m], pl.ds(STARTS[m], ROWS[m])

        @pl.when(has_role(p, 1))
        def _():
            for side in range(2):
                hops[u][4][side].wait_recv()

            def piece(s, sums):
                squares, crossed, images = sums
                rows = pl.ds(pl.multiple_of(4 * STARTS[m] + s * count, 16), count)
                value = (
                    image[v, z // 2, rows].astype(F32)
                    + ring[v, 0, 1, rows].astype(F32)
                    + ring[v, 1, 1, rows].astype(F32)
                )
                applied[h * 4 + s, rows_here] = value
                start = state[h * 4 + s, rows_here].astype(F32)
                return (
                    squares + folded(start * start),
                    crossed + folded(start * value),
                    images + folded(value * value),
                )

            sums = lax.fori_loop(0, 4, piece, (totals[0], totals[1], totals[2]))
            for k in range(3):
                totals[k] = sums[k]

    @staged
    def turn(k):
        if k == 0:
            load_left.wait()
            for item in a_swap:
                item.start()
            lax.fori_loop(0, 12, transpose_own, 0)
        if k == 1:
            for item in a_swap:
                item.wait_recv()
        if k == 2:
            lax.fori_loop(0, 12, transpose_other, 0)
        if k == 3:
            for item in load_sites:
                item.wait()
            fill_pairs()

    totals[...] = jnp.zeros((3, 8, 128), F32)
    stages = {
        OWN: start_own,
        TURN: turn,
        NEAR: pass_near,
        REST: pass_rest,
        BLOCKS: get_blocks,
        LEFT: left_item,
        DIRECT: start_direct,
        FAR: pass_far,
        MIX: mix,
        ENVS: start_envs,
        PENVS: pass_envs,
        RF: start_far_envs,
        FENVS: pass_far_envs,
        CON: contract,
        HOP: hop,
        FIN: finish,
    }
    for name, *numbers in ORDER:
        stages[name](*numbers)

    n_before = len(used)

    def drain():
        for item in used[:n_before]:
            if id(item) not in hop_copies:
                item.wait_send()
        for p in range(2):

            @pl.when(has_role(p, 1))
            def _():
                for (_, _, q), sends in zip(UNITS, hops):
                    for k in (1, 3) if q == p else (2, 4):
                        for item in sends[k]:
                            item.wait_send()

    @staged
    def all_sum(phase, values, slots, me, targets):
        slots[me] = values
        sends = [copy(slots.at[me], slots.at[me], target) for target in targets]
        for item in sends:
            item.start()
        if phase == 0:
            drain()
        for item in sends:
            item.wait_recv()
        return jnp.sum(slots[...], axis=0)

    lane = lax.broadcasted_iota(jnp.int32, (1, 128), 1)
    packed = jnp.zeros((1, 128), F32)
    for k in range(3):
        packed = jnp.where(lane == k, jnp.sum(totals[k], keepdims=True), packed)
    packed = all_sum(0, packed, sums_z, z, z_peers)
    packed = all_sum(1, packed, sums_xy, (x * Y + y) * 2 + c, xy_peers)
    square, projection, image_square = (
        jnp.sum(jnp.where(lane == k, packed, 0.0), keepdims=True) * (1.0 / ENTRIES) for k in range(3)
    )
    norm_sq = square + EPSILON
    alpha = projection / norm_sq
    residual_sq = (image_square - 2.0 * alpha * projection + alpha * alpha * square) / norm_sq
    beta = jnp.sqrt(residual_sq + EPSILON)
    scale = 1.0 / (jnp.sqrt(norm_sq) * beta)
    for k, value in enumerate((alpha, beta, scale)):
        terms[k : k + 1] = jnp.broadcast_to(value, (1, 128))
    with jax.named_scope("drain"):
        for item in used[n_before:]:
            item.wait_send()


def kernel(*refs):
    pl.run_scoped(
        functools.partial(step, *refs),
        pltpu.SemaphoreType.DMA((N_SEMS,)),
        pltpu.SemaphoreType.DMA((N_SEMS,)),
        pltpu.SemaphoreType.DMA((H + 13,)),
    )


def normalize(applied, state, terms, out, coef, result, sems):
    alpha, scale = terms[0:1], terms[2:3]
    coef[0] = terms[0, 0]
    coef[1] = terms[1, 0]
    stores = []
    for k in range(4):

        def rows_of(i, _):
            result[i] = (applied[i] - alpha * state[i].astype(F32)) * scale
            return 0

        lax.fori_loop(4 * k, 4 * k + 4, rows_of, 0)
        part = pl.ds(4 * k, 4)
        stores.append(pltpu.make_async_copy(result.at[part], out.at[part], sems.at[k]))
        stores[k].start()
    for item in stores:
        item.wait()


def body(state, left_env, right_env, site_one, site_two):
    smem = pl.BlockSpec(memory_space=pltpu.SMEM)
    anywhere = pl.BlockSpec(memory_space=pl.ANY)
    vmem = pl.BlockSpec(memory_space=pltpu.VMEM)
    state = state.reshape(16, 128, 128)
    applied, terms = pl.pallas_call(
        kernel,
        out_shape=(
            pltpu.VMEM((16, 128, 128), F32),
            pltpu.VMEM((8, 128), F32),
        ),
        in_specs=[anywhere] * 5,
        out_specs=(vmem, vmem),
        scratch_shapes=[
            pltpu.SMEM((3, 2, 2, 3), F32),
            pltpu.SMEM((3, 2, 2, 3), F32),
            pltpu.VMEM((16, 128, 128), BF16),
            pltpu.VMEM((12, 128, 1024), BF16),
            pltpu.VMEM((144, 8, 128), F32),
            pltpu.VMEM((4, 8, 4, 128, 128), BF16),
            pltpu.VMEM((4, 12, 128, 128), BF16),
            pltpu.VMEM((1536, 1024), BF16),
            pltpu.VMEM((H, 384, 512), BF16),
            pltpu.VMEM((H, 384, 512), BF16),
            pltpu.VMEM((H, 384, 512), BF16),
            pltpu.VMEM((H, TOP_ROWS, 512), F32),
            pltpu.VMEM((H, 384 - TOP_ROWS, 512), F32),
            pltpu.VMEM((H, 384, 512), F32),
            pltpu.VMEM((H, TOP_ROWS, 512), BF16),
            pltpu.VMEM((H, 384 - TOP_ROWS, 512), BF16),
            pltpu.VMEM((H, 384, 512), BF16),
            pltpu.VMEM((H, 384, 512), BF16),
            pltpu.VMEM((512, 1536), BF16),
            pltpu.VMEM((4, 8, 12, 128, 128), BF16),
            pltpu.VMEM((8, 4, 512, 128), BF16),
            pltpu.VMEM((8, 2, 2, 512, 128), BF16),
            pltpu.VMEM((3, 8, 128), F32),
            pltpu.VMEM((8, 1, 128), F32),
            pltpu.VMEM((32, 1, 128), F32),
        ],
        compiler_params=pltpu.CompilerParams(
            collective_id=0, has_side_effects=True, vmem_limit_bytes=58_500_000
        ),
        name="lanczos",
    )(
        site_one.transpose(0, 2, 3, 1),
        site_two.transpose(0, 2, 3, 1),
        state,
        left_env.reshape(12, 128, 1024),
        right_env.reshape(12, 128, 1024),
    )
    out, coef = pl.pallas_call(
        normalize,
        out_shape=(
            jax.ShapeDtypeStruct((16, 128, 128), F32),
            jax.ShapeDtypeStruct((2,), F32),
        ),
        in_specs=[vmem, vmem, vmem],
        out_specs=(anywhere, smem),
        scratch_shapes=[
            pltpu.VMEM((16, 128, 128), F32),
            pltpu.SemaphoreType.DMA((4,)),
        ],
        compiler_params=pltpu.CompilerParams(vmem_limit_bytes=8_000_000),
        name="normalize",
    )(applied, state, terms)
    return out.reshape(1, 4, 4, 128, 128), coef


def solution(mesh):
    torus = Mesh(
        mesh.devices.reshape(4, 2, mesh.shape["rb"], mesh.shape["wa"]), ("lb_0", "lb_1", "rb", "wa")
    )
    in_specs = (
        P("wa", None, None, LB, "rb"),
        P(None, None, LB, "wa", None),
        P(None, None, "rb", "wa", None),
        P(),
        P(),
    )
    out_specs = (P("wa", None, None, LB, "rb"), P())
    return jax.shard_map(body, mesh=torus, in_specs=in_specs, out_specs=out_specs, check_vma=False)
```
